32 devices in a mesh: dp: 2 (over x), tp: 16 (over z, y, core).
Axes of the slice: x: 2, y: 2, z: 4, core: 2. Of those that a mesh axis runs over, the one named last changes fastest.
Arguments:
- enc_out: bfloat16 [384, 96, 1024], P('dp'), parts along dimension 0
- w_proj: bfloat16 [1024, 8192], P(None, 'tp')
- labels: int32 [384, 24], P('dp'), parts along dimension 0
- in_len: int32 [384], P('dp'), parts along dimension 0
- lab_len: int32 [384], P('dp'), parts along dimension 0
Outputs:
- output 1: float32 [384], P('dp'), parts along dimension 0
- output 2: float32 [2048, 8192], P('dp', 'tp'), parts along dimension 0
- output 3: float32 [384, 96, 1024], P('dp'), parts along dimension 0
There are 2 independent parts. The reference program is written for one: setup_inputs(seed, part) draws one part's arguments, and reference() takes and returns one part's arrays. A program takes and returns all parts, laid end to end along the dimension named above; an argument that names none is the same for every part.
All inputs are finite; a program needn't handle non-finite values.
Results may differ from the reference program's by a relative error of at most 0.001.
Values are sent between devices in bfloat16 or wider.
A program may use at most 1 GiB of HBM per device.

```python
import math
import jax
import jax.numpy as jnp
from jax import lax

HIDDEN = 1024
VOCAB = 8192
FRAMES = 96
MAX_LABELS = 24
BATCH = 192
LAB_MIN = max(1, MAX_LABELS // 5)
NEG_FILL = -1.0e30


def draw_targets(int_key):
    key_lab, key_len, key_in, key_pos = jax.random.split(int_key, 4)
    seq_ids = jnp.arange(BATCH)
    full_pos = jax.random.randint(key_pos, (), 0, BATCH)
    tight_pos = (full_pos + BATCH // 2) % BATCH
    lab_len = jax.random.randint(key_len, (BATCH,), LAB_MIN, MAX_LABELS + 1)
    lab_len = jnp.where(seq_ids == full_pos, MAX_LABELS, jnp.where(seq_ids == tight_pos, LAB_MIN, lab_len))
    in_low = jnp.maximum(2 * lab_len + 1, FRAMES // 5)
    in_len = jax.random.randint(key_in, (BATCH,), in_low, FRAMES + 1)
    in_len = jnp.where(seq_ids == full_pos, FRAMES, jnp.where(seq_ids == tight_pos, 2 * LAB_MIN + 1, in_len))
    lab_ids = jnp.arange(MAX_LABELS)
    labels = jax.random.randint(key_lab, (BATCH, MAX_LABELS), 1, VOCAB)
    at_full = (seq_ids == full_pos)[:, None]
    labels = jnp.where(at_full & (lab_ids == 0)[None, :], 1, jnp.where(at_full & (lab_ids == MAX_LABELS - 1)[None, :], VOCAB - 1, labels))
    return labels.astype(jnp.int32), in_len.astype(jnp.int32), lab_len.astype(jnp.int32)


def setup_inputs(seed: int = 0, part: int = 0) -> dict:
    base_key = jax.random.key(seed)
    part_key = jax.random.fold_in(base_key, part)
    key_hs, key_int = jax.random.split(part_key, 2)
    key_w = jax.random.key(seed + 1)
    enc_out = jax.random.normal(key_hs, (BATCH, FRAMES, HIDDEN), jnp.float32).astype(jnp.bfloat16)
    w_proj = (jax.random.normal(key_w, (HIDDEN, VOCAB), jnp.float32) * (2.0 / math.sqrt(HIDDEN))).astype(jnp.bfloat16)
    labels, in_len, lab_len = draw_targets(key_int)
    return {"enc_out": enc_out, "w_proj": w_proj, "labels": labels, "in_len": in_len, "lab_len": lab_len}


def lattice_loss(label_lp, labels, in_len, lab_len):
    n_seq, n_frames, n_cols = label_lp.shape
    n_lab = n_cols - 1
    n_states = 2 * n_lab + 1
    blank_lp = label_lp[:, :, :1]
    interleaved = jnp.stack([jnp.broadcast_to(blank_lp, (n_seq, n_frames, n_lab)), label_lp[:, :, 1:]], axis=-1)
    emit_all = jnp.concatenate([interleaved.reshape(n_seq, n_frames, 2 * n_lab), blank_lp], axis=-1)
    emit_tm = jnp.swapaxes(emit_all, 0, 1)
    skip_lab = jnp.pad(labels[:, 1:] != labels[:, :-1], ((0, 0), (1, 0)))
    skip_ok = jnp.pad(jnp.stack([jnp.zeros_like(skip_lab), skip_lab], axis=-1).reshape(n_seq, 2 * n_lab), ((0, 0), (0, 1)))
    state_ids = jnp.arange(n_states)
    neg_one = jnp.full((n_seq, 1), NEG_FILL, label_lp.dtype)
    neg_two = jnp.full((n_seq, 2), NEG_FILL, label_lp.dtype)
    alpha_init = jnp.where(state_ids[None, :] == 0, 0.0, neg_one)

    def lattice_step(alpha_prev, step_in):
        emit_t, frame_idx = step_in
        prev_one = jnp.concatenate([neg_one, alpha_prev[:, :-1]], axis=1)
        prev_two = jnp.where(skip_ok, jnp.concatenate([neg_two, alpha_prev[:, :-2]], axis=1), NEG_FILL)
        top_val = lax.stop_gradient(jnp.maximum(jnp.maximum(alpha_prev, prev_one), prev_two))
        merged = top_val + jnp.log(jnp.exp(alpha_prev - top_val) + jnp.exp(prev_one - top_val) + jnp.exp(prev_two - top_val))
        live_seq = (frame_idx < in_len)[:, None]
        return jnp.where(live_seq, merged + emit_t, alpha_prev), None

    alpha_end, _ = lax.scan(lattice_step, alpha_init, (emit_tm, jnp.arange(n_frames)))
    end_sel = (state_ids[None, :] == 2 * lab_len[:, None]) | (state_ids[None, :] == 2 * lab_len[:, None] - 1)
    return -jax.nn.logsumexp(jnp.where(end_sel, alpha_end, NEG_FILL), axis=1)


def label_logprobs(logits, ext_seq):
    log_norm = jax.nn.logsumexp(logits, axis=-1)
    return jnp.take(logits, ext_seq, axis=1) - log_norm[:, None]


def reference(enc_out, w_proj, labels, in_len, lab_len):
    ext_all = jnp.concatenate([jnp.zeros((BATCH, 1), jnp.int32), labels], axis=1)

    def forward_seq(seq_in):
        enc_seq, ext_seq = seq_in
        logits = jnp.dot(enc_seq, w_proj, preferred_element_type=jnp.float32)
        return label_logprobs(logits, ext_seq)

    label_lp = lax.map(forward_seq, (enc_out, ext_all))
    loss, lattice_vjp = jax.vjp(lambda lp_in: lattice_loss(lp_in, labels, in_len, lab_len), label_lp)
    (lp_grad,) = lattice_vjp(jnp.ones_like(loss))

    def backward_seq(grad_acc, seq_in):
        enc_seq, ext_seq, cot_seq = seq_in
        logits = jnp.dot(enc_seq, w_proj, preferred_element_type=jnp.float32)
        _, lp_vjp = jax.vjp(lambda z_in: label_logprobs(z_in, ext_seq), logits)
        (grad_z,) = lp_vjp(cot_seq)
        grad_bf = grad_z.astype(jnp.bfloat16)
        grad_acc = grad_acc + jnp.dot(enc_seq.T, grad_bf, preferred_element_type=jnp.float32)
        grad_hs = jnp.dot(grad_bf, w_proj.T, preferred_element_type=jnp.float32)
        return grad_acc, grad_hs

    grad_w, grad_hs = lax.scan(backward_seq, jnp.zeros((HIDDEN, VOCAB), jnp.float32), (enc_out, ext_all, lp_grad))
    return loss, grad_w, grad_hs
```

```python
import functools

import jax
import jax.numpy as jnp
from jax import lax
from jax.experimental import pallas as pl
from jax.experimental.pallas import tpu as pltpu
from jax.sharding import PartitionSpec as P


NEG_FILL = -1.0e30
BIG = 1.0e30
MESH = pl.DeviceIdType.MESH
NT = (((1,), (1,)), ((), ()))
NN = (((1,), (0,)), ((), ()))
SLOTS = 32
ROWS = 8
CHUNK = 8
VMEM_LIMIT = 60 * 1024 * 1024


def dot(a, b, dims):
    return lax.dot_general(a, b, dims, preferred_element_type=jnp.float32)


def params(**kw):
    return pltpu.CompilerParams(vmem_limit_bytes=VMEM_LIMIT, **kw)


def stats_kernel(enc_ref, wt_ref, out_ref):
    n_seq, n_frames, depth = enc_ref.shape
    enc = enc_ref[...].reshape(n_seq * n_frames, depth)
    z = dot(wt_ref[...], enc, NT)
    top = jnp.max(z, axis=0, keepdims=True)
    out_ref[0, 0:1, :] = top
    out_ref[0, 1:2, :] = jnp.sum(jnp.exp(z - top), axis=0, keepdims=True)


def row_stats(enc, wt, n_owner):
    n_batch, n_frames, depth = enc.shape
    n_cols = wt.shape[0]
    n_seq = n_batch // n_owner
    rows = n_seq * n_frames
    return pl.pallas_call(
        stats_kernel,
        grid=(n_owner,),
        in_specs=[pl.BlockSpec((n_seq, n_frames, depth), lambda i: (i, 0, 0)), pl.BlockSpec((n_cols, depth), lambda i: (0, 0))],
        out_specs=pl.BlockSpec((1, 2, rows), lambda i: (i, 0, 0)),
        out_shape=jax.ShapeDtypeStruct((n_owner, 2, rows), jnp.float32),
        compiler_params=params(),
        cost_estimate=pl.CostEstimate(flops=2 * n_batch * n_frames * depth * n_cols, bytes_accessed=2 * enc.size, transcendentals=n_batch * n_frames * n_cols),
        name="row_stats",
    )(enc, wt)


def lse_kernel(n_dev, st_ref, out_ref, recv, mine, send1, recv1, send2, recv2):
    me = lax.axis_index("tp")
    barrier = pltpu.get_barrier_semaphore()
    for d in range(1, n_dev):
        pl.semaphore_signal(barrier, inc=1, device_id={"tp": lax.rem(me + d, n_dev)}, device_id_type=MESH)
    pl.semaphore_wait(barrier, n_dev - 1)
    first = []
    for d in range(1, n_dev):
        peer = lax.rem(me + d, n_dev)
        copy = pltpu.make_async_remote_copy(
            src_ref=st_ref.at[peer], dst_ref=recv.at[me], send_sem=send1.at[d], recv_sem=recv1.at[d], device_id={"tp": peer}, device_id_type=MESH
        )
        copy.start()
        first.append(copy)
    recv[me] = st_ref[me]
    for copy in first:
        copy.wait()
    top = recv[0, 0:1, :]
    for j in range(1, n_dev):
        top = jnp.maximum(top, recv[j, 0:1, :])
    total = jnp.zeros_like(top)
    for j in range(n_dev):
        total = total + recv[j, 1:2, :] * jnp.exp(recv[j, 0:1, :] - top)
    lse = top + jnp.log(total)
    mine[...] = lse
    out_ref[me] = lse
    second = []
    for d in range(1, n_dev):
        peer = lax.rem(me + d, n_dev)
        copy = pltpu.make_async_remote_copy(
            src_ref=mine, dst_ref=out_ref.at[me], send_sem=send2.at[d], recv_sem=recv2.at[d], device_id={"tp": peer}, device_id_type=MESH
        )
        copy.start()
        second.append(copy)
    for copy in second:
        copy.wait()


def exchange_lse(stats):
    n_dev, _, rows = stats.shape
    vmem = pl.BlockSpec(memory_space=pltpu.VMEM)
    return pl.pallas_call(
        functools.partial(lse_kernel, n_dev),
        in_specs=[vmem],
        out_specs=vmem,
        out_shape=jax.ShapeDtypeStruct((n_dev, 1, rows), jnp.float32),
        scratch_shapes=[
            pltpu.VMEM((n_dev, 2, rows), jnp.float32),
            pltpu.VMEM((1, rows), jnp.float32),
            pltpu.SemaphoreType.DMA((n_dev,)),
            pltpu.SemaphoreType.DMA((n_dev,)),
            pltpu.SemaphoreType.DMA((n_dev,)),
            pltpu.SemaphoreType.DMA((n_dev,)),
        ],
        compiler_params=pltpu.CompilerParams(collective_id=0, has_side_effects=True),
        name="exchange_lse",
    )(stats)


def gather_copies(n_lab, lab_ref, seq, wt_hbm, buf, row, sem):
    out = []
    for u in range(n_lab):
        base = pl.multiple_of(lab_ref[seq * n_lab + u] & -ROWS, ROWS)
        out.append(pltpu.make_async_copy(wt_hbm.at[pl.ds(base, ROWS), :], buf.at[row, pl.ds(u * ROWS, ROWS), :], sem))
    return out


def label_kernel(n_lab, step_seqs, lab_ref, scal_ref, enc_ref, wt_hbm, out_ref, buf, z_ref, sem):
    i = pl.program_id(0)
    n = pl.num_programs(0)

    def fetch(step, slot):
        for s in range(step_seqs):
            for copy in gather_copies(n_lab, lab_ref, step * step_seqs + s, wt_hbm, buf.at[slot], s, sem.at[slot]):
                copy.start()

    @pl.when(i == 0)
    def _():
        buf[...] = jnp.zeros_like(buf)
        fetch(0, 0)

    slot = lax.rem(i, 2)

    @pl.when(i + 1 < n)
    def _():
        fetch(i + 1, 1 - slot)

    for s in range(step_seqs):
        for copy in gather_copies(n_lab, lab_ref, i * step_seqs + s, wt_hbm, buf.at[slot], s, sem.at[slot]):
            copy.wait()
    for s in range(step_seqs):
        z_ref[s] = dot(buf[slot, s], enc_ref[s], NT)
    for s in range(step_seqs):
        for u in range(n_lab):
            row = u * ROWS + (lab_ref[(i * step_seqs + s) * n_lab + u] & (ROWS - 1))
            out_ref[s, u : u + 1, :] = z_ref[s, pl.ds(row, 1), :]
        out_ref[s, n_lab:SLOTS, :] = jnp.zeros((SLOTS - n_lab, out_ref.shape[2]), jnp.float32)


def label_logits(lab_flat, scal, enc, wt_all, n_mine, n_lab):
    _, n_frames, depth = enc.shape
    step_seqs = 4
    return pl.pallas_call(
        functools.partial(label_kernel, n_lab, step_seqs),
        grid_spec=pltpu.PrefetchScalarGridSpec(
            num_scalar_prefetch=2,
            grid=(n_mine // step_seqs,),
            in_specs=[
                pl.BlockSpec((step_seqs, n_frames, depth), lambda i, lab, scal: (scal[0] * (n_mine // step_seqs) + i, 0, 0)),
                pl.BlockSpec(memory_space=pl.ANY),
            ],
            out_specs=pl.BlockSpec((step_seqs, SLOTS, n_frames), lambda i, lab, scal: (i, 0, 0)),
            scratch_shapes=[
                pltpu.VMEM((2, step_seqs, n_lab * ROWS + 8, depth), jnp.bfloat16),
                pltpu.VMEM((step_seqs, n_lab * ROWS + 8, n_frames), jnp.float32),
                pltpu.SemaphoreType.DMA((2,)),
            ],
        ),
        out_shape=jax.ShapeDtypeStruct((n_mine, SLOTS, n_frames), jnp.float32),
        compiler_params=params(),
        cost_estimate=pl.CostEstimate(flops=2 * n_mine * n_lab * ROWS * n_frames * depth, bytes_accessed=4 * n_mine * n_lab * ROWS * depth, transcendentals=0),
        name="label_logits",
    )(lab_flat, scal, enc, wt_all)


def lattice_kernel(n_lab, dup_ref, zl_ref, lse_ref, lab_ref, skip_ref, first_ref, in_ref, len_ref, gl_ref, loss_ref, bb, lb, ll, bl, sl, occ):
    n_frames = zl_ref.shape[0]
    shape = zl_ref.shape[1:]
    slot = lax.broadcasted_iota(jnp.int32, shape, 0)
    in_len = in_ref[...]
    lab_len = len_ref[...]
    skip = skip_ref[...] > 0
    neg = jnp.full(shape, NEG_FILL, jnp.float32)

    def forward(t, carry):
        b, l = carry
        e = zl_ref[t] - lse_ref[pl.ds(t, 1), :]
        eb = e[n_lab - 1 : n_lab, :]
        prev = jnp.where(slot == 0, neg, pltpu.roll(l, 1, 0))
        top_b = jnp.maximum(b, prev)
        x0 = jnp.exp(b - top_b)
        x1 = jnp.exp(prev - top_b)
        sum_b = x0 + x1
        hop = jnp.where(skip, prev, neg)
        top_l = jnp.maximum(jnp.maximum(l, b), hop)
        y0 = jnp.exp(l - top_l)
        y1 = jnp.exp(b - top_l)
        y2 = jnp.exp(hop - top_l)
        sum_l = y0 + y1 + y2
        inv_b = 1.0 / sum_b
        inv_l = 1.0 / sum_l
        bb[t] = x0 * inv_b
        lb[t] = x1 * inv_b
        ll[t] = y0 * inv_l
        bl[t] = y1 * inv_l
        sl[t] = y2 * inv_l
        live = t < in_len
        new_b = jnp.where(live, top_b + jnp.log(sum_b) + eb, b)
        new_l = jnp.where(live, top_l + jnp.log(sum_l) + e, l)
        return new_b, new_l

    b, l = lax.fori_loop(0, n_frames, forward, (jnp.where(slot == 0, 0.0, neg), neg))
    end_b = jnp.where(slot == lab_len, b, neg)
    end_l = jnp.where(slot == lab_len - 1, l, neg)
    top = jnp.max(jnp.maximum(end_b, end_l), axis=0, keepdims=True)
    total = jnp.sum(jnp.exp(end_b - top) + jnp.exp(end_l - top), axis=0, keepdims=True)
    log_like = top + jnp.log(total)
    loss_ref[...] = -log_like

    def backward(i, carry):
        t = n_frames - 1 - i
        gb, gl = carry
        live = t < in_len
        blank = jnp.sum(gb, axis=0, keepdims=True)
        occ[t] = jnp.where(live, jnp.where(slot < n_lab - 1, gl, jnp.where(slot == n_lab - 1, blank, 0.0)), 0.0)
        back = pltpu.roll(gb * lb[t] + gl * sl[t], shape[0] - 1, 0)
        new_b = gb * bb[t] + gl * bl[t]
        new_l = gl * ll[t] + back
        return jnp.where(live, new_b, gb), jnp.where(live, new_l, gl)

    lax.fori_loop(0, n_frames, backward, (jnp.exp(end_b - log_like), jnp.exp(end_l - log_like)))

    lab = lab_ref[...]
    first = first_ref[...] > 0
    for v in range(1, n_lab - 1):

        @pl.when(dup_ref[v] > 0)
        def _():
            other = lab_ref[v : v + 1, :]
            take = (lab == other) & first & (first_ref[v : v + 1, :] <= 0) & (slot < n_lab - 1)

            def add(t, _):
                row = occ[t]
                occ[t] = row + jnp.where(take, row[v : v + 1, :], 0.0)
                return 0

            lax.fori_loop(0, n_frames, add, 0)

    def emit(t, _):
        p = jnp.exp(zl_ref[t] - lse_ref[pl.ds(t, 1), :])
        gl_ref[t] = jnp.where(first & (t < in_len), p - occ[t], 0.0).astype(gl_ref.dtype)
        return 0

    lax.fori_loop(0, n_frames, emit, 0)


def lattice(dup, zl, lse, lab, skip, first, in_len, lab_len, n_lab):
    n_frames, slots, lanes = zl.shape
    vmem = pl.BlockSpec(memory_space=pltpu.VMEM)
    return pl.pallas_call(
        functools.partial(lattice_kernel, n_lab + 1),
        in_specs=[pl.BlockSpec(memory_space=pltpu.SMEM)] + [vmem] * 7,
        out_specs=(vmem, vmem),
        out_shape=(jax.ShapeDtypeStruct((n_frames, slots, lanes), jnp.bfloat16), jax.ShapeDtypeStruct((1, lanes), jnp.float32)),
        scratch_shapes=[pltpu.VMEM((n_frames, slots, lanes), jnp.float32)] * 6,
        compiler_params=params(),
        cost_estimate=pl.CostEstimate(flops=2 * 10**10, bytes_accessed=2 * zl.size, transcendentals=0),
        name="lattice",
    )(dup, zl, lse, lab, skip, first, in_len, lab_len)


def place_start(recvs, out_ref, rows_ref, base, sem):
    step = pl.program_id(0)
    copies = []
    for i, ref in enumerate(recvs):
        n = ref.shape[0]
        row = pl.multiple_of(rows_ref[base + i] + step * n, 8)
        copy = pltpu.make_async_copy(ref, out_ref.at[pl.ds(row, n), :], sem.at[i])
        copy.start()
        copies.append(copy)
    return copies


def hs_kernel(n_lab, n_recv, has_prev, k, lab_ref, scal_ref, enc_ref, wt_ref, wt_hbm, lse_ref, keep_ref, gl_ref, rem_ref, *refs):
    recvs = refs[:n_recv]
    refs = refs[n_recv + has_prev :]
    out_ref, sy_ref, sz_ref, buf, shift, sem_g, sem_r, sem_o = refs
    j = pl.program_id(0)
    n = pl.num_programs(0)
    n_seq, n_frames, depth = enc_ref.shape
    half = n_seq // 2

    def gathers():
        return [c for s in range(n_seq) for c in gather_copies(n_lab, lab_ref, k * n_seq + s, wt_hbm, buf, s, sem_g)]

    placed = place_start(recvs, out_ref, scal_ref, 2, sem_r)

    @pl.when(j == 0)
    def _():
        buf[:, n_lab * ROWS :, :] = jnp.zeros((n_seq, buf.shape[1] - n_lab * ROWS, depth), buf.dtype)
        for copy in gathers():
            copy.start()
        cols = jnp.transpose(lse_ref[...])
        for s in range(n_seq):
            shift[s] = jnp.broadcast_to(cols[:n_frames, s : s + 1], (n_frames, 128))
        sy_ref[...] = jnp.zeros_like(sy_ref)
        sz_ref[...] = jnp.zeros_like(sz_ref)

    w = wt_ref[...]
    width = w.shape[0]
    for part, acc in ((0, sy_ref), (1, sz_ref)):
        enc = enc_ref[part * half : (part + 1) * half].reshape(half * n_frames, depth)
        z = dot(enc, w, NT)
        ps = []
        for s in range(half):
            seq = part * half + s
            keep = keep_ref[seq : seq + 1, :] > 0
            low = jnp.concatenate([shift[seq]] * (width // 128), axis=1)
            p = jnp.exp(z[s * n_frames : (s + 1) * n_frames, :] - low)
            ps.append(jnp.where(keep, p, 0.0).astype(jnp.bfloat16))
        p = jnp.concatenate(ps, axis=0)
        acc[...] += dot(p, w, NN)

    @pl.when(j == n - 1)
    def _():
        for copy in gathers():
            copy.wait()
        span = buf.shape[1]
        lane = lax.broadcasted_iota(jnp.int32, (SLOTS, span), 1)
        slot = lax.broadcasted_iota(jnp.int32, (SLOTS, span), 0)
        for part, acc in ((0, sy_ref), (1, sz_ref)):
            for s in range(half):
                seq = part * half + s
                spread = ((lane == slot * ROWS + rem_ref[seq]) & (slot < n_lab)).astype(jnp.bfloat16)
                wide = dot(gl_ref[seq], spread, NN).astype(jnp.bfloat16)
                acc[s * n_frames : (s + 1) * n_frames, :] += dot(wide, buf[seq], NN)
        rows = half * n_frames
        done = []
        for part, acc in ((0, sy_ref), (1, sz_ref)):
            row = pl.multiple_of(scal_ref[1] + (k * n_seq + part * half) * n_frames, 8)
            copy = pltpu.make_async_copy(acc, out_ref.at[pl.ds(row, rows), :], sem_o.at[part])
            copy.start()
            done.append(copy)
        for copy in done:
            copy.wait()

    for copy in placed:
        copy.wait()


def hs_chunk(k, n_mine, n_lab, lab_flat, scal, enc, wt_all, lse, keep, gl, rem, recvs, prev):
    _, n_frames, depth = enc.shape
    n_vocab = wt_all.shape[0]
    n_batch = enc.shape[0]
    width = 512 if n_vocab % 512 == 0 and n_vocab >= 8192 else 128
    steps = n_vocab // width
    n_chunk = n_mine // CHUNK
    half_rows = CHUNK // 2 * n_frames
    any_spec = pl.BlockSpec(memory_space=pl.ANY)
    in_specs = [
        pl.BlockSpec((CHUNK, n_frames, depth), lambda j, lab, scal: (scal[0] * n_chunk + k, 0, 0)),
        pl.BlockSpec((width, depth), lambda j, lab, scal: (j, 0)),
        any_spec,
        pl.BlockSpec((CHUNK, 128), lambda j, lab, scal: (scal[0] * n_chunk + k, 0)),
        pl.BlockSpec((CHUNK, width), lambda j, lab, scal: (k, j)),
        pl.BlockSpec((CHUNK, n_frames, SLOTS), lambda j, lab, scal: (k, 0, 0)),
        pl.BlockSpec((CHUNK, SLOTS, 1), lambda j, lab, scal: (k, 0, 0)),
    ]
    for r in recvs:
        in_specs.append(pl.BlockSpec((r.shape[0] // steps, depth), lambda j, lab, scal: (j, 0)))
    args = [lab_flat, scal, enc, wt_all, wt_all, lse, keep, gl, rem, *recvs]
    aliases = {}
    if prev is not None:
        in_specs.append(any_spec)
        aliases = {len(args): 0}
        args.append(prev)
    send = jax.ShapeDtypeStruct((half_rows, depth), jnp.float32)
    rows = CHUNK * n_frames
    return pl.pallas_call(
        functools.partial(hs_kernel, n_lab, len(recvs), int(prev is not None), k),
        grid_spec=pltpu.PrefetchScalarGridSpec(
            num_scalar_prefetch=2,
            grid=(steps,),
            in_specs=in_specs,
            out_specs=(any_spec, pl.BlockSpec((half_rows, depth), lambda j, lab, scal: (0, 0)), pl.BlockSpec((half_rows, depth), lambda j, lab, scal: (0, 0))),
            scratch_shapes=[
                pltpu.VMEM((CHUNK, n_lab * ROWS + 8, depth), jnp.bfloat16),
                pltpu.VMEM((CHUNK, n_frames, 128), jnp.float32),
                pltpu.SemaphoreType.DMA,
                pltpu.SemaphoreType.DMA((max(len(recvs), 1),)),
                pltpu.SemaphoreType.DMA((2,)),
            ],
        ),
        out_shape=(jax.ShapeDtypeStruct((n_batch * n_frames, depth), jnp.float32), send, send),
        input_output_aliases=aliases,
        compiler_params=params(),
        cost_estimate=pl.CostEstimate(flops=4 * rows * depth * n_vocab, bytes_accessed=2 * n_vocab * depth, transcendentals=rows * n_vocab),
        name="hs_chunk",
    )(*args)


def gw_kernel(n_recv, is_first, is_last, scal_ref, enc_ref, wt_ref, lse_ref, lab_ref, gl_ref, *refs):
    recvs = refs[:n_recv]
    acc_in = None if is_first else refs[n_recv]
    refs = refs[n_recv + (not is_first) + 1 :]
    out_ref, gw_ref, acc, bias, fan, diag, sem_r = refs
    i = pl.program_id(0)
    n = pl.num_programs(0)
    n_seq, n_frames, depth = enc_ref.shape
    n_cols = wt_ref.shape[0]
    rows = n_seq * n_frames
    placed = place_start(recvs, out_ref, scal_ref, 2, sem_r)

    @pl.when(i == 0)
    def _():
        seq_r = lax.broadcasted_iota(jnp.int32, (n_seq * SLOTS, rows), 0) // SLOTS
        seq_c = lax.broadcasted_iota(jnp.int32, (n_seq * SLOTS, rows), 1) // n_frames
        same = seq_r == seq_c
        bias[...] = jnp.where(same, NEG_FILL, 0.0).astype(jnp.bfloat16)
        diag[...] = jnp.where(same, 1.0, 0.0)
        t_r = lax.broadcasted_iota(jnp.int32, (n_frames, rows), 0)
        t_c = lax.rem(lax.broadcasted_iota(jnp.int32, (n_frames, rows), 1), n_frames)
        fan[...] = (t_r == t_c).astype(jnp.bfloat16)
        if is_first:
            acc[...] = jnp.zeros_like(acc)
        else:
            acc[...] = acc_in[...]

    enc = enc_ref[...].reshape(rows, depth)
    col = scal_ref[0] + lax.broadcasted_iota(jnp.int32, (n_cols, n_seq * SLOTS), 0)
    hot = (col == lab_ref[0]).astype(jnp.bfloat16)
    z = dot(wt_ref[...], enc, NT) + dot(hot, bias[...], NN)
    p = jnp.exp(z - lse_ref[0])
    wide = (dot(gl_ref[...].reshape(n_seq * SLOTS, n_frames), fan[...], NN) * diag[...]).astype(jnp.bfloat16)
    g = p.astype(jnp.bfloat16) + dot(hot, wide, NN).astype(jnp.bfloat16)
    acc[...] += dot(g, enc, NN)

    @pl.when(i == n - 1)
    def _():
        if is_last:
            gw_ref[...] = jnp.transpose(acc[...])
        else:
            gw_ref[...] = acc[...]

    for copy in placed:
        copy.wait()


def gw_part(part, n_part, scal, enc, wt, lse_rows, lab_rows, gl, recvs, acc, prev):
    n_batch, n_frames, depth = enc.shape
    n_cols = wt.shape[0]
    steps = n_batch // CHUNK // n_part
    base = part * steps
    rows = CHUNK * n_frames
    is_first, is_last = part == 0, part == n_part - 1
    any_spec = pl.BlockSpec(memory_space=pl.ANY)
    in_specs = [
        pl.BlockSpec((CHUNK, n_frames, depth), lambda i, scal: (base + i, 0, 0)),
        pl.BlockSpec((n_cols, depth), lambda i, scal: (0, 0)),
        pl.BlockSpec((1, 1, rows), lambda i, scal: (base + i, 0, 0)),
        pl.BlockSpec((1, 1, CHUNK * SLOTS), lambda i, scal: (base + i, 0, 0)),
        pl.BlockSpec((CHUNK, SLOTS, n_frames), lambda i, scal: (base + i, 0, 0)),
    ]
    for r in recvs:
        in_specs.append(pl.BlockSpec((r.shape[0] // steps, depth), lambda i, scal: (i, 0)))
    args = [scal, enc, wt, lse_rows, lab_rows, gl, *recvs]
    if not is_first:
        in_specs.append(pl.BlockSpec((n_cols, depth), lambda i, scal: (0, 0)))
        args.append(acc)
    in_specs.append(any_spec)
    aliases = {len(args): 0}
    args.append(prev)
    shape = (depth, n_cols) if is_last else (n_cols, depth)
    return pl.pallas_call(
        functools.partial(gw_kernel, len(recvs), is_first, is_last),
        grid_spec=pltpu.PrefetchScalarGridSpec(
            num_scalar_prefetch=1,
            grid=(steps,),
            in_specs=in_specs,
            out_specs=(any_spec, pl.BlockSpec(shape, lambda i, scal: (0, 0))),
            scratch_shapes=[
                pltpu.VMEM((n_cols, depth), jnp.float32),
                pltpu.VMEM((CHUNK * SLOTS, rows), jnp.bfloat16),
                pltpu.VMEM((n_frames, rows), jnp.bfloat16),
                pltpu.VMEM((CHUNK * SLOTS, rows), jnp.float32),
                pltpu.SemaphoreType.DMA((max(len(recvs), 1),)),
            ],
        ),
        out_shape=(jax.ShapeDtypeStruct(prev.shape, jnp.float32), jax.ShapeDtypeStruct(shape, jnp.float32)),
        input_output_aliases=aliases,
        compiler_params=params(),
        cost_estimate=pl.CostEstimate(flops=4 * steps * rows * depth * n_cols, bytes_accessed=2 * steps * rows * depth, transcendentals=steps * rows * n_cols),
        name="gw_part",
    )(*args)


def place_kernel(n_recv, scal_ref, *refs):
    copies = place_start(refs[:n_recv], refs[n_recv + 1], scal_ref, 2, refs[n_recv + 2])
    for copy in copies:
        copy.wait()


def place(scal, recvs, prev):
    depth = prev.shape[1]
    steps = 4
    any_spec = pl.BlockSpec(memory_space=pl.ANY)
    in_specs = [pl.BlockSpec((r.shape[0] // steps, depth), lambda i, scal: (i, 0)) for r in recvs] + [any_spec]
    return pl.pallas_call(
        functools.partial(place_kernel, len(recvs)),
        grid_spec=pltpu.PrefetchScalarGridSpec(
            num_scalar_prefetch=1, grid=(steps,), in_specs=in_specs, out_specs=any_spec, scratch_shapes=[pltpu.SemaphoreType.DMA((len(recvs),))]
        ),
        out_shape=jax.ShapeDtypeStruct(prev.shape, jnp.float32),
        input_output_aliases={1 + len(recvs): 0},
        compiler_params=params(),
        name="place",
    )(scal, *recvs, prev)


def solution(mesh):
    n_dev = mesh.shape["tp"]

    def swap(x, bit):
        return lax.ppermute(x, "tp", [(i, i ^ bit) for i in range(n_dev)])

    def device_fn(enc, w_loc, labels, in_len, lab_len):
        n_batch, n_frames, depth = enc.shape
        n_cols = w_loc.shape[1]
        n_lab = labels.shape[1]
        n_mine = n_batch // 4
        n_chunk = n_mine // CHUNK
        tp = lax.axis_index("tp")
        core = tp % 2
        colour = (tp // 2 + tp // 4) % 2
        mine = 2 * colour + core

        wt = w_loc.T
        wt_all = lax.all_gather(wt, "tp", axis=0, tiled=True)
        lse = exchange_lse(row_stats(enc, wt, n_dev)).reshape(n_batch, n_frames)
        frame = jnp.arange(n_frames)
        lse_live = jnp.where(frame[None, :] < in_len[:, None], lse, BIG)
        lse_pad = jnp.pad(lse_live, ((0, 0), (0, 128 - n_frames)), constant_values=BIG)

        u = jnp.arange(n_lab)
        valid = u[None, :] < lab_len[:, None]
        earlier = (labels[:, :, None] == labels[:, None, :]) & (u[None, :] < u[:, None])[None]
        first = valid & ~jnp.any(earlier, axis=2)
        slot_lab = jnp.concatenate(
            [jnp.where(first, labels, -1), jnp.zeros((n_batch, 1), jnp.int32), jnp.full((n_batch, SLOTS - n_lab - 1), -1, jnp.int32)], axis=1
        )

        def take(x):
            return lax.dynamic_slice_in_dim(x, mine * n_mine, n_mine, axis=0)

        lab_m = take(labels)
        slot_m = take(slot_lab)
        first_m = take(first)
        ext_m = jnp.concatenate([lab_m, jnp.zeros((n_mine, 1), jnp.int32)], axis=1)
        lab_flat = ext_m.reshape(-1)
        vocab = jnp.arange(n_dev * n_cols)
        keep = jnp.where(jnp.any(slot_m[:, :, None] == vocab[None, None, :], axis=1), 0.0, 1.0)
        rem = jnp.pad(ext_m % ROWS, ((0, 0), (0, SLOTS - n_lab - 1)))[:, :, None]

        def lanes(x, fill):
            return jnp.pad(x, ((0, 0),) * (x.ndim - 1) + ((0, 128 - n_mine),), constant_values=fill)

        scal_z = jnp.stack([mine, mine]).astype(jnp.int32)
        zl = label_logits(lab_flat, scal_z, enc, wt_all, n_mine, n_lab + 1)
        zl_t = lanes(jnp.transpose(zl, (2, 1, 0)), 0.0)
        lse_t = lanes(take(lse).T, 0.0)
        lab_t = jnp.pad(lanes(lab_m.T, -1), ((0, SLOTS - n_lab), (0, 0)), constant_values=-1)
        skip = jnp.pad(lab_m[:, 1:] != lab_m[:, :-1], ((0, 0), (1, 0)))
        skip_t = jnp.pad(lanes(skip.T.astype(jnp.int32), 0), ((0, SLOTS - n_lab), (0, 0)))
        first_t = jnp.pad(lanes(first_m.T.astype(jnp.int32), 0), ((0, SLOTS - n_lab), (0, 0)))
        first_t = jnp.where(jnp.arange(SLOTS)[:, None] == n_lab, 1, first_t)
        dup = jnp.pad(jnp.any(take(valid) & ~first_m, axis=0).astype(jnp.int32), (0, SLOTS - n_lab))
        gl_t, loss_m = lattice(dup, zl_t, lse_t, lab_t, skip_t, first_t, lanes(take(in_len)[None, :], 0), lanes(take(lab_len)[None, :], 4), n_lab)
        gl_t = gl_t[:, :, :n_mine]
        loss_m = loss_m[0, :n_mine]
        gl_hs = jnp.transpose(gl_t, (2, 0, 1))
        gl_gw = jnp.transpose(gl_t, (2, 1, 0))

        def spread(x):
            other = swap(x, 2)
            partner = swap(x, 1)
            last = swap(other, 1)
            out = jnp.zeros((4,) + x.shape, x.dtype)
            for value, where in ((x, mine), (other, mine ^ 2), (partner, mine ^ 1), (last, mine ^ 3)):
                out = lax.dynamic_update_index_in_dim(out, value, where, 0)
            return out.reshape((4 * x.shape[0],) + x.shape[1:])

        loss = spread(loss_m)
        gl_all = spread(gl_gw)

        set_rows = n_mine * n_frames
        half = CHUNK // 2 * n_frames
        moved = {}

        def rows_of(kinds):
            return [((mine ^ flip) * set_rows + k * CHUNK * n_frames + part * half) for k, part, flip in kinds]

        def scal_of(head, kinds):
            vals = list(head) + rows_of(kinds)
            vals += [0] * (8 - len(vals))
            return jnp.stack([jnp.asarray(v, jnp.int32) for v in vals])

        def arrived(k_direct, k_forward):
            kinds, data = [], []
            for k, flips in ((k_direct, (2, 1)), (k_forward, (3,))):
                if 0 <= k < n_chunk:
                    for flip in flips:
                        for part in (0, 1):
                            kinds.append((k, part, flip))
                            data.append(moved[(k, part, flip)])
            return kinds, data

        out = None
        for k in range(n_chunk):
            kinds, data = arrived(k - 2, k - 3)
            scal = scal_of((mine, mine * set_rows), kinds)
            out, sy, sz = hs_chunk(k, n_mine, n_lab + 1, lab_flat, scal, enc, wt_all, lse_pad, keep, gl_hs, rem, data, out)
            for part, x, bit in ((0, sy, 2), (1, sz, 4)):
                moved[(k, part, 2)] = swap(x, bit)
                moved[(k, part, 1)] = swap(x, 1)
                moved[(k, part, 3)] = swap(moved[(k, part, 2)], 1)

        lse_rows = lse_live.reshape(n_batch // CHUNK, 1, CHUNK * n_frames)
        lab_rows = slot_lab.reshape(n_batch // CHUNK, 1, CHUNK * SLOTS)
        acc = None
        for part in range(2):
            kinds, data = arrived(n_chunk + part - 2, n_chunk + part - 3)
            scal = scal_of((tp * n_cols, 0), kinds)
            out, acc = gw_part(part, 2, scal, enc, wt, lse_rows, lab_rows, gl_all, data, acc, out)
        kinds, data = arrived(-1, n_chunk - 1)
        out = place(scal_of((0, 0), kinds), data, out)
        return loss, acc, out.reshape(n_batch, n_frames, depth)

    return jax.shard_map(
        device_fn,
        mesh=mesh,
        in_specs=(P("dp"), P(None, "tp"), P("dp"), P("dp"), P("dp")),
        out_specs=(P("dp"), P("dp", "tp"), P("dp")),
        check_vma=False,
    )
```

```python
import functools

import jax
import jax.numpy as jnp
from jax import lax
from jax.experimental import pallas as pl
from jax.experimental.pallas import tpu as pltpu
from jax.sharding import PartitionSpec as P


NEG_FILL = -1.0e30
BIG = 1.0e30
MESH = pl.DeviceIdType.MESH
NT = (((1,), (1,)), ((), ()))
NN = (((1,), (0,)), ((), ()))
TN = (((0,), (0,)), ((), ()))
SLOTS = 32
ROWS = 8
HS_WIDTH = 1024
CHUNK = 8
VMEM_LIMIT = 60 * 1024 * 1024


def dot(a, b, dims):
    return lax.dot_general(a, b, dims, preferred_element_type=jnp.float32)


def params(**kw):
    return pltpu.CompilerParams(vmem_limit_bytes=VMEM_LIMIT, **kw)


SUBS = 4
N_Z = 4
HOPS = SUBS * (N_Z - 1)
IDS = SUBS + 2 * HOPS


def spread_kernel(n_dev, n_dp, enc_hbm, w_ref, all_ref, lse_ref, *scratch):
    encbuf, st, recv, mine, enc_sem, own_sem, dn_send, dn_recv, up_send, up_recv, y_send, y_recv, x_send, x_recv, c_send, c_recv = scratch[:16]
    s1_send, s1_recv, s2_send, s2_recv = scratch[16:]
    dp = lax.axis_index("dp")
    tp = lax.axis_index("tp")
    core = lax.rem(tp, 2)
    z = lax.div(tp, 4)
    mate = tp + 1 - 2 * core
    across = tp + 2 - 4 * lax.rem(lax.div(tp, 2), 2)
    block = w_ref.shape[0]
    piece = block // SUBS
    crosses = (core == dp) if n_dp > 1 else (core >= 0)
    n_seq, n_frames, depth = encbuf.shape[1:]

    def rows(owner, s):
        return all_ref.at[pl.ds(pl.multiple_of(owner * block + s * piece, piece), piece), :]

    def move(src, owner, s, send, got, dst):
        return pltpu.make_async_remote_copy(src_ref=src, dst_ref=rows(owner, s), send_sem=send, recv_sem=got, device_id=dst, device_id_type=MESH)

    def to(dev):
        return {"tp": dev}

    def owner_of(base, kind, q):
        hop = lax.div(q, SUBS) + 1
        return base + (4 * hop if kind == 1 else -4 * hop)

    def there(kind, q):
        hop = lax.div(q, SUBS) + 1
        return (q >= 0) & (q < HOPS) & ((z + hop <= N_Z - 1) if kind == 1 else (z - hop >= 0))

    barrier = pltpu.get_barrier_semaphore()
    for d in range(1, n_dev):
        pl.semaphore_signal(barrier, inc=1, device_id={"tp": lax.rem(tp + d, n_dev)}, device_id_type=MESH)
    if n_dp > 1:
        pl.semaphore_signal(barrier, inc=1, device_id={"dp": 1 - dp}, device_id_type=MESH)
    pl.semaphore_wait(barrier, n_dev - 1 + (n_dp > 1))

    own = pltpu.make_async_copy(w_ref, all_ref.at[pl.ds(pl.multiple_of(tp * block, block), block), :], own_sem)
    own.start()

    def own_moves(s):
        src = w_ref.at[pl.ds(pl.multiple_of(s * piece, piece), piece), :]
        return (
            (z >= 1, move(src, tp, s, dn_send.at[s], dn_recv.at[s], to(tp - 4))),
            (z <= N_Z - 2, move(src, tp, s, up_send.at[s], up_recv.at[s], to(tp + 4))),
            (crosses, move(src, tp, s, y_send.at[s], y_recv.at[s], to(across))),
            (z >= 0, move(src, tp, s, c_send.at[s], c_recv.at[s], to(mate))),
        )

    def z_moves(kind, q):
        owner = owner_of(tp, kind, q)
        s = lax.rem(q, SUBS)
        src = rows(owner, s)
        got = dn_recv if kind == 1 else up_recv
        send = dn_send if kind == 1 else up_send
        number = SUBS + q + (0 if kind == 1 else HOPS)
        last = (z >= 1) if kind == 1 else (z <= N_Z - 2)
        nxt = lax.rem(q + SUBS, HOPS)
        here = there(kind, q)
        return (
            here,
            move(src, owner, s, send.at[SUBS + q], got.at[q], to(tp)),
            (
                (here & last, move(src, owner, s, send.at[SUBS + q], got.at[nxt], to(tp - 4 if kind == 1 else tp + 4))),
                (here, move(src, owner, s, c_send.at[number], c_recv.at[number], to(mate))),
                (here & crosses, move(src, owner, s, y_send.at[number], y_recv.at[number], to(across))),
            ),
        )

    def far_parts(kind, q):
        if kind == 0:
            q0 = lax.rem(q + SUBS, SUBS)
            return across, q0, q0, (q >= 0) & (q < SUBS)
        q0 = lax.rem(q + HOPS, HOPS)
        return owner_of(across, kind, q0), lax.rem(q0, SUBS), SUBS + q0 + (0 if kind == 1 else HOPS), there(kind, q)

    def y_moves(kind, q):
        owner, s, number, here = far_parts(kind, q)
        src = rows(owner, s)
        return (
            here & crosses,
            move(src, owner, s, y_send.at[number], y_recv.at[number], to(tp)),
            (
                (here & crosses & (n_dp > 1), move(src, owner, s, x_send.at[number], x_recv.at[number], {"dp": 1 - dp if n_dp > 1 else dp})),
                (here & crosses, move(src, owner, s, c_send.at[IDS + number], c_recv.at[IDS + number], to(mate))),
            ),
        )

    def x_moves(kind, q):
        owner, s, number, here = far_parts(kind, q)
        src = rows(owner, s)
        return (
            here & jnp.logical_not(crosses),
            move(src, owner, s, x_send.at[number], x_recv.at[number], to(tp)),
            ((here & jnp.logical_not(crosses), move(src, owner, s, c_send.at[IDS + number], c_recv.at[IDS + number], to(mate))),),
        )

    def start_all(moves):
        for cond, copy in moves:

            @pl.when(cond)
            def _():
                copy.start()

    def relay(group):
        cond, arrival, moves = group

        @pl.when(cond)
        def _():
            arrival.wait_recv()

        start_all(moves)

    def service(q):
        for kind in (1, 2):
            relay(z_moves(kind, q))
        relay(y_moves(0, jnp.minimum(q, SUBS)))
        for kind in (1, 2):
            relay(y_moves(kind, q - 1))
        if n_dp > 1:
            relay(x_moves(0, jnp.minimum(q - 1, SUBS)))
            for kind in (1, 2):
                relay(x_moves(kind, q - 2))

    def enc_copy(i):
        slot = lax.rem(i, 2)
        return pltpu.make_async_copy(enc_hbm.at[pl.ds(i * n_seq, n_seq)], encbuf.at[slot], enc_sem.at[slot])

    enc_copy(0).start()
    for s in range(SUBS):
        start_all(own_moves(s))

    per = n_dev // SUBS

    def tile(i, carry):
        enc_copy(i).wait()

        @pl.when(i + 1 < n_dev)
        def _():
            enc_copy(i + 1).start()

        enc = encbuf[lax.rem(i, 2)].reshape(n_seq * n_frames, depth)
        zt = dot(w_ref[...], enc, NT)
        top = jnp.max(zt, axis=0, keepdims=True)
        st[i, 0:1, :] = top
        st[i, 1:2, :] = jnp.sum(jnp.exp(zt - top), axis=0, keepdims=True)
        return carry

    def with_tiles(q, carry):
        lax.fori_loop(q * per, (q + 1) * per, tile, 0)
        service(q)
        return carry

    def plain(q, carry):
        service(q)
        return carry

    lax.fori_loop(0, SUBS, with_tiles, 0)
    first = []
    for d in range(1, n_dev):
        peer = lax.rem(tp + d, n_dev)
        first.append(
            pltpu.make_async_remote_copy(
                src_ref=st.at[peer], dst_ref=recv.at[tp], send_sem=s1_send.at[d], recv_sem=s1_recv.at[d], device_id=to(peer), device_id_type=MESH
            )
        )
    for copy in first:
        copy.start()
    recv[tp] = st[tp]
    lax.fori_loop(SUBS, SUBS + 2, plain, 0)
    for copy in first:
        copy.wait()
    top = recv[0, 0:1, :]
    for j in range(1, n_dev):
        top = jnp.maximum(top, recv[j, 0:1, :])
    total = jnp.zeros_like(top)
    for j in range(n_dev):
        total = total + recv[j, 1:2, :] * jnp.exp(recv[j, 0:1, :] - top)
    lse = top + jnp.log(total)
    mine[...] = lse
    lse_ref[tp] = lse
    lax.fori_loop(SUBS + 2, SUBS + 3, plain, 0)
    second = []
    for d in range(1, n_dev):
        peer = lax.rem(tp + d, n_dev)
        second.append(
            pltpu.make_async_remote_copy(
                src_ref=mine, dst_ref=lse_ref.at[tp], send_sem=s2_send.at[d], recv_sem=s2_recv.at[d], device_id=to(peer), device_id_type=MESH
            )
        )
    for copy in second:
        copy.start()
    lax.fori_loop(SUBS + 3, HOPS, plain, 0)

    for kind in (1, 2):
        relay(y_moves(kind, HOPS - 1))
    if n_dp > 1:
        for q in (HOPS - 2, HOPS - 1):
            for kind in (1, 2):
                relay(x_moves(kind, q))
    for copy in second:
        copy.wait()
    own.wait()

    def drain(cond, copy):
        @pl.when(cond)
        def _():
            copy.wait_send()

    def finish_own(s, carry):
        for cond, copy in own_moves(s):
            drain(cond, copy)
        move(rows(mate, s), mate, s, c_send.at[s], c_recv.at[s], to(tp)).wait_recv()
        far = mate + across - tp
        move(rows(far, s), far, s, c_send.at[IDS + s], c_recv.at[IDS + s], to(tp)).wait_recv()
        for moves in (y_moves(0, s), x_moves(0, s)) if n_dp > 1 else (y_moves(0, s),):
            for cond, copy in moves[2]:
                drain(cond, copy)
        return carry

    def finish(q, carry):
        for kind in (1, 2):
            here, _, moves = z_moves(kind, q)
            for cond, copy in moves:
                drain(cond, copy)
            for group in (y_moves(kind, q), x_moves(kind, q)) if n_dp > 1 else (y_moves(kind, q),):
                for cond, copy in group[2]:
                    drain(cond, copy)
            number = SUBS + q + (0 if kind == 1 else HOPS)
            s = lax.rem(q, SUBS)

            @pl.when(here)
            def _():
                near = owner_of(mate, kind, q)
                move(rows(near, s), near, s, c_send.at[number], c_recv.at[number], to(tp)).wait_recv()
                far = owner_of(mate + across - tp, kind, q)
                move(rows(far, s), far, s, c_send.at[IDS + number], c_recv.at[IDS + number], to(tp)).wait_recv()

        return carry

    lax.fori_loop(0, SUBS, finish_own, 0)
    lax.fori_loop(0, HOPS, finish, 0)


def spread_projection(enc, wt, n_dev, n_dp):
    n_batch, n_frames, depth = enc.shape
    n_cols = wt.shape[0]
    n_seq = n_batch // n_dev
    rows = n_seq * n_frames
    vmem = pl.BlockSpec(memory_space=pltpu.VMEM)
    any_spec = pl.BlockSpec(memory_space=pl.ANY)
    dma = pltpu.SemaphoreType.DMA
    return pl.pallas_call(
        functools.partial(spread_kernel, n_dev, n_dp),
        in_specs=[any_spec, vmem],
        out_specs=(any_spec, vmem),
        out_shape=(jax.ShapeDtypeStruct((n_dev * n_cols, depth), wt.dtype), jax.ShapeDtypeStruct((n_dev, 1, rows), jnp.float32)),
        scratch_shapes=[
            pltpu.VMEM((2, n_seq, n_frames, depth), enc.dtype),
            pltpu.VMEM((n_dev, 2, rows), jnp.float32),
            pltpu.VMEM((n_dev, 2, rows), jnp.float32),
            pltpu.VMEM((1, rows), jnp.float32),
            dma((2,)),
            dma,
            dma((SUBS + HOPS,)),
            dma((HOPS,)),
            dma((SUBS + HOPS,)),
            dma((HOPS,)),
            dma((IDS,)),
            dma((IDS,)),
            dma((IDS,)),
            dma((IDS,)),
            dma((2 * IDS,)),
            dma((2 * IDS,)),
            dma((n_dev,)),
            dma((n_dev,)),
            dma((n_dev,)),
            dma((n_dev,)),
        ],
        compiler_params=params(collective_id=0, has_side_effects=True),
        cost_estimate=pl.CostEstimate(flops=2 * n_batch * n_frames * depth * n_cols, bytes_accessed=2 * enc.size, transcendentals=0),
        name="spread_projection",
    )(enc, wt)


def label_kernel(n_lab, step_seqs, lab_ref, scal_ref, enc_ref, rem_ref, wt_hbm, out_ref, rows_ref, buf, sem):
    i = pl.program_id(0)
    n = pl.num_programs(0)
    span = buf.shape[2]

    def fetch(step, slot):
        for s in range(step_seqs):
            for u in range(n_lab):
                base = pl.multiple_of(lab_ref[(step * step_seqs + s) * n_lab + u] & -ROWS, ROWS)
                pltpu.make_async_copy(wt_hbm.at[pl.ds(base, ROWS), :], buf.at[slot, s, pl.ds(u * ROWS, ROWS), :], sem.at[slot, s]).start()

    @pl.when(i == 0)
    def _():
        buf[:, :, n_lab * ROWS :, :] = jnp.zeros((2, step_seqs, span - n_lab * ROWS, buf.shape[3]), buf.dtype)
        fetch(0, 0)

    slot = lax.rem(i, 2)

    @pl.when(i + 1 < n)
    def _():
        fetch(i + 1, 1 - slot)

    lane = lax.broadcasted_iota(jnp.int32, (SLOTS, span), 1)
    row = lax.broadcasted_iota(jnp.int32, (SLOTS, span), 0)
    for s in range(step_seqs):
        whole = pl.ds(0, n_lab * ROWS)
        pltpu.make_async_copy(wt_hbm.at[whole, :], buf.at[slot, s, whole, :], sem.at[slot, s]).wait()
    for s in range(step_seqs):
        pick = ((lane == row * ROWS + rem_ref[s]) & (row < n_lab)).astype(jnp.bfloat16)
        rows_ref[s] = dot(pick, buf[slot, s], NN).astype(rows_ref.dtype)
    for s in range(step_seqs):
        out_ref[s] = dot(rows_ref[s], enc_ref[s], NT)


def label_logits(lab_flat, scal, enc, rem, wt_all, n_mine, n_lab):
    _, n_frames, depth = enc.shape
    step_seqs = 4
    span = (n_lab * ROWS + 15) // 16 * 16
    return pl.pallas_call(
        functools.partial(label_kernel, n_lab, step_seqs),
        grid_spec=pltpu.PrefetchScalarGridSpec(
            num_scalar_prefetch=2,
            grid=(n_mine // step_seqs,),
            in_specs=[
                pl.BlockSpec((step_seqs, n_frames, depth), lambda i, lab, scal: (scal[0] * (n_mine // step_seqs) + i, 0, 0)),
                pl.BlockSpec((step_seqs, SLOTS, 1), lambda i, lab, scal: (i, 0, 0)),
                pl.BlockSpec(memory_space=pl.ANY),
            ],
            out_specs=(
                pl.BlockSpec((step_seqs, SLOTS, n_frames), lambda i, lab, scal: (i, 0, 0)),
                pl.BlockSpec((step_seqs, SLOTS, depth), lambda i, lab, scal: (i, 0, 0)),
            ),
            scratch_shapes=[pltpu.VMEM((2, step_seqs, span, depth), jnp.bfloat16), pltpu.SemaphoreType.DMA((2, step_seqs))],
        ),
        out_shape=(jax.ShapeDtypeStruct((n_mine, SLOTS, n_frames), jnp.float32), jax.ShapeDtypeStruct((n_mine, SLOTS, depth), jnp.bfloat16)),
        compiler_params=params(),
        cost_estimate=pl.CostEstimate(flops=2 * n_mine * n_lab * ROWS * n_frames * depth, bytes_accessed=4 * n_mine * n_lab * ROWS * depth, transcendentals=0),
        name="label_logits",
    )(lab_flat, scal, enc, rem, wt_all)


def lattice_kernel(n_lab, dup_ref, zl_ref, lse_ref, lab_ref, skip_ref, first_ref, in_ref, len_ref, gl_ref, loss_ref, bb, lb, ll, bl, sl, occ):
    n_frames = zl_ref.shape[0]
    shape = zl_ref.shape[1:]
    slot = lax.broadcasted_iota(jnp.int32, shape, 0)
    in_len = in_ref[...]
    lab_len = len_ref[...]
    skip = skip_ref[...] > 0
    neg = jnp.full(shape, NEG_FILL, jnp.float32)

    def forward(t, carry):
        b, l = carry
        e = zl_ref[t] - lse_ref[pl.ds(t, 1), :]
        eb = e[n_lab - 1 : n_lab, :]
        prev = jnp.where(slot == 0, neg, pltpu.roll(l, 1, 0))
        top_b = jnp.maximum(b, prev)
        x0 = jnp.exp(b - top_b)
        x1 = jnp.exp(prev - top_b)
        sum_b = x0 + x1
        hop = jnp.where(skip, prev, neg)
        top_l = jnp.maximum(jnp.maximum(l, b), hop)
        y0 = jnp.exp(l - top_l)
        y1 = jnp.exp(b - top_l)
        y2 = jnp.exp(hop - top_l)
        sum_l = y0 + y1 + y2
        inv_b = 1.0 / sum_b
        inv_l = 1.0 / sum_l
        bb[t] = x0 * inv_b
        lb[t] = x1 * inv_b
        ll[t] = y0 * inv_l
        bl[t] = y1 * inv_l
        sl[t] = y2 * inv_l
        live = t < in_len
        new_b = jnp.where(live, top_b + jnp.log(sum_b) + eb, b)
        new_l = jnp.where(live, top_l + jnp.log(sum_l) + e, l)
        return new_b, new_l

    b, l = lax.fori_loop(0, n_frames, forward, (jnp.where(slot == 0, 0.0, neg), neg))
    end_b = jnp.where(slot == lab_len, b, neg)
    end_l = jnp.where(slot == lab_len - 1, l, neg)
    top = jnp.max(jnp.maximum(end_b, end_l), axis=0, keepdims=True)
    total = jnp.sum(jnp.exp(end_b - top) + jnp.exp(end_l - top), axis=0, keepdims=True)
    log_like = top + jnp.log(total)
    loss_ref[...] = -log_like

    def backward(i, carry):
        t = n_frames - 1 - i
        gb, gl = carry
        live = t < in_len
        blank = jnp.sum(gb, axis=0, keepdims=True)
        occ[t] = jnp.where(live, jnp.where(slot < n_lab - 1, gl, jnp.where(slot == n_lab - 1, blank, 0.0)), 0.0)
        back = pltpu.roll(gb * lb[t] + gl * sl[t], shape[0] - 1, 0)
        new_b = gb * bb[t] + gl * bl[t]
        new_l = gl * ll[t] + back
        return jnp.where(live, new_b, gb), jnp.where(live, new_l, gl)

    lax.fori_loop(0, n_frames, backward, (jnp.exp(end_b - log_like), jnp.exp(end_l - log_like)))

    lab = lab_ref[...]
    first = first_ref[...] > 0
    for v in range(1, n_lab - 1):

        @pl.when(dup_ref[v] > 0)
        def _():
            other = lab_ref[v : v + 1, :]
            take = (lab == other) & first & (first_ref[v : v + 1, :] <= 0) & (slot < n_lab - 1)

            def add(t, _):
                row = occ[t]
                occ[t] = row + jnp.where(take, row[v : v + 1, :], 0.0)
                return 0

            lax.fori_loop(0, n_frames, add, 0)

    def emit(t, _):
        p = jnp.exp(zl_ref[t] - lse_ref[pl.ds(t, 1), :])
        gl_ref[t] = jnp.where(first & (t < in_len), p - occ[t], 0.0).astype(gl_ref.dtype)
        return 0

    lax.fori_loop(0, n_frames, emit, 0)


def lattice(dup, zl, lse, lab, skip, first, in_len, lab_len, n_lab):
    n_frames, slots, lanes = zl.shape
    vmem = pl.BlockSpec(memory_space=pltpu.VMEM)
    return pl.pallas_call(
        functools.partial(lattice_kernel, n_lab + 1),
        in_specs=[pl.BlockSpec(memory_space=pltpu.SMEM)] + [vmem] * 7,
        out_specs=(vmem, vmem),
        out_shape=(jax.ShapeDtypeStruct((n_frames, slots, lanes), jnp.bfloat16), jax.ShapeDtypeStruct((1, lanes), jnp.float32)),
        scratch_shapes=[pltpu.VMEM((n_frames, slots, lanes), jnp.float32)] * 6,
        compiler_params=params(),
        cost_estimate=pl.CostEstimate(flops=2 * 10**10, bytes_accessed=2 * zl.size, transcendentals=0),
        name="lattice",
    )(dup, zl, lse, lab, skip, first, in_len, lab_len)


def place_start(recvs, out_ref, rows_ref, base, sem):
    step = pl.program_id(0)
    copies = []
    for i, ref in enumerate(recvs):
        n = ref.shape[0]
        row = pl.multiple_of(rows_ref[base + i] + step * n, 8)
        copy = pltpu.make_async_copy(ref, out_ref.at[pl.ds(row, n), :], sem.at[i])
        copy.start()
        copies.append(copy)
    return copies


def hs_kernel(n_lab, n_recv, has_prev, k, scal_ref, enc_ref, wt_ref, lse_ref, slot_ref, gl_ref, rows_ref, *refs):
    recvs = refs[:n_recv]
    refs = refs[n_recv + has_prev :]
    out_ref, sy_ref, sz_ref, shift, sem_r, sem_o = refs
    j = pl.program_id(0)
    n = pl.num_programs(0)
    n_seq, n_frames, depth = enc_ref.shape
    half = n_seq // 2
    placed = place_start(recvs, out_ref, scal_ref, 2, sem_r)

    @pl.when(j == 0)
    def _():
        cols = jnp.transpose(lse_ref[...])
        for s in range(n_seq):
            shift[s] = jnp.broadcast_to(cols[:n_frames, s : s + 1], (n_frames, 128))
        for part, acc in ((0, sy_ref), (1, sz_ref)):
            for s in range(half):
                seq = part * half + s
                acc[s * n_frames : (s + 1) * n_frames, :] = dot(gl_ref[seq], rows_ref[seq], TN)

    w = wt_ref[...]
    width = w.shape[0]
    col = j * width + lax.broadcasted_iota(jnp.int32, (n_seq, width), 1)
    bias = jnp.zeros((n_seq, width), jnp.float32)
    for u in range(n_lab):
        bias = jnp.where(col == slot_ref[:, u : u + 1], NEG_FILL, bias)
    for part, acc in ((0, sy_ref), (1, sz_ref)):
        enc = enc_ref[part * half : (part + 1) * half].reshape(half * n_frames, depth)
        z = dot(enc, w, NT)
        ps = []
        for s in range(half):
            seq = part * half + s
            low = jnp.concatenate([shift[seq]] * (width // 128), axis=1)
            p = jnp.exp(z[s * n_frames : (s + 1) * n_frames, :] - low + bias[seq : seq + 1, :])
            ps.append(p.astype(jnp.bfloat16))
        p = jnp.concatenate(ps, axis=0)
        acc[...] += dot(p, w, NN)

    @pl.when(j == n - 1)
    def _():
        rows = half * n_frames
        done = []
        for part, acc in ((0, sy_ref), (1, sz_ref)):
            row = pl.multiple_of(scal_ref[1] + (k * n_seq + part * half) * n_frames, 8)
            copy = pltpu.make_async_copy(acc, out_ref.at[pl.ds(row, rows), :], sem_o.at[part])
            copy.start()
            done.append(copy)
        for copy in done:
            copy.wait()

    for copy in placed:
        copy.wait()


def hs_chunk(k, n_mine, n_lab, scal, enc, wt_all, lse, slots, gl, lab_rows, recvs, prev):
    n_batch, n_frames, depth = enc.shape
    n_vocab = wt_all.shape[0]
    width = HS_WIDTH if n_vocab >= 8192 else 128
    steps = n_vocab // width
    n_chunk = n_mine // CHUNK
    half_rows = CHUNK // 2 * n_frames
    any_spec = pl.BlockSpec(memory_space=pl.ANY)
    in_specs = [
        pl.BlockSpec((CHUNK, n_frames, depth), lambda j, scal: (scal[0] * n_chunk + k, 0, 0)),
        pl.BlockSpec((width, depth), lambda j, scal: (j, 0)),
        pl.BlockSpec((CHUNK, 128), lambda j, scal: (scal[0] * n_chunk + k, 0)),
        pl.BlockSpec((CHUNK, SLOTS), lambda j, scal: (k, 0)),
        pl.BlockSpec((CHUNK, SLOTS, n_frames), lambda j, scal: (k, 0, 0)),
        pl.BlockSpec((CHUNK, SLOTS, depth), lambda j, scal: (k, 0, 0)),
    ]
    for r in recvs:
        in_specs.append(pl.BlockSpec((r.shape[0] // steps, depth), lambda j, scal: (j, 0)))
    args = [scal, enc, wt_all, lse, slots, gl, lab_rows, *recvs]
    aliases = {}
    if prev is not None:
        in_specs.append(any_spec)
        aliases = {len(args): 0}
        args.append(prev)
    send = jax.ShapeDtypeStruct((half_rows, depth), jnp.float32)
    rows = CHUNK * n_frames
    return pl.pallas_call(
        functools.partial(hs_kernel, n_lab, len(recvs), int(prev is not None), k),
        grid_spec=pltpu.PrefetchScalarGridSpec(
            num_scalar_prefetch=1,
            grid=(steps,),
            in_specs=in_specs,
            out_specs=(any_spec, pl.BlockSpec((half_rows, depth), lambda j, scal: (0, 0)), pl.BlockSpec((half_rows, depth), lambda j, scal: (0, 0))),
            scratch_shapes=[
                pltpu.VMEM((CHUNK, n_frames, 128), jnp.float32),
                pltpu.SemaphoreType.DMA((max(len(recvs), 1),)),
                pltpu.SemaphoreType.DMA((2,)),
            ],
        ),
        out_shape=(jax.ShapeDtypeStruct((n_batch * n_frames, depth), jnp.float32), send, send),
        input_output_aliases=aliases,
        compiler_params=params(),
        cost_estimate=pl.CostEstimate(flops=4 * rows * depth * n_vocab, bytes_accessed=2 * n_vocab * depth, transcendentals=rows * n_vocab),
        name="hs_chunk",
    )(*args)


def gw_kernel(n_recv, is_first, is_last, scal_ref, enc_ref, wt_ref, lse_ref, lab_ref, gl_ref, *refs):
    recvs = refs[:n_recv]
    acc_in = None if is_first else refs[n_recv]
    refs = refs[n_recv + (not is_first) + 1 :]
    out_ref, gw_ref, acc, bias, fan, diag, sem_r = refs
    i = pl.program_id(0)
    n = pl.num_programs(0)
    n_seq, n_frames, depth = enc_ref.shape
    n_cols = wt_ref.shape[0]
    rows = n_seq * n_frames
    placed = place_start(recvs, out_ref, scal_ref, 2, sem_r)

    @pl.when(i == 0)
    def _():
        seq_r = lax.broadcasted_iota(jnp.int32, (n_seq * SLOTS, rows), 0) // SLOTS
        seq_c = lax.broadcasted_iota(jnp.int32, (n_seq * SLOTS, rows), 1) // n_frames
        same = seq_r == seq_c
        bias[...] = jnp.where(same, NEG_FILL, 0.0).astype(jnp.bfloat16)
        diag[...] = jnp.where(same, 1.0, 0.0)
        t_r = lax.broadcasted_iota(jnp.int32, (n_frames, rows), 0)
        t_c = lax.rem(lax.broadcasted_iota(jnp.int32, (n_frames, rows), 1), n_frames)
        fan[...] = (t_r == t_c).astype(jnp.bfloat16)
        if is_first:
            acc[...] = jnp.zeros_like(acc)
        else:
            acc[...] = acc_in[...]

    enc = enc_ref[...].reshape(rows, depth)
    col = scal_ref[0] + lax.broadcasted_iota(jnp.int32, (n_cols, n_seq * SLOTS), 0)
    hot = (col == lab_ref[0]).astype(jnp.bfloat16)
    z = dot(wt_ref[...], enc, NT) + dot(hot, bias[...], NN)
    p = jnp.exp(z - lse_ref[0])
    wide = (dot(gl_ref[...].reshape(n_seq * SLOTS, n_frames), fan[...], NN) * diag[...]).astype(jnp.bfloat16)
    g = p.astype(jnp.bfloat16) + dot(hot, wide, NN).astype(jnp.bfloat16)
    acc[...] += dot(g, enc, NN)

    @pl.when(i == n - 1)
    def _():
        if is_last:
            gw_ref[...] = jnp.transpose(acc[...])
        else:
            gw_ref[...] = acc[...]

    for copy in placed:
        copy.wait()


def gw_part(part, n_part, scal, enc, wt, lse_rows, lab_rows, gl, recvs, acc, prev):
    n_batch, n_frames, depth = enc.shape
    n_cols = wt.shape[0]
    steps = n_batch // CHUNK // n_part
    base = part * steps
    rows = CHUNK * n_frames
    is_first, is_last = part == 0, part == n_part - 1
    any_spec = pl.BlockSpec(memory_space=pl.ANY)
    in_specs = [
        pl.BlockSpec((CHUNK, n_frames, depth), lambda i, scal: (base + i, 0, 0)),
        pl.BlockSpec((n_cols, depth), lambda i, scal: (0, 0)),
        pl.BlockSpec((1, 1, rows), lambda i, scal: (base + i, 0, 0)),
        pl.BlockSpec((1, 1, CHUNK * SLOTS), lambda i, scal: (base + i, 0, 0)),
        pl.BlockSpec((CHUNK, SLOTS, n_frames), lambda i, scal: (base + i, 0, 0)),
    ]
    for r in recvs:
        in_specs.append(pl.BlockSpec((r.shape[0] // steps, depth), lambda i, scal: (i, 0)))
    args = [scal, enc, wt, lse_rows, lab_rows, gl, *recvs]
    if not is_first:
        in_specs.append(pl.BlockSpec((n_cols, depth), lambda i, scal: (0, 0)))
        args.append(acc)
    in_specs.append(any_spec)
    aliases = {len(args): 0}
    args.append(prev)
    shape = (depth, n_cols) if is_last else (n_cols, depth)
    return pl.pallas_call(
        functools.partial(gw_kernel, len(recvs), is_first, is_last),
        grid_spec=pltpu.PrefetchScalarGridSpec(
            num_scalar_prefetch=1,
            grid=(steps,),
            in_specs=in_specs,
            out_specs=(any_spec, pl.BlockSpec(shape, lambda i, scal: (0, 0))),
            scratch_shapes=[
                pltpu.VMEM((n_cols, depth), jnp.float32),
                pltpu.VMEM((CHUNK * SLOTS, rows), jnp.bfloat16),
                pltpu.VMEM((n_frames, rows), jnp.bfloat16),
                pltpu.VMEM((CHUNK * SLOTS, rows), jnp.float32),
                pltpu.SemaphoreType.DMA((max(len(recvs), 1),)),
            ],
        ),
        out_shape=(jax.ShapeDtypeStruct(prev.shape, jnp.float32), jax.ShapeDtypeStruct(shape, jnp.float32)),
        input_output_aliases=aliases,
        compiler_params=params(),
        cost_estimate=pl.CostEstimate(flops=4 * steps * rows * depth * n_cols, bytes_accessed=2 * steps * rows * depth, transcendentals=steps * rows * n_cols),
        name="gw_part",
    )(*args)


def place_kernel(n_recv, scal_ref, *refs):
    copies = place_start(refs[:n_recv], refs[n_recv + 1], scal_ref, 2, refs[n_recv + 2])
    for copy in copies:
        copy.wait()


def place(scal, recvs, prev):
    depth = prev.shape[1]
    steps = 4
    any_spec = pl.BlockSpec(memory_space=pl.ANY)
    in_specs = [pl.BlockSpec((r.shape[0] // steps, depth), lambda i, scal: (i, 0)) for r in recvs] + [any_spec]
    return pl.pallas_call(
        functools.partial(place_kernel, len(recvs)),
        grid_spec=pltpu.PrefetchScalarGridSpec(
            num_scalar_prefetch=1, grid=(steps,), in_specs=in_specs, out_specs=any_spec, scratch_shapes=[pltpu.SemaphoreType.DMA((len(recvs),))]
        ),
        out_shape=jax.ShapeDtypeStruct(prev.shape, jnp.float32),
        input_output_aliases={1 + len(recvs): 0},
        compiler_params=params(),
        name="place",
    )(scal, *recvs, prev)


def solution(mesh):
    n_dev = mesh.shape["tp"]

    def swap(x, bit):
        return lax.ppermute(x, "tp", [(i, i ^ bit) for i in range(n_dev)])

    def device_fn(enc, w_loc, labels, in_len, lab_len):
        n_batch, n_frames, depth = enc.shape
        n_cols = w_loc.shape[1]
        n_lab = labels.shape[1]
        n_mine = n_batch // 4
        n_chunk = n_mine // CHUNK
        tp = lax.axis_index("tp")
        core = tp % 2
        colour = (tp // 2 + tp // 4) % 2
        mine = 2 * colour + core

        wt = w_loc.T
        wt_all, lse = spread_projection(enc, wt, n_dev, mesh.shape["dp"])
        lse = lse.reshape(n_batch, n_frames)
        frame = jnp.arange(n_frames)
        lse_live = jnp.where(frame[None, :] < in_len[:, None], lse, BIG)
        lse_pad = jnp.pad(lse_live, ((0, 0), (0, 128 - n_frames)), constant_values=BIG)

        u = jnp.arange(n_lab)
        valid = u[None, :] < lab_len[:, None]
        earlier = (labels[:, :, None] == labels[:, None, :]) & (u[None, :] < u[:, None])[None]
        first = valid & ~jnp.any(earlier, axis=2)
        slot_lab = jnp.concatenate(
            [jnp.where(first, labels, -1), jnp.zeros((n_batch, 1), jnp.int32), jnp.full((n_batch, SLOTS - n_lab - 1), -1, jnp.int32)], axis=1
        )

        def take(x):
            return lax.dynamic_slice_in_dim(x, mine * n_mine, n_mine, axis=0)

        lab_m = take(labels)
        slot_m = take(slot_lab)
        first_m = take(first)
        ext_m = jnp.concatenate([lab_m, jnp.zeros((n_mine, 1), jnp.int32)], axis=1)
        lab_flat = ext_m.reshape(-1)
        rem = jnp.pad(ext_m % ROWS, ((0, 0), (0, SLOTS - n_lab - 1)))[:, :, None]

        def lanes(x, fill):
            return jnp.pad(x, ((0, 0),) * (x.ndim - 1) + ((0, 128 - n_mine),), constant_values=fill)

        scal_z = jnp.stack([mine, mine]).astype(jnp.int32)
        zl, lab_proj = label_logits(lab_flat, scal_z, enc, rem, wt_all, n_mine, n_lab + 1)
        zl_t = lanes(jnp.transpose(zl, (2, 1, 0)), 0.0)
        lse_t = lanes(take(lse).T, 0.0)
        lab_t = jnp.pad(lanes(lab_m.T, -1), ((0, SLOTS - n_lab), (0, 0)), constant_values=-1)
        skip = jnp.pad(lab_m[:, 1:] != lab_m[:, :-1], ((0, 0), (1, 0)))
        skip_t = jnp.pad(lanes(skip.T.astype(jnp.int32), 0), ((0, SLOTS - n_lab), (0, 0)))
        first_t = jnp.pad(lanes(first_m.T.astype(jnp.int32), 0), ((0, SLOTS - n_lab), (0, 0)))
        first_t = jnp.where(jnp.arange(SLOTS)[:, None] == n_lab, 1, first_t)
        dup = jnp.pad(jnp.any(take(valid) & ~first_m, axis=0).astype(jnp.int32), (0, SLOTS - n_lab))
        gl_t, loss_m = lattice(dup, zl_t, lse_t, lab_t, skip_t, first_t, lanes(take(in_len)[None, :], 0), lanes(take(lab_len)[None, :], 4), n_lab)
        gl_t = gl_t[:, :, :n_mine]
        loss_m = loss_m[0, :n_mine]
        gl_gw = jnp.transpose(gl_t, (2, 1, 0))

        def spread(x):
            other = swap(x, 2)
            partner = swap(x, 1)
            last = swap(other, 1)
            out = jnp.zeros((4,) + x.shape, x.dtype)
            for value, where in ((x, mine), (other, mine ^ 2), (partner, mine ^ 1), (last, mine ^ 3)):
                out = lax.dynamic_update_index_in_dim(out, value, where, 0)
            return out.reshape((4 * x.shape[0],) + x.shape[1:])

        loss = spread(loss_m)
        gl_all = spread(gl_gw)

        set_rows = n_mine * n_frames
        half = CHUNK // 2 * n_frames
        moved = {}

        def rows_of(kinds):
            return [((mine ^ flip) * set_rows + k * CHUNK * n_frames + part * half) for k, part, flip in kinds]

        def scal_of(head, kinds):
            vals = list(head) + rows_of(kinds)
            vals += [0] * (8 - len(vals))
            return jnp.stack([jnp.asarray(v, jnp.int32) for v in vals])

        def arrived(*wanted):
            kinds = [(k, part, flip) for k, flip in wanted if 0 <= k < n_chunk for part in (0, 1)]
            return kinds, [moved[kind] for kind in kinds]

        def forward(k, after):
            for part in (0, 1):
                block = moved[(k, part, 2)]
                if after is not None:
                    block, after = lax.optimization_barrier((block, after))
                moved[(k, part, 3)] = swap(block, 1)
            return after

        out = None
        for k in range(n_chunk):
            kinds, data = arrived((k - 2, 1), (k - 3, 2), (k - 4, 3))
            scal = scal_of((mine, mine * set_rows), kinds)
            if k == 1:
                scal, loss, gl_all = lax.optimization_barrier((scal, loss, gl_all))
            out, sy, sz = hs_chunk(k, n_mine, n_lab + 1, scal, enc, wt_all, lse_pad, slot_m, gl_gw, lab_proj, data, out)
            for part, x, bit in ((0, sy, 2), (1, sz, 4)):
                moved[(k, part, 2)] = swap(x, bit)
                moved[(k, part, 1)] = swap(x, 1)
            if k >= 2:
                forward(k - 2, None)

        lse_rows = lse_live.reshape(n_batch // CHUNK, 1, CHUNK * n_frames)
        lab_rows = slot_lab.reshape(n_batch // CHUNK, 1, CHUNK * SLOTS)
        acc = None
        n_part = 3 if n_batch // CHUNK % 3 == 0 else 1
        for part in range(n_part):
            k = n_chunk + part
            kinds, data = arrived((k - 2, 1), (k - 3, 2), (k - 4, 3)) if n_part == 3 else ([], [])
            if part == 2:
                kinds, data = arrived((k - 4, 3))
            scal = scal_of((tp * n_cols, 0), kinds)
            out, acc = gw_part(part, n_part, scal, enc, wt, lse_rows, lab_rows, gl_all, data, acc, out)
            if part < 2 and n_part == 3:
                acc = forward(k - 2, acc)
        if n_part == 3:
            kinds, data = arrived((n_chunk - 1, 2), (n_chunk - 1, 3))
        else:
            for k in (n_chunk - 2, n_chunk - 1):
                forward(k, None)
            left = [(k, f) for k in range(n_chunk) for f in (1, 2, 3) if k + (2, 3, 4)[f - 1] >= n_chunk]
            for item in left[:-2]:
                kinds, data = arrived(item)
                out = place(scal_of((0, 0), kinds), data, out)
            kinds, data = arrived(*left[-2:])
        out = place(scal_of((0, 0), kinds), data, out)
        return loss, acc, out.reshape(n_batch, n_frames, depth)

    return jax.shard_map(
        device_fn,
        mesh=mesh,
        in_specs=(P("dp"), P(None, "tp"), P("dp"), P("dp"), P("dp")),
        out_specs=(P("dp"), P("dp", "tp"), P("dp")),
        check_vma=False,
    )
```

```python
import functools

import jax
import jax.numpy as jnp
from jax import lax
from jax.experimental import pallas as pl
from jax.experimental.pallas import tpu as pltpu
from jax.sharding import PartitionSpec as P


NEG_FILL = -1.0e30
BIG = 1.0e30
MESH = pl.DeviceIdType.MESH
NT = (((1,), (1,)), ((), ()))
NN = (((1,), (0,)), ((), ()))
TN = (((0,), (0,)), ((), ()))
SLOTS = 32
ROWS = 8
HS_WIDTH = 1024
CHUNK = 8
VMEM_LIMIT = 60 * 1024 * 1024


def dot(a, b, dims):
    return lax.dot_general(a, b, dims, preferred_element_type=jnp.float32)


def whole(*shape):
    return pl.BlockSpec(shape, lambda *_: (0,) * len(shape))


def blocks(shape, first):
    return pl.BlockSpec(shape, lambda *g: (first(*g),) + (0,) * (len(shape) - 1))


def in_place():
    return pl.BlockSpec(memory_space=pl.ANY)


def in_vmem():
    return pl.BlockSpec(memory_space=pltpu.VMEM)


def params(**kw):
    return pltpu.CompilerParams(vmem_limit_bytes=VMEM_LIMIT, **kw)


SUBS = 4
N_Z = 4
HOPS = SUBS * (N_Z - 1)
IDS = SUBS + 2 * HOPS


def spread_kernel(n_dev, n_dp, enc_hbm, w_ref, lab_ref, all_ref, lse_ref, z_hbm, *scratch):
    encbuf, st, recv, mine, bias, zbuf, enc_sem, own_sem, z_sem, *sems = scratch
    dn_send, dn_recv, up_send, up_recv, y_send, y_recv, x_send, x_recv, v_send, v_recv, c_send, c_recv, s1_send, s1_recv, s2_send, s2_recv = sems
    dp = lax.axis_index("dp")
    tp = lax.axis_index("tp")
    core = lax.rem(tp, 2)
    z = lax.div(tp, 4)
    mate = tp + 1 - 2 * core
    across = tp + 2 - 4 * lax.rem(lax.div(tp, 2), 2)
    block = w_ref.shape[0]
    piece = block // SUBS
    crosses = (core == dp) if n_dp > 1 else (core >= 0)
    n_seq, n_frames, depth = encbuf.shape[1:]

    def rows(owner, s):
        return all_ref.at[pl.ds(pl.multiple_of(owner * block + s * piece, piece), piece), :]

    def move(src, owner, s, send, got, dst):
        return pltpu.make_async_remote_copy(src_ref=src, dst_ref=rows(owner, s), send_sem=send, recv_sem=got, device_id=dst, device_id_type=MESH)

    def to(dev):
        return {"tp": dev}

    beside = {"dp": 1 - dp} if n_dp > 1 else to(tp)

    def owner_of(base, kind, q):
        hop = lax.div(q, SUBS) + 1
        return base + (4 * hop if kind == 1 else -4 * hop)

    def there(kind, q):
        hop = lax.div(q, SUBS) + 1
        return (q >= 0) & (q < HOPS) & ((z + hop <= N_Z - 1) if kind == 1 else (z - hop >= 0))

    def by_z(q):
        return (q < HOPS - SUBS) | crosses if n_dp > 1 else q >= 0

    barrier = pltpu.get_barrier_semaphore()
    for d in range(1, n_dev):
        pl.semaphore_signal(barrier, inc=1, device_id={"tp": lax.rem(tp + d, n_dev)}, device_id_type=MESH)
    if n_dp > 1:
        pl.semaphore_signal(barrier, inc=1, device_id=beside, device_id_type=MESH)
    pl.semaphore_wait(barrier, n_dev - 1 + (n_dp > 1))

    own = pltpu.make_async_copy(w_ref, all_ref.at[pl.ds(pl.multiple_of(tp * block, block), block), :], own_sem)
    own.start()

    def own_moves(s):
        src = w_ref.at[pl.ds(pl.multiple_of(s * piece, piece), piece), :]
        return (
            (z >= 1, move(src, tp, s, dn_send.at[s], dn_recv.at[s], to(tp - 4))),
            (z <= N_Z - 2, move(src, tp, s, up_send.at[s], up_recv.at[s], to(tp + 4))),
            (crosses, move(src, tp, s, y_send.at[s], y_recv.at[s], to(across))),
            (z >= 0, move(src, tp, s, c_send.at[s], c_recv.at[s], to(mate))),
        )

    def z_moves(kind, q):
        owner = owner_of(tp, kind, q)
        s = lax.rem(q, SUBS)
        src = rows(owner, s)
        got = dn_recv if kind == 1 else up_recv
        send = dn_send if kind == 1 else up_send
        number = SUBS + q + (0 if kind == 1 else HOPS)
        last = (z >= 1) if kind == 1 else (z <= N_Z - 2)
        nxt = lax.rem(q + SUBS, HOPS)
        here = there(kind, q) & by_z(q)
        return (
            here,
            move(src, owner, s, send.at[SUBS + q], got.at[q], to(tp)),
            (
                (here & last & by_z(q + SUBS), move(src, owner, s, send.at[SUBS + q], got.at[nxt], to(tp - 4 if kind == 1 else tp + 4))),
                (here, move(src, owner, s, c_send.at[number], c_recv.at[number], to(mate))),
                (here & crosses, move(src, owner, s, y_send.at[number], y_recv.at[number], to(across))),
                (here & (q >= HOPS - SUBS) & (n_dp > 1), move(src, owner, s, v_send.at[number], v_recv.at[number], beside)),
            ),
        )

    def v_moves(kind, q):
        q0 = lax.rem(q + HOPS, HOPS)
        owner, s, number = owner_of(tp, kind, q0), lax.rem(q0, SUBS), SUBS + q0 + (0 if kind == 1 else HOPS)
        src = rows(owner, s)
        here = there(kind, q) & jnp.logical_not(by_z(q))
        return (
            here,
            move(src, owner, s, v_send.at[number], v_recv.at[number], to(tp)),
            ((here, move(src, owner, s, c_send.at[number], c_recv.at[number], to(mate))),),
        )

    def far_parts(kind, q):
        if kind == 0:
            q0 = lax.rem(q + SUBS, SUBS)
            return across, q0, q0, (q >= 0) & (q < SUBS)
        q0 = lax.rem(q + HOPS, HOPS)
        return owner_of(across, kind, q0), lax.rem(q0, SUBS), SUBS + q0 + (0 if kind == 1 else HOPS), there(kind, q)

    def y_moves(kind, q):
        owner, s, number, here = far_parts(kind, q)
        src = rows(owner, s)
        return (
            here & crosses,
            move(src, owner, s, y_send.at[number], y_recv.at[number], to(tp)),
            (
                (here & crosses & (n_dp > 1), move(src, owner, s, x_send.at[number], x_recv.at[number], beside)),
                (here & crosses, move(src, owner, s, c_send.at[IDS + number], c_recv.at[IDS + number], to(mate))),
            ),
        )

    def x_moves(kind, q):
        owner, s, number, here = far_parts(kind, q)
        src = rows(owner, s)
        return (
            here & jnp.logical_not(crosses),
            move(src, owner, s, x_send.at[number], x_recv.at[number], to(tp)),
            ((here & jnp.logical_not(crosses), move(src, owner, s, c_send.at[IDS + number], c_recv.at[IDS + number], to(mate))),),
        )

    def start_all(moves):
        for cond, copy in moves:

            @pl.when(cond)
            def _():
                copy.start()

    def relay(group):
        cond, arrival, moves = group

        @pl.when(cond)
        def _():
            arrival.wait_recv()

        start_all(moves)

    def service(q):
        for kind in (1, 2):
            relay(z_moves(kind, q))
        relay(y_moves(0, jnp.minimum(q, SUBS)))
        for kind in (1, 2):
            relay(y_moves(kind, q - 1))
        if n_dp > 1:
            for kind in (1, 2):
                relay(v_moves(kind, q - 1))
            relay(x_moves(0, jnp.minimum(q - 1, SUBS)))
            for kind in (1, 2):
                relay(x_moves(kind, q - 2))

    def enc_copy(i):
        slot = lax.rem(i, 2)
        return pltpu.make_async_copy(enc_hbm.at[pl.ds(i * n_seq, n_seq)], encbuf.at[slot], enc_sem.at[slot])

    def z_copy(i):
        slot = lax.rem(i, 2)
        size = n_seq * n_frames
        return pltpu.make_async_copy(zbuf.at[slot], z_hbm.at[:, pl.ds(pl.multiple_of(i * size, 128), size)], z_sem.at[slot])

    enc_copy(0).start()
    for s in range(SUBS):
        start_all(own_moves(s))
    seq_r = lax.div(lax.broadcasted_iota(jnp.int32, bias.shape, 0), SLOTS)
    seq_c = lax.div(lax.broadcasted_iota(jnp.int32, bias.shape, 1), n_frames)
    bias[...] = jnp.where(seq_r == seq_c, NEG_FILL, 0.0).astype(bias.dtype)
    col = tp * block + lax.broadcasted_iota(jnp.int32, (block, n_seq * SLOTS), 0)

    per = n_dev // SUBS

    def tile(i, carry):
        enc_copy(i).wait()

        @pl.when(i + 1 < n_dev)
        def _():
            enc_copy(i + 1).start()

        slot = lax.rem(i, 2)
        enc = encbuf[slot].reshape(n_seq * n_frames, depth)
        zt = dot(w_ref[...], enc, NT)
        top = jnp.max(zt, axis=0, keepdims=True)
        st[i, 0:1, :] = top
        st[i, 1:2, :] = jnp.sum(jnp.exp(zt - top), axis=0, keepdims=True)

        @pl.when(i >= 2)
        def _():
            z_copy(i - 2).wait()

        hot = (col == lab_ref[i]).astype(jnp.bfloat16)
        zbuf[slot] = zt + dot(hot, bias[...], NN)
        z_copy(i).start()
        return carry

    def with_tiles(q, carry):
        lax.fori_loop(q * per, (q + 1) * per, tile, 0)
        service(q)
        return carry

    def plain(q, carry):
        service(q)
        return carry

    lax.fori_loop(0, SUBS, with_tiles, 0)
    first = []
    for d in range(1, n_dev):
        peer = lax.rem(tp + d, n_dev)
        first.append(
            pltpu.make_async_remote_copy(
                src_ref=st.at[peer], dst_ref=recv.at[tp], send_sem=s1_send.at[d], recv_sem=s1_recv.at[d], device_id=to(peer), device_id_type=MESH
            )
        )
    for copy in first:
        copy.start()
    recv[tp] = st[tp]
    lax.fori_loop(SUBS, SUBS + 2, plain, 0)
    for copy in first:
        copy.wait()
    top = recv[0, 0:1, :]
    for j in range(1, n_dev):
        top = jnp.maximum(top, recv[j, 0:1, :])
    total = jnp.zeros_like(top)
    for j in range(n_dev):
        total = total + recv[j, 1:2, :] * jnp.exp(recv[j, 0:1, :] - top)
    lse = top + jnp.log(total)
    mine[...] = lse
    lse_ref[tp] = lse
    lax.fori_loop(SUBS + 2, SUBS + 3, plain, 0)
    second = []
    for d in range(1, n_dev):
        peer = lax.rem(tp + d, n_dev)
        second.append(
            pltpu.make_async_remote_copy(
                src_ref=mine, dst_ref=lse_ref.at[tp], send_sem=s2_send.at[d], recv_sem=s2_recv.at[d], device_id=to(peer), device_id_type=MESH
            )
        )
    for copy in second:
        copy.start()
    lax.fori_loop(SUBS + 3, HOPS, plain, 0)

    for kind in (1, 2):
        relay(y_moves(kind, HOPS - 1))
    if n_dp > 1:
        for kind in (1, 2):
            relay(v_moves(kind, HOPS - 1))
        for q in (HOPS - 2, HOPS - 1):
            for kind in (1, 2):
                relay(x_moves(kind, q))
    for copy in second:
        copy.wait()
    own.wait()
    for i in (n_dev - 2, n_dev - 1):
        z_copy(i).wait()

    def drain(cond, copy):
        @pl.when(cond)
        def _():
            copy.wait_send()

    def finish_own(s, carry):
        for cond, copy in own_moves(s):
            drain(cond, copy)
        move(rows(mate, s), mate, s, c_send.at[s], c_recv.at[s], to(tp)).wait_recv()
        far = mate + across - tp
        move(rows(far, s), far, s, c_send.at[IDS + s], c_recv.at[IDS + s], to(tp)).wait_recv()
        for _, _, moves in (y_moves(0, s), x_moves(0, s)) if n_dp > 1 else (y_moves(0, s),):
            for cond, copy in moves:
                drain(cond, copy)
        return carry

    def finish(q, carry):
        for kind in (1, 2):
            here = there(kind, q)
            groups = (z_moves(kind, q), y_moves(kind, q))
            if n_dp > 1:
                groups += (v_moves(kind, q), x_moves(kind, q))
            for _, _, moves in groups:
                for cond, copy in moves:
                    drain(cond, copy)
            number = SUBS + q + (0 if kind == 1 else HOPS)
            s = lax.rem(q, SUBS)

            @pl.when(here)
            def _():
                near = owner_of(mate, kind, q)
                move(rows(near, s), near, s, c_send.at[number], c_recv.at[number], to(tp)).wait_recv()
                far = owner_of(mate + across - tp, kind, q)
                move(rows(far, s), far, s, c_send.at[IDS + number], c_recv.at[IDS + number], to(tp)).wait_recv()

        return carry

    lax.fori_loop(0, SUBS, finish_own, 0)
    lax.fori_loop(0, HOPS, finish, 0)


def spread_projection(enc, wt, slot_lab, n_dev, n_dp):
    n_batch, n_frames, depth = enc.shape
    n_cols = wt.shape[0]
    n_seq = n_batch // n_dev
    rows = n_seq * n_frames
    dma = pltpu.SemaphoreType.DMA
    sems = [SUBS + HOPS, HOPS] * 2 + [IDS] * 6 + [2 * IDS] * 2 + [n_dev] * 4
    return pl.pallas_call(
        functools.partial(spread_kernel, n_dev, n_dp),
        in_specs=[in_place(), in_vmem(), in_vmem()],
        out_specs=(in_place(), in_vmem(), in_place()),
        out_shape=(
            jax.ShapeDtypeStruct((n_dev * n_cols, depth), wt.dtype),
            jax.ShapeDtypeStruct((n_dev, 1, rows), jnp.float32),
            jax.ShapeDtypeStruct((n_cols, n_batch * n_frames), jnp.float32),
        ),
        scratch_shapes=[
            pltpu.VMEM((2, n_seq, n_frames, depth), enc.dtype),
            pltpu.VMEM((n_dev, 2, rows), jnp.float32),
            pltpu.VMEM((n_dev, 2, rows), jnp.float32),
            pltpu.VMEM((1, rows), jnp.float32),
            pltpu.VMEM((n_seq * SLOTS, rows), jnp.bfloat16),
            pltpu.VMEM((2, n_cols, rows), jnp.float32),
            dma((2,)),
            dma,
            dma((2,)),
            *[dma((n,)) for n in sems],
        ],
        compiler_params=params(collective_id=0, has_side_effects=True),
        cost_estimate=pl.CostEstimate(flops=2 * n_batch * n_frames * depth * n_cols, bytes_accessed=2 * enc.size, transcendentals=0),
        name="spread_projection",
    )(enc, wt, slot_lab.reshape(n_dev, 1, n_seq * SLOTS))


def label_kernel(n_lab, step_seqs, lab_ref, scal_ref, enc_ref, rem_ref, wt_hbm, out_ref, rows_ref, buf, sem):
    i = pl.program_id(0)
    n_mine, span, depth = buf.shape
    used = n_lab * ROWS

    @pl.when(i == 0)
    def _():
        def fetch(s, carry):
            for u in range(n_lab):
                base = pl.multiple_of(lab_ref[s * n_lab + u] & -ROWS, ROWS)
                pltpu.make_async_copy(wt_hbm.at[pl.ds(base, ROWS), :], buf.at[s, pl.ds(u * ROWS, ROWS), :], sem.at[s]).start()
            return carry

        lax.fori_loop(0, n_mine, fetch, 0)
        buf[:, used:, :] = jnp.zeros((n_mine, span - used, depth), buf.dtype)

    lane = lax.broadcasted_iota(jnp.int32, (SLOTS, span), 1)
    row = lax.broadcasted_iota(jnp.int32, (SLOTS, span), 0)
    for s in range(step_seqs):
        at = i * step_seqs + s
        pltpu.make_async_copy(wt_hbm.at[pl.ds(0, used), :], buf.at[at, pl.ds(0, used), :], sem.at[at]).wait()
    for s in range(step_seqs):
        pick = ((lane == row * ROWS + rem_ref[s]) & (row < n_lab)).astype(jnp.bfloat16)
        rows_ref[s] = dot(pick, buf[i * step_seqs + s], NN).astype(rows_ref.dtype)
    for s in range(step_seqs):
        out_ref[s] = dot(rows_ref[s], enc_ref[s], NT)


def label_logits(lab_flat, scal, enc, rem, wt_all, n_mine, n_lab):
    _, n_frames, depth = enc.shape
    step_seqs = CHUNK
    steps = n_mine // step_seqs
    span = (n_lab * ROWS + 15) // 16 * 16
    return pl.pallas_call(
        functools.partial(label_kernel, n_lab, step_seqs),
        grid_spec=pltpu.PrefetchScalarGridSpec(
            num_scalar_prefetch=2,
            grid=(steps,),
            in_specs=[
                blocks((step_seqs, n_frames, depth), lambda i, lab, scal: scal[0] * steps + i),
                blocks((step_seqs, SLOTS, 1), lambda i, lab, scal: i),
                in_place(),
            ],
            out_specs=(blocks((step_seqs, SLOTS, n_frames), lambda i, *_: i), blocks((step_seqs, SLOTS, depth), lambda i, *_: i)),
            scratch_shapes=[pltpu.VMEM((n_mine, span, depth), jnp.bfloat16), pltpu.SemaphoreType.DMA((n_mine,))],
        ),
        out_shape=(jax.ShapeDtypeStruct((n_mine, SLOTS, n_frames), jnp.float32), jax.ShapeDtypeStruct((n_mine, SLOTS, depth), jnp.bfloat16)),
        compiler_params=params(),
        cost_estimate=pl.CostEstimate(flops=2 * n_mine * n_lab * ROWS * n_frames * depth, bytes_accessed=4 * n_mine * n_lab * ROWS * depth, transcendentals=0),
        name="label_logits",
    )(lab_flat, scal, enc, rem, wt_all)


def lattice_kernel(n_lab, dup_ref, zl_ref, lse_ref, lab_ref, gl_ref, loss_ref, bb, lb, ll, bl, sl, occ):
    n_frames = zl_ref.shape[0]
    shape = zl_ref.shape[1:]
    slot = lax.broadcasted_iota(jnp.int32, shape, 0)
    blank_slot = n_lab - 1
    lab = lab_ref[...]
    in_len = lab_ref[blank_slot:n_lab, :]
    lab_len = lab_ref[n_lab : n_lab + 1, :]
    skip = (slot > 0) & (lab != pltpu.roll(lab, 1, 0))
    first = slot < lab_len
    for v in range(blank_slot - 1):
        first = first & ((lab != lab_ref[v : v + 1, :]) | (slot <= v))
    first = (first & (slot < blank_slot)) | (slot == blank_slot)
    neg = jnp.full(shape, NEG_FILL, jnp.float32)

    def forward(t, carry):
        b, l = carry
        e = zl_ref[t] - lse_ref[pl.ds(t, 1), :]
        eb = e[blank_slot:n_lab, :]
        prev = jnp.where(slot == 0, neg, pltpu.roll(l, 1, 0))
        top_b = jnp.maximum(b, prev)
        x0 = jnp.exp(b - top_b)
        x1 = jnp.exp(prev - top_b)
        sum_b = x0 + x1
        hop = jnp.where(skip, prev, neg)
        top_l = jnp.maximum(jnp.maximum(l, b), hop)
        y0 = jnp.exp(l - top_l)
        y1 = jnp.exp(b - top_l)
        y2 = jnp.exp(hop - top_l)
        sum_l = y0 + y1 + y2
        inv_b = 1.0 / sum_b
        inv_l = 1.0 / sum_l
        bb[t] = x0 * inv_b
        lb[t] = x1 * inv_b
        ll[t] = y0 * inv_l
        bl[t] = y1 * inv_l
        sl[t] = y2 * inv_l
        live = t < in_len
        new_b = jnp.where(live, top_b + jnp.log(sum_b) + eb, b)
        new_l = jnp.where(live, top_l + jnp.log(sum_l) + e, l)
        return new_b, new_l

    b, l = lax.fori_loop(0, n_frames, forward, (jnp.where(slot == 0, 0.0, neg), neg))
    end_b = jnp.where(slot == lab_len, b, neg)
    end_l = jnp.where(slot == lab_len - 1, l, neg)
    top = jnp.max(jnp.maximum(end_b, end_l), axis=0, keepdims=True)
    total = jnp.sum(jnp.exp(end_b - top) + jnp.exp(end_l - top), axis=0, keepdims=True)
    log_like = top + jnp.log(total)
    loss_ref[...] = -log_like

    def backward(i, carry):
        t = n_frames - 1 - i
        gb, gl = carry
        live = t < in_len
        blank = jnp.sum(gb, axis=0, keepdims=True)
        occ[t] = jnp.where(live, jnp.where(slot < blank_slot, gl, jnp.where(slot == blank_slot, blank, 0.0)), 0.0)
        back = pltpu.roll(gb * lb[t] + gl * sl[t], shape[0] - 1, 0)
        new_b = gb * bb[t] + gl * bl[t]
        new_l = gl * ll[t] + back
        return jnp.where(live, new_b, gb), jnp.where(live, new_l, gl)

    lax.fori_loop(0, n_frames, backward, (jnp.exp(end_b - log_like), jnp.exp(end_l - log_like)))

    for v in range(1, blank_slot):

        @pl.when(dup_ref[v] > 0)
        def _():
            take = (lab == lab_ref[v : v + 1, :]) & first & (slot < v)

            def add(t, _):
                row = occ[t]
                occ[t] = row + jnp.where(take, row[v : v + 1, :], 0.0)
                return 0

            lax.fori_loop(0, n_frames, add, 0)

    def emit(t, _):
        p = jnp.exp(zl_ref[t] - lse_ref[pl.ds(t, 1), :])
        gl_ref[t] = jnp.where(first & (t < in_len), p - occ[t], 0.0).astype(gl_ref.dtype)
        return 0

    lax.fori_loop(0, n_frames, emit, 0)


def lattice(dup, zl, lse, table, n_lab):
    n_frames, slots, lanes = zl.shape
    return pl.pallas_call(
        functools.partial(lattice_kernel, n_lab + 1),
        in_specs=[pl.BlockSpec(memory_space=pltpu.SMEM)] + [in_vmem()] * 3,
        out_specs=(in_vmem(), in_vmem()),
        out_shape=(jax.ShapeDtypeStruct((n_frames, slots, lanes), jnp.bfloat16), jax.ShapeDtypeStruct((1, lanes), jnp.float32)),
        scratch_shapes=[pltpu.VMEM((n_frames, slots, lanes), jnp.float32)] * 6,
        compiler_params=params(),
        cost_estimate=pl.CostEstimate(flops=2 * 10**10, bytes_accessed=2 * zl.size, transcendentals=0),
        name="lattice",
    )(dup, zl, lse, table)


def place_start(recvs, out_ref, scal_ref, sem):
    step = pl.program_id(0)
    copies = []
    for i, ref in enumerate(recvs):
        n = ref.shape[0]
        row = pl.multiple_of(scal_ref[1 + i] + step * n, 8)
        copy = pltpu.make_async_copy(ref, out_ref.at[pl.ds(row, n), :], sem.at[i])
        copy.start()
        copies.append(copy)
    return copies


def hs_kernel(n_lab, n_recv, has_prev, scal_ref, enc_ref, wt_ref, lse_ref, slot_ref, gl_ref, rows_ref, *refs):
    recvs = refs[:n_recv]
    refs = refs[n_recv + has_prev :]
    out_ref, sy_ref, sz_ref, shift, sem_r = refs
    j = pl.program_id(0)
    n_seq, n_frames, depth = enc_ref.shape
    half = n_seq // 2
    placed = place_start(recvs, out_ref, scal_ref, sem_r)

    @pl.when(j == 0)
    def _():
        cols = jnp.transpose(lse_ref[...])
        for s in range(n_seq):
            shift[s] = jnp.broadcast_to(cols[:n_frames, s : s + 1], (n_frames, 128))
        for part, acc in ((0, sy_ref), (1, sz_ref)):
            for s in range(half):
                seq = part * half + s
                acc[s * n_frames : (s + 1) * n_frames, :] = dot(gl_ref[seq], rows_ref[seq], TN)

    w = wt_ref[...]
    width = w.shape[0]
    col = j * width + lax.broadcasted_iota(jnp.int32, (n_seq, width), 1)
    bias = jnp.zeros((n_seq, width), jnp.float32)
    for u in range(n_lab):
        bias = jnp.where(col == slot_ref[:, u : u + 1], NEG_FILL, bias)
    for part, acc in ((0, sy_ref), (1, sz_ref)):
        enc = enc_ref[part * half : (part + 1) * half].reshape(half * n_frames, depth)
        z = dot(enc, w, NT)
        ps = []
        for s in range(half):
            seq = part * half + s
            low = jnp.concatenate([shift[seq]] * (width // 128), axis=1)
            p = jnp.exp(z[s * n_frames : (s + 1) * n_frames, :] - low + bias[seq : seq + 1, :])
            ps.append(p.astype(jnp.bfloat16))
        p = jnp.concatenate(ps, axis=0)
        acc[...] += dot(p, w, NN)

    for copy in placed:
        copy.wait()


def hs_chunk(k, n_mine, n_lab, scal, enc, wt_all, lse, slots, gl, lab_rows, recvs, prev):
    n_batch, n_frames, depth = enc.shape
    n_vocab = wt_all.shape[0]
    width = HS_WIDTH if n_vocab >= 8192 else 128
    steps = n_vocab // width
    n_chunk = n_mine // CHUNK
    half_rows = CHUNK // 2 * n_frames
    in_specs = [
        blocks((CHUNK, n_frames, depth), lambda j, scal: scal[0] * n_chunk + k),
        blocks((width, depth), lambda j, scal: j),
        blocks((CHUNK, 128), lambda j, scal: scal[0] * n_chunk + k),
        blocks((CHUNK, SLOTS), lambda *_: k),
        blocks((CHUNK, SLOTS, n_frames), lambda *_: k),
        blocks((CHUNK, SLOTS, depth), lambda *_: k),
    ]
    in_specs += [blocks((r.shape[0] // steps, depth), lambda j, scal: j) for r in recvs]
    args = [scal, enc, wt_all, lse, slots, gl, lab_rows, *recvs]
    aliases = {}
    if prev is not None:
        in_specs.append(in_place())
        aliases = {len(args): 0}
        args.append(prev)
    send = jax.ShapeDtypeStruct((half_rows, depth), jnp.float32)
    rows = CHUNK * n_frames
    return pl.pallas_call(
        functools.partial(hs_kernel, n_lab, len(recvs), int(prev is not None)),
        grid_spec=pltpu.PrefetchScalarGridSpec(
            num_scalar_prefetch=1,
            grid=(steps,),
            in_specs=in_specs,
            out_specs=(in_place(), whole(half_rows, depth), whole(half_rows, depth)),
            scratch_shapes=[pltpu.VMEM((CHUNK, n_frames, 128), jnp.float32), pltpu.SemaphoreType.DMA((max(len(recvs), 1),))],
        ),
        out_shape=(jax.ShapeDtypeStruct((n_batch * n_frames, depth), jnp.float32), send, send),
        input_output_aliases=aliases,
        compiler_params=params(),
        cost_estimate=pl.CostEstimate(flops=4 * rows * depth * n_vocab, bytes_accessed=2 * n_vocab * depth, transcendentals=rows * n_vocab),
        name="hs_chunk",
    )(*args)


def gw_kernel(n_recv, is_first, is_last, scal_ref, enc_ref, z_ref, lse_ref, lab_ref, gl_ref, *refs):
    recvs = refs[:n_recv]
    acc_in = None if is_first else refs[n_recv]
    refs = refs[n_recv + (not is_first) + 1 :]
    out_ref, gw_ref, acc, fan, diag, sem_r = refs
    i = pl.program_id(0)
    n_seq, n_frames, depth = enc_ref.shape
    n_cols, rows = z_ref.shape
    placed = place_start(recvs, out_ref, scal_ref, sem_r)

    @pl.when(i == 0)
    def _():
        seq_r = lax.div(lax.broadcasted_iota(jnp.int32, diag.shape, 0), SLOTS)
        seq_c = lax.div(lax.broadcasted_iota(jnp.int32, diag.shape, 1), n_frames)
        diag[...] = jnp.where(seq_r == seq_c, 1.0, 0.0)
        t_r = lax.broadcasted_iota(jnp.int32, fan.shape, 0)
        t_c = lax.rem(lax.broadcasted_iota(jnp.int32, fan.shape, 1), n_frames)
        fan[...] = (t_r == t_c).astype(jnp.bfloat16)
        if is_first:
            acc[...] = jnp.zeros_like(acc)
        else:
            acc[...] = acc_in[...]

    col = scal_ref[0] + lax.broadcasted_iota(jnp.int32, (n_cols, n_seq * SLOTS), 0)
    hot = (col == lab_ref[0]).astype(jnp.bfloat16)
    wide = (dot(gl_ref[...].reshape(n_seq * SLOTS, n_frames), fan[...], NN) * diag[...]).astype(jnp.bfloat16)
    g = jnp.exp(z_ref[...] - lse_ref[0]).astype(jnp.bfloat16) + dot(hot, wide, NN).astype(jnp.bfloat16)
    acc[...] += dot(g, enc_ref[...].reshape(rows, depth), NN)

    @pl.when(i == pl.num_programs(0) - 1)
    def _():
        gw_ref[...] = jnp.transpose(acc[...]) if is_last else acc[...]

    for copy in placed:
        copy.wait()


def gw_part(part, n_part, scal, enc, z, lse_rows, lab_rows, gl, recvs, acc, prev):
    n_batch, n_frames, depth = enc.shape
    n_cols = z.shape[0]
    steps = n_batch // CHUNK // n_part
    base = part * steps
    rows = CHUNK * n_frames
    is_first, is_last = part == 0, part == n_part - 1

    def here(i, scal):
        return base + i

    in_specs = [
        blocks((CHUNK, n_frames, depth), here),
        pl.BlockSpec((n_cols, rows), lambda i, scal: (0, base + i)),
        blocks((1, 1, rows), here),
        blocks((1, 1, CHUNK * SLOTS), here),
        blocks((CHUNK, SLOTS, n_frames), here),
    ]
    in_specs += [blocks((r.shape[0] // steps, depth), lambda i, scal: i) for r in recvs]
    args = [scal, enc, z, lse_rows, lab_rows, gl, *recvs]
    if not is_first:
        in_specs.append(whole(n_cols, depth))
        args.append(acc)
    in_specs.append(in_place())
    aliases = {len(args): 0}
    args.append(prev)
    shape = (depth, n_cols) if is_last else (n_cols, depth)
    return pl.pallas_call(
        functools.partial(gw_kernel, len(recvs), is_first, is_last),
        grid_spec=pltpu.PrefetchScalarGridSpec(
            num_scalar_prefetch=1,
            grid=(steps,),
            in_specs=in_specs,
            out_specs=(in_place(), whole(*shape)),
            scratch_shapes=[
                pltpu.VMEM((n_cols, depth), jnp.float32),
                pltpu.VMEM((n_frames, rows), jnp.bfloat16),
                pltpu.VMEM((CHUNK * SLOTS, rows), jnp.float32),
                pltpu.SemaphoreType.DMA((max(len(recvs), 1),)),
            ],
        ),
        out_shape=(jax.ShapeDtypeStruct(prev.shape, jnp.float32), jax.ShapeDtypeStruct(shape, jnp.float32)),
        input_output_aliases=aliases,
        compiler_params=params(),
        cost_estimate=pl.CostEstimate(flops=2 * steps * rows * depth * n_cols, bytes_accessed=4 * steps * rows * n_cols, transcendentals=steps * rows * n_cols),
        name="gw_part",
    )(*args)


def place_kernel(n_recv, scal_ref, *refs):
    copies = place_start(refs[:n_recv], refs[n_recv + 1], scal_ref, refs[n_recv + 2])
    for copy in copies:
        copy.wait()


def place(scal, recvs, prev):
    depth = prev.shape[1]
    steps = 4
    in_specs = [blocks((r.shape[0] // steps, depth), lambda i, scal: i) for r in recvs] + [in_place()]
    return pl.pallas_call(
        functools.partial(place_kernel, len(recvs)),
        grid_spec=pltpu.PrefetchScalarGridSpec(
            num_scalar_prefetch=1, grid=(steps,), in_specs=in_specs, out_specs=in_place(), scratch_shapes=[pltpu.SemaphoreType.DMA((len(recvs),))]
        ),
        out_shape=jax.ShapeDtypeStruct(prev.shape, jnp.float32),
        input_output_aliases={1 + len(recvs): 0},
        compiler_params=params(),
        name="place",
    )(scal, *recvs, prev)


def solution(mesh):
    n_dev = mesh.shape["tp"]

    def swap(x, bit):
        return lax.ppermute(x, "tp", [(i, i ^ bit) for i in range(n_dev)])

    def device_fn(enc, w_loc, labels, in_len, lab_len):
        n_batch, n_frames, depth = enc.shape
        n_cols = w_loc.shape[1]
        n_lab = labels.shape[1]
        n_mine = n_batch // 4
        n_chunk = n_mine // CHUNK
        tp = lax.axis_index("tp")
        core = tp % 2
        colour = (tp // 2 + tp // 4) % 2
        mine = 2 * colour + core

        u = jnp.arange(n_lab)
        valid = u[None, :] < lab_len[:, None]
        earlier = (labels[:, :, None] == labels[:, None, :]) & (u[None, :] < u[:, None])[None]
        first = valid & ~jnp.any(earlier, axis=2)
        slot_lab = jnp.concatenate(
            [jnp.where(first, labels, -1), jnp.zeros((n_batch, 1), jnp.int32), jnp.full((n_batch, SLOTS - n_lab - 1), -1, jnp.int32)], axis=1
        )

        wt = w_loc.T
        wt_all, lse, z_loc = spread_projection(enc, wt, slot_lab, n_dev, mesh.shape["dp"])
        lse = lse.reshape(n_batch, n_frames)
        lse_live = jnp.where(jnp.arange(n_frames)[None, :] < in_len[:, None], lse, BIG)
        lse_pad = jnp.pad(lse_live, ((0, 0), (0, 128 - n_frames)), constant_values=BIG)

        def take(x):
            return lax.dynamic_slice_in_dim(x, mine * n_mine, n_mine, axis=0)

        lab_m = take(labels)
        slot_m = take(slot_lab)
        ext_m = jnp.concatenate([lab_m, jnp.zeros((n_mine, SLOTS - n_lab), jnp.int32)], axis=1)
        rem = (ext_m & (ROWS - 1))[:, :, None]
        table = jnp.concatenate([lab_m, take(in_len)[:, None], take(lab_len)[:, None], ext_m[:, n_lab + 2 :]], axis=1).T
        dup = jnp.pad(jnp.any(take(valid & ~first), axis=0).astype(jnp.int32), (0, SLOTS - n_lab))

        zl, lab_proj = label_logits(ext_m[:, : n_lab + 1].reshape(-1), jnp.stack([mine, mine]).astype(jnp.int32), enc, rem, wt_all, n_mine, n_lab + 1)
        gl_t, loss_m = lattice(dup, jnp.transpose(zl, (2, 1, 0)), take(lse).T, table, n_lab)
        loss_m = loss_m[0]
        gl_gw = jnp.transpose(gl_t, (2, 1, 0))

        def spread(x):
            other = swap(x, 2)
            partner = swap(x, 1)
            last = swap(other, 1)
            out = jnp.zeros((4,) + x.shape, x.dtype)
            for value, where in ((x, mine), (other, mine ^ 2), (partner, mine ^ 1), (last, mine ^ 3)):
                out = lax.dynamic_update_index_in_dim(out, value, where, 0)
            return out.reshape((4 * x.shape[0],) + x.shape[1:])

        loss = spread(loss_m)
        gl_all = spread(gl_gw)

        set_rows = n_mine * n_frames
        half = CHUNK // 2 * n_frames
        moved = {}

        def rows_of(kinds):
            return [((mine ^ flip) * set_rows + k * CHUNK * n_frames + part * half) for k, part, flip in kinds]

        def scal_of(head, kinds):
            vals = [head] + rows_of(kinds)
            vals += [0] * (SLOTS // 2 - len(vals))
            return jnp.stack([jnp.asarray(v, jnp.int32) for v in vals])

        def arrived(*wanted):
            kinds = [(k, part, flip) for k, flip in wanted if 0 <= k < n_chunk for part in (0, 1)]
            return kinds, [moved[kind] for kind in kinds]

        def forward(k, after):
            for part in (0, 1):
                block = moved[(k, part, 2)]
                if after is not None:
                    block, after = lax.optimization_barrier((block, after))
                moved[(k, part, 3)] = swap(block, 1)
            return after

        def due(i):
            return arrived((i - 1, 0), (i - 2, 1), (i - 3, 2), (i - 4, 3))

        out = None
        for k in range(n_chunk):
            kinds, data = due(k)
            scal = scal_of(mine, kinds)
            if k == 1:
                scal, loss, gl_all = lax.optimization_barrier((scal, loss, gl_all))
            out, sy, sz = hs_chunk(k, n_mine, n_lab + 1, scal, enc, wt_all, lse_pad, slot_m, gl_gw, lab_proj, data, out)
            for part, x, bit in ((0, sy, 2), (1, sz, 4)):
                moved[(k, part, 0)] = x
                moved[(k, part, 1)] = swap(x, 1)
                moved[(k, part, 2)] = swap(x, bit)
            if k >= 2:
                forward(k - 2, None)

        lse_rows = lse_live.reshape(n_batch // CHUNK, 1, CHUNK * n_frames)
        lab_rows = slot_lab.reshape(n_batch // CHUNK, 1, CHUNK * SLOTS)
        acc = None
        n_part = 3
        for part in range(n_part):
            kinds, data = due(n_chunk + part) if part < n_part - 1 else arrived((n_chunk - 2, 3))
            out, acc = gw_part(part, n_part, scal_of(tp * n_cols, kinds), enc, z_loc, lse_rows, lab_rows, gl_all, data, acc, out)
            if part < n_part - 1:
                acc = forward(n_chunk + part - 2, acc)
        kinds, data = arrived((n_chunk - 1, 2), (n_chunk - 1, 3))
        out = place(scal_of(tp, kinds), data, out)
        return loss, acc, out.reshape(n_batch, n_frames, depth)

    return jax.shard_map(
        device_fn,
        mesh=mesh,
        in_specs=(P("dp"), P(None, "tp"), P("dp"), P("dp"), P("dp")),
        out_specs=(P("dp"), P("dp", "tp"), P("dp")),
        check_vma=False,
    )
```

```python
import functools

import jax
import jax.numpy as jnp
from jax import lax
from jax.experimental import pallas as pl
from jax.experimental.pallas import tpu as pltpu
from jax.sharding import PartitionSpec as P


NEG_FILL = -1.0e30
BIG = 1.0e30
MESH = pl.DeviceIdType.MESH
NT = (((1,), (1,)), ((), ()))
NN = (((1,), (0,)), ((), ()))
TN = (((0,), (0,)), ((), ()))
SLOTS = 32
ROWS = 8
HS_WIDTH = 1024
CHUNK = 12
GROUP = 8
VMEM_LIMIT = 60 * 1024 * 1024


def dot(a, b, dims):
    return lax.dot_general(a, b, dims, preferred_element_type=jnp.float32)


def whole(*shape):
    return pl.BlockSpec(shape, lambda *_: (0,) * len(shape))


def blocks(shape, first):
    return pl.BlockSpec(shape, lambda *g: (first(*g),) + (0,) * (len(shape) - 1))


def in_place():
    return pl.BlockSpec(memory_space=pl.ANY)


def in_vmem():
    return pl.BlockSpec(memory_space=pltpu.VMEM)


def params(**kw):
    return pltpu.CompilerParams(vmem_limit_bytes=VMEM_LIMIT, **kw)


SUBS = 4
N_Z = 4
HOPS = SUBS * (N_Z - 1)
IDS = SUBS + 2 * HOPS


def spread_kernel(n_dev, n_dp, enc_hbm, w_ref, lab_ref, all_ref, lse_ref, z_hbm, *scratch):
    encbuf, st, recv, mine, bias, zbuf, enc_sem, own_sem, z_sem, *sems = scratch
    dn_send, dn_recv, up_send, up_recv, y_send, y_recv, x_send, x_recv, v_send, v_recv, c_send, c_recv, s1_send, s1_recv, s2_send, s2_recv = sems
    dp = lax.axis_index("dp")
    tp = lax.axis_index("tp")
    core = lax.rem(tp, 2)
    z = lax.div(tp, 4)
    mate = tp + 1 - 2 * core
    across = tp + 2 - 4 * lax.rem(lax.div(tp, 2), 2)
    block = w_ref.shape[0]
    piece = block // SUBS
    crosses = (core == dp) if n_dp > 1 else (core >= 0)
    n_seq, n_frames, depth = encbuf.shape[1:]

    def rows(owner, s):
        return all_ref.at[pl.ds(pl.multiple_of(owner * block + s * piece, piece), piece), :]

    def move(src, owner, s, send, got, dst):
        return pltpu.make_async_remote_copy(src_ref=src, dst_ref=rows(owner, s), send_sem=send, recv_sem=got, device_id=dst, device_id_type=MESH)

    def to(dev):
        return {"tp": dev}

    beside = {"dp": 1 - dp} if n_dp > 1 else to(tp)

    def owner_of(base, kind, q):
        hop = lax.div(q, SUBS) + 1
        return base + (4 * hop if kind == 1 else -4 * hop)

    def there(kind, q):
        hop = lax.div(q, SUBS) + 1
        return (q >= 0) & (q < HOPS) & ((z + hop <= N_Z - 1) if kind == 1 else (z - hop >= 0))

    def by_z(q):
        return (q < HOPS - SUBS) | crosses if n_dp > 1 else q >= 0

    barrier = pltpu.get_barrier_semaphore()
    for d in range(1, n_dev):
        pl.semaphore_signal(barrier, inc=1, device_id={"tp": lax.rem(tp + d, n_dev)}, device_id_type=MESH)
    if n_dp > 1:
        pl.semaphore_signal(barrier, inc=1, device_id=beside, device_id_type=MESH)
    pl.semaphore_wait(barrier, n_dev - 1 + (n_dp > 1))

    own = pltpu.make_async_copy(w_ref, all_ref.at[pl.ds(pl.multiple_of(tp * block, block), block), :], own_sem)
    own.start()

    def own_moves(s):
        src = w_ref.at[pl.ds(pl.multiple_of(s * piece, piece), piece), :]
        return (
            (z >= 1, move(src, tp, s, dn_send.at[s], dn_recv.at[s], to(tp - 4))),
            (z <= N_Z - 2, move(src, tp, s, up_send.at[s], up_recv.at[s], to(tp + 4))),
            (crosses, move(src, tp, s, y_send.at[s], y_recv.at[s], to(across))),
            (z >= 0, move(src, tp, s, c_send.at[s], c_recv.at[s], to(mate))),
        )

    def z_moves(kind, q):
        owner = owner_of(tp, kind, q)
        s = lax.rem(q, SUBS)
        src = rows(owner, s)
        got = dn_recv if kind == 1 else up_recv
        send = dn_send if kind == 1 else up_send
        number = SUBS + q + (0 if kind == 1 else HOPS)
        last = (z >= 1) if kind == 1 else (z <= N_Z - 2)
        nxt = lax.rem(q + SUBS, HOPS)
        here = there(kind, q) & by_z(q)
        return (
            here,
            move(src, owner, s, send.at[SUBS + q], got.at[q], to(tp)),
            (
                (here & last & by_z(q + SUBS), move(src, owner, s, send.at[SUBS + q], got.at[nxt], to(tp - 4 if kind == 1 else tp + 4))),
                (here, move(src, owner, s, c_send.at[number], c_recv.at[number], to(mate))),
                (here & crosses, move(src, owner, s, y_send.at[number], y_recv.at[number], to(across))),
                (here & (q >= HOPS - SUBS) & (n_dp > 1), move(src, owner, s, v_send.at[number], v_recv.at[number], beside)),
            ),
        )

    def v_moves(kind, q):
        q0 = lax.rem(q + HOPS, HOPS)
        owner, s, number = owner_of(tp, kind, q0), lax.rem(q0, SUBS), SUBS + q0 + (0 if kind == 1 else HOPS)
        src = rows(owner, s)
        here = there(kind, q) & jnp.logical_not(by_z(q))
        return (
            here,
            move(src, owner, s, v_send.at[number], v_recv.at[number], to(tp)),
            ((here, move(src, owner, s, c_send.at[number], c_recv.at[number], to(mate))),),
        )

    def far_parts(kind, q):
        if kind == 0:
            q0 = lax.rem(q + SUBS, SUBS)
            return across, q0, q0, (q >= 0) & (q < SUBS)
        q0 = lax.rem(q + HOPS, HOPS)
        return owner_of(across, kind, q0), lax.rem(q0, SUBS), SUBS + q0 + (0 if kind == 1 else HOPS), there(kind, q)

    def y_moves(kind, q):
        owner, s, number, here = far_parts(kind, q)
        src = rows(owner, s)
        return (
            here & crosses,
            move(src, owner, s, y_send.at[number], y_recv.at[number], to(tp)),
            (
                (here & crosses & (n_dp > 1), move(src, owner, s, x_send.at[number], x_recv.at[number], beside)),
                (here & crosses, move(src, owner, s, c_send.at[IDS + number], c_recv.at[IDS + number], to(mate))),
            ),
        )

    def x_moves(kind, q):
        owner, s, number, here = far_parts(kind, q)
        src = rows(owner, s)
        return (
            here & jnp.logical_not(crosses),
            move(src, owner, s, x_send.at[number], x_recv.at[number], to(tp)),
            ((here & jnp.logical_not(crosses), move(src, owner, s, c_send.at[IDS + number], c_recv.at[IDS + number], to(mate))),),
        )

    def start_all(moves):
        for cond, copy in moves:

            @pl.when(cond)
            def _():
                copy.start()

    def relay(group):
        cond, arrival, moves = group

        @pl.when(cond)
        def _():
            arrival.wait_recv()

        start_all(moves)

    def service(q):
        for kind in (1, 2):
            relay(z_moves(kind, q))
        relay(y_moves(0, jnp.minimum(q, SUBS)))
        for kind in (1, 2):
            relay(y_moves(kind, q - 1))
        if n_dp > 1:
            for kind in (1, 2):
                relay(v_moves(kind, q - 1))
            relay(x_moves(0, jnp.minimum(q - 1, SUBS)))
            for kind in (1, 2):
                relay(x_moves(kind, q - 2))

    def enc_copy(i):
        slot = lax.rem(i, 2)
        return pltpu.make_async_copy(enc_hbm.at[pl.ds(i * n_seq, n_seq)], encbuf.at[slot], enc_sem.at[slot])

    def z_copy(i):
        slot = lax.rem(i, 2)
        size = n_seq * n_frames
        return pltpu.make_async_copy(zbuf.at[slot], z_hbm.at[:, pl.ds(pl.multiple_of(i * size, 128), size)], z_sem.at[slot])

    enc_copy(0).start()
    for s in range(SUBS):
        start_all(own_moves(s))
    seq_r = lax.div(lax.broadcasted_iota(jnp.int32, bias.shape, 0), SLOTS)
    seq_c = lax.div(lax.broadcasted_iota(jnp.int32, bias.shape, 1), n_frames)
    bias[...] = jnp.where(seq_r == seq_c, NEG_FILL, 0.0).astype(bias.dtype)
    col = tp * block + lax.broadcasted_iota(jnp.int32, (block, n_seq * SLOTS), 0)

    busy = 2 * SUBS
    per = n_dev // busy

    def tile(i, carry):
        enc_copy(i).wait()

        @pl.when(i + 1 < n_dev)
        def _():
            enc_copy(i + 1).start()

        slot = lax.rem(i, 2)
        enc = encbuf[slot].reshape(n_seq * n_frames, depth)
        zt = dot(w_ref[...], enc, NT)
        top = jnp.max(zt, axis=0, keepdims=True)
        st[i, 0:1, :] = top
        st[i, 1:2, :] = jnp.sum(jnp.exp(zt - top), axis=0, keepdims=True)

        @pl.when(i >= 2)
        def _():
            z_copy(i - 2).wait()

        hot = (col == lab_ref[i]).astype(jnp.bfloat16)
        zbuf[slot] = zt + dot(hot, bias[...], NN)
        z_copy(i).start()
        return carry

    def with_tiles(q, carry):
        lax.fori_loop(q * per, (q + 1) * per, tile, 0)
        service(q)
        return carry

    def plain(q, carry):
        service(q)
        return carry

    lax.fori_loop(0, busy, with_tiles, 0)
    first = []
    for d in range(1, n_dev):
        peer = lax.rem(tp + d, n_dev)
        first.append(
            pltpu.make_async_remote_copy(
                src_ref=st.at[peer], dst_ref=recv.at[tp], send_sem=s1_send.at[d], recv_sem=s1_recv.at[d], device_id=to(peer), device_id_type=MESH
            )
        )
    for copy in first:
        copy.start()
    recv[tp] = st[tp]
    lax.fori_loop(busy, busy + 1, plain, 0)
    for copy in first:
        copy.wait()
    top = recv[0, 0:1, :]
    for j in range(1, n_dev):
        top = jnp.maximum(top, recv[j, 0:1, :])
    total = jnp.zeros_like(top)
    for j in range(n_dev):
        total = total + recv[j, 1:2, :] * jnp.exp(recv[j, 0:1, :] - top)
    lse = top + jnp.log(total)
    mine[...] = lse
    lse_ref[tp] = lse
    second = []
    for d in range(1, n_dev):
        peer = lax.rem(tp + d, n_dev)
        second.append(
            pltpu.make_async_remote_copy(
                src_ref=mine, dst_ref=lse_ref.at[tp], send_sem=s2_send.at[d], recv_sem=s2_recv.at[d], device_id=to(peer), device_id_type=MESH
            )
        )
    for copy in second:
        copy.start()
    lax.fori_loop(busy + 1, HOPS, plain, 0)

    for kind in (1, 2):
        relay(y_moves(kind, HOPS - 1))
    if n_dp > 1:
        for kind in (1, 2):
            relay(v_moves(kind, HOPS - 1))
        for q in (HOPS - 2, HOPS - 1):
            for kind in (1, 2):
                relay(x_moves(kind, q))
    for copy in second:
        copy.wait()
    own.wait()
    for i in (n_dev - 2, n_dev - 1):
        z_copy(i).wait()

    def drain(cond, copy):
        @pl.when(cond)
        def _():
            copy.wait_send()

    def finish_own(s, carry):
        for cond, copy in own_moves(s):
            drain(cond, copy)
        move(rows(mate, s), mate, s, c_send.at[s], c_recv.at[s], to(tp)).wait_recv()
        far = mate + across - tp
        move(rows(far, s), far, s, c_send.at[IDS + s], c_recv.at[IDS + s], to(tp)).wait_recv()
        for _, _, moves in (y_moves(0, s), x_moves(0, s)) if n_dp > 1 else (y_moves(0, s),):
            for cond, copy in moves:
                drain(cond, copy)
        return carry

    def finish(q, carry):
        for kind in (1, 2):
            here = there(kind, q)
            groups = (z_moves(kind, q), y_moves(kind, q))
            if n_dp > 1:
                groups += (v_moves(kind, q), x_moves(kind, q))
            for _, _, moves in groups:
                for cond, copy in moves:
                    drain(cond, copy)
            number = SUBS + q + (0 if kind == 1 else HOPS)
            s = lax.rem(q, SUBS)

            @pl.when(here)
            def _():
                near = owner_of(mate, kind, q)
                move(rows(near, s), near, s, c_send.at[number], c_recv.at[number], to(tp)).wait_recv()
                far = owner_of(mate + across - tp, kind, q)
                move(rows(far, s), far, s, c_send.at[IDS + number], c_recv.at[IDS + number], to(tp)).wait_recv()

        return carry

    lax.fori_loop(0, SUBS, finish_own, 0)
    lax.fori_loop(0, HOPS, finish, 0)


def spread_projection(enc, wt, slot_lab, n_dev, n_dp):
    n_batch, n_frames, depth = enc.shape
    n_cols = wt.shape[0]
    n_seq = n_batch // n_dev
    rows = n_seq * n_frames
    dma = pltpu.SemaphoreType.DMA
    sems = [SUBS + HOPS, HOPS] * 2 + [IDS] * 6 + [2 * IDS] * 2 + [n_dev] * 4
    return pl.pallas_call(
        functools.partial(spread_kernel, n_dev, n_dp),
        in_specs=[in_place(), in_vmem(), in_vmem()],
        out_specs=(in_place(), in_vmem(), in_place()),
        out_shape=(
            jax.ShapeDtypeStruct((n_dev * n_cols, depth), wt.dtype),
            jax.ShapeDtypeStruct((n_dev, 1, rows), jnp.float32),
            jax.ShapeDtypeStruct((n_cols, n_batch * n_frames), jnp.float32),
        ),
        scratch_shapes=[
            pltpu.VMEM((2, n_seq, n_frames, depth), enc.dtype),
            pltpu.VMEM((n_dev, 2, rows), jnp.float32),
            pltpu.VMEM((n_dev, 2, rows), jnp.float32),
            pltpu.VMEM((1, rows), jnp.float32),
            pltpu.VMEM((n_seq * SLOTS, rows), jnp.bfloat16),
            pltpu.VMEM((2, n_cols, rows), jnp.float32),
            dma((2,)),
            dma,
            dma((2,)),
            *[dma((n,)) for n in sems],
        ],
        compiler_params=params(collective_id=0, has_side_effects=True),
        cost_estimate=pl.CostEstimate(flops=2 * n_batch * n_frames * depth * n_cols, bytes_accessed=2 * enc.size, transcendentals=0),
        name="spread_projection",
    )(enc, wt, slot_lab.reshape(n_dev, 1, n_seq * SLOTS))


def label_kernel(n_lab, step_seqs, lab_ref, scal_ref, enc_ref, tab_ref, wt_hbm, out_ref, rows_ref, buf, sem):
    i = pl.program_id(0)
    n_mine, span, depth = buf.shape
    used = n_lab * ROWS

    def fetch(s, carry):
        for u in range(n_lab):
            base = pl.multiple_of(lab_ref[s * n_lab + u] & -ROWS, ROWS)
            pltpu.make_async_copy(wt_hbm.at[pl.ds(base, ROWS), :], buf.at[s, pl.ds(u * ROWS, ROWS), :], sem.at[s]).start()
        return carry

    ahead = 2 * step_seqs

    @pl.when(i == 0)
    def _():
        lax.fori_loop(0, jnp.minimum(ahead, n_mine), fetch, 0)
        buf[:, used:, :] = jnp.zeros((n_mine, span - used, depth), buf.dtype)

    lax.fori_loop(jnp.minimum(i * step_seqs + ahead, n_mine), jnp.minimum((i + 1) * step_seqs + ahead, n_mine), fetch, 0)

    lane = lax.broadcasted_iota(jnp.int32, (SLOTS, span), 1)
    row = lax.broadcasted_iota(jnp.int32, (SLOTS, span), 0)
    for s in range(step_seqs):
        at = i * step_seqs + s
        pltpu.make_async_copy(wt_hbm.at[pl.ds(0, used), :], buf.at[at, pl.ds(0, used), :], sem.at[at]).wait()
    table = tab_ref[...]
    seq = lax.broadcasted_iota(jnp.int32, table.shape, 1)
    for s in range(step_seqs):
        mine = jnp.sum(jnp.where(seq == i * step_seqs + s, table, 0.0), axis=1, keepdims=True).astype(jnp.int32)
        pick = ((lane == row * ROWS + (mine & (ROWS - 1))) & (row < n_lab)).astype(jnp.bfloat16)
        rows_ref[s] = dot(pick, buf[i * step_seqs + s], NN).astype(rows_ref.dtype)
    for s in range(step_seqs):
        out_ref[s] = dot(rows_ref[s], enc_ref[s], NT)


def label_logits(lab_flat, scal, enc, table, wt_all, n_mine, n_lab):
    _, n_frames, depth = enc.shape
    step_seqs = GROUP
    steps = n_mine // step_seqs
    span = (n_lab * ROWS + 15) // 16 * 16
    return pl.pallas_call(
        functools.partial(label_kernel, n_lab, step_seqs),
        grid_spec=pltpu.PrefetchScalarGridSpec(
            num_scalar_prefetch=2,
            grid=(steps,),
            in_specs=[
                blocks((step_seqs, n_frames, depth), lambda i, lab, scal: scal[0] * steps + i),
                whole(*table.shape),
                in_place(),
            ],
            out_specs=(blocks((step_seqs, SLOTS, n_frames), lambda i, *_: i), blocks((step_seqs, SLOTS, depth), lambda i, *_: i)),
            scratch_shapes=[pltpu.VMEM((n_mine, span, depth), jnp.bfloat16), pltpu.SemaphoreType.DMA((n_mine,))],
        ),
        out_shape=(jax.ShapeDtypeStruct((n_mine, SLOTS, n_frames), jnp.float32), jax.ShapeDtypeStruct((n_mine, SLOTS, depth), jnp.bfloat16)),
        compiler_params=params(),
        cost_estimate=pl.CostEstimate(flops=2 * n_mine * n_lab * ROWS * n_frames * depth, bytes_accessed=4 * n_mine * n_lab * ROWS * depth, transcendentals=0),
        name="label_logits",
    )(lab_flat, scal, enc, table, wt_all)


def several(body, n, width):
    def run(i, carry):
        for j in range(width):
            carry = body(i * width + j, carry)
        return carry

    return 0, n // width, run


def lattice_kernel(n_lab, dup_ref, seq_ref, lse_ref, lab_ref, out_ref, loss_ref, zl_ref, gl_ref, turned, bb, lb, ll, bl, sl, occ):
    n_frames, n_seq = lse_ref.shape
    shape = lab_ref.shape
    slots = shape[0]
    slot = lax.broadcasted_iota(jnp.int32, shape, 0)
    for u in range(slots):
        zl_ref[pl.ds(u, n_frames, slots), :] = jnp.transpose(seq_ref[pl.ds(u, n_seq, slots), :])

    def at(t):
        return pl.ds(pl.multiple_of(t * slots, slots), slots)

    blank_slot = n_lab - 1
    lab = lab_ref[...]
    in_len = lab_ref[blank_slot:n_lab, :]
    lab_len = lab_ref[n_lab : n_lab + 1, :]
    skip = (slot > 0) & (lab != pltpu.roll(lab, 1, 0))
    first = slot < lab_len
    for v in range(blank_slot - 1):
        first = first & ((lab != lab_ref[v : v + 1, :]) | (slot <= v))
    first = (first & (slot < blank_slot)) | (slot == blank_slot)
    neg = jnp.full(shape, NEG_FILL, jnp.float32)

    def forward(t, carry):
        b, l = carry
        e = zl_ref[at(t), :] - lse_ref[pl.ds(t, 1), :]
        eb = e[blank_slot:n_lab, :]
        prev = jnp.where(slot == 0, neg, pltpu.roll(l, 1, 0))
        top_b = jnp.maximum(b, prev)
        x0 = jnp.exp(b - top_b)
        x1 = jnp.exp(prev - top_b)
        sum_b = x0 + x1
        hop = jnp.where(skip, prev, neg)
        top_l = jnp.maximum(jnp.maximum(l, b), hop)
        y0 = jnp.exp(l - top_l)
        y1 = jnp.exp(b - top_l)
        y2 = jnp.exp(hop - top_l)
        sum_l = y0 + y1 + y2
        inv_b = 1.0 / sum_b
        inv_l = 1.0 / sum_l
        bb[t] = x0 * inv_b
        lb[t] = x1 * inv_b
        ll[t] = y0 * inv_l
        bl[t] = y1 * inv_l
        sl[t] = y2 * inv_l
        live = t < in_len
        new_b = jnp.where(live, top_b + jnp.log(sum_b) + eb, b)
        new_l = jnp.where(live, top_l + jnp.log(sum_l) + e, l)
        return new_b, new_l

    b, l = lax.fori_loop(*several(forward, n_frames, 4), (jnp.where(slot == 0, 0.0, neg), neg))
    end_b = jnp.where(slot == lab_len, b, neg)
    end_l = jnp.where(slot == lab_len - 1, l, neg)
    top = jnp.max(jnp.maximum(end_b, end_l), axis=0, keepdims=True)
    total = jnp.sum(jnp.exp(end_b - top) + jnp.exp(end_l - top), axis=0, keepdims=True)
    log_like = top + jnp.log(total)
    loss_ref[...] = -log_like

    def backward(i, carry):
        t = n_frames - 1 - i
        gb, gl = carry
        live = t < in_len
        blank = jnp.sum(gb, axis=0, keepdims=True)
        occ[t] = jnp.where(live, jnp.where(slot < blank_slot, gl, jnp.where(slot == blank_slot, blank, 0.0)), 0.0)
        back = pltpu.roll(gb * lb[t] + gl * sl[t], shape[0] - 1, 0)
        new_b = gb * bb[t] + gl * bl[t]
        new_l = gl * ll[t] + back
        return jnp.where(live, new_b, gb), jnp.where(live, new_l, gl)

    lax.fori_loop(*several(backward, n_frames, 4), (jnp.exp(end_b - log_like), jnp.exp(end_l - log_like)))

    for v in range(1, blank_slot):

        @pl.when(dup_ref[v] > 0)
        def _():
            take = (lab == lab_ref[v : v + 1, :]) & first & (slot < v)

            def add(t, _):
                row = occ[t]
                occ[t] = row + jnp.where(take, row[v : v + 1, :], 0.0)
                return 0

            lax.fori_loop(0, n_frames, add, 0)

    def emit(t, _):
        p = jnp.exp(zl_ref[at(t), :] - lse_ref[pl.ds(t, 1), :])
        gl_ref[at(t), :] = jnp.where(first & (t < in_len), p - occ[t], 0.0)
        return 0

    lax.fori_loop(*several(emit, n_frames, 4), 0)
    turned[...] = jnp.zeros_like(turned)
    for u in range(n_lab):
        turned[pl.ds(u, n_seq, slots), :] = jnp.transpose(gl_ref[pl.ds(u, n_frames, slots), :])
    out_ref[...] = turned[...].astype(out_ref.dtype)


def lattice(dup, zl, lse, table, n_lab):
    n_seq, slots, n_frames = zl.shape
    by_frame = pltpu.VMEM((n_frames * slots, n_seq), jnp.float32)
    by_seq = (n_seq * slots, n_frames)
    gl, loss = pl.pallas_call(
        functools.partial(lattice_kernel, n_lab + 1),
        in_specs=[pl.BlockSpec(memory_space=pltpu.SMEM)] + [in_vmem()] * 3,
        out_specs=(in_vmem(), in_vmem()),
        out_shape=(jax.ShapeDtypeStruct(by_seq, jnp.bfloat16), jax.ShapeDtypeStruct((1, n_seq), jnp.float32)),
        scratch_shapes=[by_frame, by_frame, pltpu.VMEM(by_seq, jnp.float32)] + [pltpu.VMEM((n_frames, slots, n_seq), jnp.float32)] * 6,
        compiler_params=params(),
        cost_estimate=pl.CostEstimate(flops=2 * 10**10, bytes_accessed=2 * zl.size, transcendentals=0),
        name="lattice",
    )(dup, zl.reshape(by_seq), lse, table)
    return gl.reshape(zl.shape), loss


def place_start(recvs, out_ref, scal_ref, sem):
    step = pl.program_id(0)
    copies = []
    for i, ref in enumerate(recvs):
        n = ref.shape[0]
        row = pl.multiple_of(scal_ref[1 + i] + step * n, 8)
        copy = pltpu.make_async_copy(ref, out_ref.at[pl.ds(row, n), :], sem.at[i])
        copy.start()
        copies.append(copy)
    return copies


def hs_kernel(n_lab, n_recv, has_prev, scal_ref, enc_ref, wt_ref, lse_ref, slot_ref, gl_ref, rows_ref, *refs):
    recvs = refs[:n_recv]
    refs = refs[n_recv + has_prev :]
    out_ref, sy_ref, sz_ref, shift, sem_r = refs
    j = pl.program_id(0)
    n_seq, n_frames, depth = enc_ref.shape
    half = n_seq // 2
    placed = place_start(recvs, out_ref, scal_ref, sem_r)

    @pl.when(j == 0)
    def _():
        cols = jnp.transpose(lse_ref[0])
        for s in range(n_seq):
            shift[s] = jnp.broadcast_to(cols[:n_frames, s : s + 1], (n_frames, 128))
        for part, acc in ((0, sy_ref), (1, sz_ref)):
            for s in range(half):
                seq = part * half + s
                acc[s * n_frames : (s + 1) * n_frames, :] = dot(gl_ref[seq], rows_ref[seq], TN)

    w = wt_ref[...]
    width = w.shape[0]
    col = j * width + lax.broadcasted_iota(jnp.int32, (n_seq, width), 1)
    bias = jnp.zeros((n_seq, width), jnp.float32)
    for u in range(n_lab):
        bias = jnp.where(col == slot_ref[0, :, u : u + 1], NEG_FILL, bias)
    for part, acc in ((0, sy_ref), (1, sz_ref)):
        enc = enc_ref[part * half : (part + 1) * half].reshape(half * n_frames, depth)
        z = dot(enc, w, NT)
        ps = []
        for s in range(half):
            seq = part * half + s
            low = jnp.concatenate([shift[seq]] * (width // 128), axis=1)
            p = jnp.exp(z[s * n_frames : (s + 1) * n_frames, :] - low + bias[seq : seq + 1, :])
            ps.append(p.astype(jnp.bfloat16))
        p = jnp.concatenate(ps, axis=0)
        acc[...] += dot(p, w, NN)

    for copy in placed:
        copy.wait()


def hs_chunk(k, n_mine, n_lab, scal, enc, wt_all, lse, slots, gl, lab_rows, recvs, prev):
    n_batch, n_frames, depth = enc.shape
    n_vocab = wt_all.shape[0]
    width = HS_WIDTH if n_vocab >= 8192 else 128
    steps = n_vocab // width
    n_chunk = n_mine // CHUNK
    half_rows = CHUNK // 2 * n_frames
    in_specs = [
        blocks((CHUNK, n_frames, depth), lambda j, scal: scal[0] * n_chunk + k),
        blocks((width, depth), lambda j, scal: j),
        blocks((1,) + lse.shape[1:], lambda j, scal: scal[0] * n_chunk + k),
        blocks((1, CHUNK, SLOTS), lambda *_: k),
        blocks((CHUNK, SLOTS, n_frames), lambda *_: k),
        blocks((CHUNK, SLOTS, depth), lambda *_: k),
    ]
    in_specs += [blocks((r.shape[0] // steps, depth), lambda j, scal: j) for r in recvs]
    args = [scal, enc, wt_all, lse, slots, gl, lab_rows, *recvs]
    aliases = {}
    if prev is not None:
        in_specs.append(in_place())
        aliases = {len(args): 0}
        args.append(prev)
    send = jax.ShapeDtypeStruct((half_rows, depth), jnp.float32)
    rows = CHUNK * n_frames
    return pl.pallas_call(
        functools.partial(hs_kernel, n_lab, len(recvs), int(prev is not None)),
        grid_spec=pltpu.PrefetchScalarGridSpec(
            num_scalar_prefetch=1,
            grid=(steps,),
            in_specs=in_specs,
            out_specs=(in_place(), whole(half_rows, depth), whole(half_rows, depth)),
            scratch_shapes=[pltpu.VMEM((CHUNK, n_frames, 128), jnp.float32), pltpu.SemaphoreType.DMA((max(len(recvs), 1),))],
        ),
        out_shape=(jax.ShapeDtypeStruct((n_batch * n_frames, depth), jnp.float32), send, send),
        input_output_aliases=aliases,
        compiler_params=params(),
        cost_estimate=pl.CostEstimate(flops=4 * rows * depth * n_vocab, bytes_accessed=2 * n_vocab * depth, transcendentals=rows * n_vocab),
        name="hs_chunk",
    )(*args)


def gw_kernel(n_recv, is_first, is_last, scal_ref, enc_ref, z_ref, lse_ref, lab0_ref, gl0_ref, lab_ref, gl_ref, *refs):
    recvs = refs[:n_recv]
    acc_in = None if is_first else refs[n_recv]
    refs = refs[n_recv + (not is_first) + 1 :]
    out_ref, gw_ref, acc, fan, diag, part, sem_r = refs
    i = pl.program_id(0)
    n_seq, n_frames, depth = enc_ref.shape
    n_cols, rows = z_ref.shape
    placed = place_start(recvs, out_ref, scal_ref, sem_r)

    def fanned(gl):
        return (dot(gl[...].reshape(n_seq * SLOTS, n_frames), fan[...], NN) * diag[...]).astype(jnp.bfloat16)

    def label_part(lab, wide):
        col = scal_ref[0] + lax.broadcasted_iota(jnp.int32, (n_cols, n_seq * SLOTS), 0)
        return dot((col == lab[0]).astype(jnp.bfloat16), wide, NN).astype(jnp.bfloat16)

    @pl.when(i == 0)
    def _():
        seq_r = lax.div(lax.broadcasted_iota(jnp.int32, diag.shape, 0), SLOTS)
        seq_c = lax.div(lax.broadcasted_iota(jnp.int32, diag.shape, 1), n_frames)
        diag[...] = jnp.where(seq_r == seq_c, 1.0, 0.0)
        t_r = lax.broadcasted_iota(jnp.int32, fan.shape, 0)
        t_c = lax.rem(lax.broadcasted_iota(jnp.int32, fan.shape, 1), n_frames)
        fan[...] = (t_r == t_c).astype(jnp.bfloat16)
        if is_first:
            acc[...] = jnp.zeros_like(acc)
        else:
            acc[...] = acc_in[...]
        part[0] = label_part(lab0_ref, fanned(gl0_ref))

    now = lax.rem(i, 2)
    enc = enc_ref[...].reshape(rows, depth)
    half = depth // 2
    wide = fanned(gl_ref)
    g = jnp.exp(z_ref[...] - lse_ref[0]).astype(jnp.bfloat16) + part[now]
    acc[:, :half] += dot(g, enc[:, :half], NN)
    part[1 - now] = label_part(lab_ref, wide)
    acc[:, half:] += dot(g, enc[:, half:], NN)

    @pl.when(i == pl.num_programs(0) - 1)
    def _():
        gw_ref[...] = jnp.transpose(acc[...]) if is_last else acc[...]

    for copy in placed:
        copy.wait()


def gw_part(part, n_part, scal, enc, z, lse_rows, lab_rows, gl, recvs, acc, prev):
    n_batch, n_frames, depth = enc.shape
    n_cols = z.shape[0]
    steps = n_batch // GROUP // n_part
    base = part * steps
    rows = GROUP * n_frames
    is_first, is_last = part == 0, part == n_part - 1

    def here(i, scal):
        return base + i

    def then(i, scal):
        return base + jnp.minimum(i + 1, steps - 1)

    lab_block, gl_block = (1, 1, GROUP * SLOTS), (GROUP, SLOTS, n_frames)
    in_specs = [
        blocks((GROUP, n_frames, depth), here),
        pl.BlockSpec((n_cols, rows), lambda i, scal: (0, base + i)),
        blocks((1, 1, rows), here),
        blocks(lab_block, lambda *_: base),
        blocks(gl_block, lambda *_: base),
        blocks(lab_block, then),
        blocks(gl_block, then),
    ]
    in_specs += [blocks((r.shape[0] // steps, depth), lambda i, scal: i) for r in recvs]
    args = [scal, enc, z, lse_rows, lab_rows, gl, lab_rows, gl, *recvs]
    if not is_first:
        in_specs.append(whole(n_cols, depth))
        args.append(acc)
    in_specs.append(in_place())
    aliases = {len(args): 0}
    args.append(prev)
    shape = (depth, n_cols) if is_last else (n_cols, depth)
    return pl.pallas_call(
        functools.partial(gw_kernel, len(recvs), is_first, is_last),
        grid_spec=pltpu.PrefetchScalarGridSpec(
            num_scalar_prefetch=1,
            grid=(steps,),
            in_specs=in_specs,
            out_specs=(in_place(), whole(*shape)),
            scratch_shapes=[
                pltpu.VMEM((n_cols, depth), jnp.float32),
                pltpu.VMEM((n_frames, rows), jnp.bfloat16),
                pltpu.VMEM((GROUP * SLOTS, rows), jnp.float32),
                pltpu.VMEM((2, n_cols, rows), jnp.bfloat16),
                pltpu.SemaphoreType.DMA((max(len(recvs), 1),)),
            ],
        ),
        out_shape=(jax.ShapeDtypeStruct(prev.shape, jnp.float32), jax.ShapeDtypeStruct(shape, jnp.float32)),
        input_output_aliases=aliases,
        compiler_params=params(),
        cost_estimate=pl.CostEstimate(flops=2 * steps * rows * depth * n_cols, bytes_accessed=4 * steps * rows * n_cols, transcendentals=steps * rows * n_cols),
        name="gw_part",
    )(*args)


def place_kernel(n_recv, scal_ref, *refs):
    copies = place_start(refs[:n_recv], refs[n_recv + 1], scal_ref, refs[n_recv + 2])
    for copy in copies:
        copy.wait()


def place(scal, recvs, prev):
    depth = prev.shape[1]
    steps = 4
    in_specs = [blocks((r.shape[0] // steps, depth), lambda i, scal: i) for r in recvs] + [in_place()]
    return pl.pallas_call(
        functools.partial(place_kernel, len(recvs)),
        grid_spec=pltpu.PrefetchScalarGridSpec(
            num_scalar_prefetch=1, grid=(steps,), in_specs=in_specs, out_specs=in_place(), scratch_shapes=[pltpu.SemaphoreType.DMA((len(recvs),))]
        ),
        out_shape=jax.ShapeDtypeStruct(prev.shape, jnp.float32),
        input_output_aliases={1 + len(recvs): 0},
        compiler_params=params(),
        name="place",
    )(scal, *recvs, prev)


def solution(mesh):
    n_dev = mesh.shape["tp"]

    def swap(x, bit):
        return lax.ppermute(x, "tp", [(i, i ^ bit) for i in range(n_dev)])

    def device_fn(enc, w_loc, labels, in_len, lab_len):
        n_batch, n_frames, depth = enc.shape
        n_cols = w_loc.shape[1]
        n_lab = labels.shape[1]
        n_mine = n_batch // 4
        n_chunk = n_mine // CHUNK
        tp = lax.axis_index("tp")
        core = tp % 2
        colour = (tp // 2 + tp // 4) % 2
        mine = 2 * colour + core

        u = jnp.arange(n_lab)
        valid = u[None, :] < lab_len[:, None]
        earlier = (labels[:, :, None] == labels[:, None, :]) & (u[None, :] < u[:, None])[None]
        first = valid & ~jnp.any(earlier, axis=2)
        slot_lab = jnp.concatenate(
            [jnp.where(first, labels, -1), jnp.zeros((n_batch, 1), jnp.int32), jnp.full((n_batch, SLOTS - n_lab - 1), -1, jnp.int32)], axis=1
        )

        wt = w_loc.T
        wt_all, lse, z_loc = spread_projection(enc, wt, slot_lab, n_dev, mesh.shape["dp"])
        lse = lse.reshape(n_batch, n_frames)
        lse_live = jnp.where(jnp.arange(n_frames)[None, :] < in_len[:, None], lse, BIG)
        lse_pad = jnp.pad(lse_live.reshape(-1, CHUNK, n_frames), ((0, 0), (0, -CHUNK % 8), (0, 128 - n_frames)), constant_values=BIG)

        def take(x):
            return lax.dynamic_slice_in_dim(x, mine * n_mine, n_mine, axis=0)

        lab_m = take(labels)
        slot_m = take(slot_lab)
        ext_m = jnp.concatenate([lab_m, jnp.zeros((n_mine, SLOTS - n_lab), jnp.int32)], axis=1)
        table = jnp.concatenate([lab_m, take(in_len)[:, None], take(lab_len)[:, None], ext_m[:, n_lab + 2 :]], axis=1).T
        lab_cols = ext_m.T.astype(jnp.float32)
        dup = jnp.pad(jnp.any(take(valid & ~first), axis=0).astype(jnp.int32), (0, SLOTS - n_lab))

        zl, lab_proj = label_logits(ext_m[:, : n_lab + 1].reshape(-1), jnp.stack([mine, mine]).astype(jnp.int32), enc, lab_cols, wt_all, n_mine, n_lab + 1)
        gl_gw, loss_m = lattice(dup, zl, take(lse).T, table, n_lab)
        loss_m = loss_m[0]

        def spread(x):
            other = swap(x, 2)
            partner = swap(x, 1)
            last = swap(other, 1)
            out = jnp.zeros((4,) + x.shape, x.dtype)
            for value, where in ((x, mine), (other, mine ^ 2), (partner, mine ^ 1), (last, mine ^ 3)):
                out = lax.dynamic_update_index_in_dim(out, value, where, 0)
            return out.reshape((4 * x.shape[0],) + x.shape[1:])

        loss = spread(loss_m)
        gl_all = spread(gl_gw)

        set_rows = n_mine * n_frames
        half = CHUNK // 2 * n_frames
        moved = {}

        def rows_of(kinds):
            return [((mine ^ flip) * set_rows + k * CHUNK * n_frames + part * half) for k, part, flip in kinds]

        def scal_of(head, kinds):
            vals = [head] + rows_of(kinds)
            vals += [0] * (SLOTS // 2 - len(vals))
            return jnp.stack([jnp.asarray(v, jnp.int32) for v in vals])

        def arrived(*wanted):
            kinds = [(k, part, flip) for k, flip in wanted if 0 <= k < n_chunk for part in (0, 1)]
            return kinds, [moved[kind] for kind in kinds]

        def forward(k, after):
            for part in (0, 1):
                block = moved[(k, part, 2)]
                if after is not None:
                    block, after = lax.optimization_barrier((block, after))
                moved[(k, part, 3)] = swap(block, 1)
            return after

        def due(i):
            return arrived((i - 1, 0), (i - 2, 1), (i - 3, 2), (i - 4, 3))

        out = None
        for k in range(n_chunk):
            kinds, data = due(k)
            scal = scal_of(mine, kinds)
            if k == 2:
                scal, loss, gl_all = lax.optimization_barrier((scal, loss, gl_all))
            out, sy, sz = hs_chunk(k, n_mine, n_lab + 1, scal, enc, wt_all, lse_pad, slot_m.reshape(n_chunk, CHUNK, SLOTS), gl_gw, lab_proj, data, out)
            for part, x, bit in ((0, sy, 2), (1, sz, 4)):
                moved[(k, part, 0)] = x
                moved[(k, part, 1)] = swap(x, 1)
                moved[(k, part, 2)] = swap(x, bit)
            if k >= 2:
                forward(k - 2, None)

        lse_rows = lse_live.reshape(n_batch // GROUP, 1, GROUP * n_frames)
        lab_rows = slot_lab.reshape(n_batch // GROUP, 1, GROUP * SLOTS)
        acc = None
        n_part = 3
        for part in range(n_part):
            kinds, data = due(n_chunk + part) if part < n_part - 1 else arrived((n_chunk - 2, 3))
            out, acc = gw_part(part, n_part, scal_of(tp * n_cols, kinds), enc, z_loc, lse_rows, lab_rows, gl_all, data, acc, out)
            if part < n_part - 1:
                acc = forward(n_chunk + part - 2, acc)
        kinds, data = arrived((n_chunk - 1, 2), (n_chunk - 1, 3))
        out = place(scal_of(tp, kinds), data, out)
        return loss, acc, out.reshape(n_batch, n_frames, depth)

    return jax.shard_map(
        device_fn,
        mesh=mesh,
        in_specs=(P("dp"), P(None, "tp"), P("dp"), P("dp"), P("dp")),
        out_specs=(P("dp"), P("dp", "tp"), P("dp")),
        check_vma=False,
    )
```

```python
import functools

import jax
import jax.numpy as jnp
from jax import lax
from jax.experimental import pallas as pl
from jax.experimental.pallas import tpu as pltpu
from jax.sharding import PartitionSpec as P


NEG_FILL = -1.0e30
BIG = 1.0e30
MESH = pl.DeviceIdType.MESH
NT = (((1,), (1,)), ((), ()))
NN = (((1,), (0,)), ((), ()))
TN = (((0,), (0,)), ((), ()))
SLOTS = 32
ROWS = 8
HS_WIDTH = 1024
UNIT = 6
PLACE = 72
GROUP = 8
GW_SPLIT = 4
VMEM_LIMIT = 60 * 1024 * 1024


def dot(a, b, dims):
    return lax.dot_general(a, b, dims, preferred_element_type=jnp.float32)


def whole(*shape):
    return pl.BlockSpec(shape, lambda *_: (0,) * len(shape))


def blocks(shape, first):
    return pl.BlockSpec(shape, lambda *g: (first(*g),) + (0,) * (len(shape) - 1))


def in_place():
    return pl.BlockSpec(memory_space=pl.ANY)


def in_vmem():
    return pl.BlockSpec(memory_space=pltpu.VMEM)


def params(**kw):
    return pltpu.CompilerParams(vmem_limit_bytes=VMEM_LIMIT, **kw)


SUBS = 8
N_Z = 4
HOPS = SUBS * (N_Z - 1)
LAG_Y, LAG_X = 2, 4
IDS = SUBS + 2 * HOPS


def spread_kernel(n_dev, n_dp, enc_hbm, w_ref, lab_ref, all_ref, lse_ref, z_hbm, *scratch):
    encbuf, st, recv, mine, bias, zbuf, enc_sem, own_sem, z_sem, *sems = scratch
    dn_send, dn_recv, up_send, up_recv, y_send, y_recv, x_send, x_recv, v_send, v_recv, c_send, c_recv, s1_send, s1_recv, s2_send, s2_recv = sems
    dp = lax.axis_index("dp")
    tp = lax.axis_index("tp")
    core = lax.rem(tp, 2)
    z = lax.div(tp, 4)
    mate = tp + 1 - 2 * core
    across = tp + 2 - 4 * lax.rem(lax.div(tp, 2), 2)
    block = w_ref.shape[0]
    piece = block // SUBS
    crosses = (core == dp) if n_dp > 1 else (core >= 0)
    n_seq, n_frames, depth = encbuf.shape[1:]

    def rows(owner, s):
        return all_ref.at[pl.ds(pl.multiple_of(owner * block + s * piece, piece), piece), :]

    def move(src, owner, s, send, got, dst):
        return pltpu.make_async_remote_copy(src_ref=src, dst_ref=rows(owner, s), send_sem=send, recv_sem=got, device_id=dst, device_id_type=MESH)

    def to(dev):
        return {"tp": dev}

    beside = {"dp": 1 - dp} if n_dp > 1 else to(tp)

    def owner_of(base, kind, q):
        hop = lax.div(q, SUBS) + 1
        return base + (4 * hop if kind == 1 else -4 * hop)

    def there(kind, q):
        hop = lax.div(q, SUBS) + 1
        return (q >= 0) & (q < HOPS) & ((z + hop <= N_Z - 1) if kind == 1 else (z - hop >= 0))

    def by_z(q):
        return (q < HOPS - SUBS) | crosses if n_dp > 1 else q >= 0

    barrier = pltpu.get_barrier_semaphore()
    for d in range(1, n_dev):
        pl.semaphore_signal(barrier, inc=1, device_id={"tp": lax.rem(tp + d, n_dev)}, device_id_type=MESH)
    if n_dp > 1:
        pl.semaphore_signal(barrier, inc=1, device_id=beside, device_id_type=MESH)
    pl.semaphore_wait(barrier, n_dev - 1 + (n_dp > 1))

    own = pltpu.make_async_copy(w_ref, all_ref.at[pl.ds(pl.multiple_of(tp * block, block), block), :], own_sem)
    own.start()

    def own_moves(s):
        src = w_ref.at[pl.ds(pl.multiple_of(s * piece, piece), piece), :]
        return (
            (z >= 1, move(src, tp, s, dn_send.at[s], dn_recv.at[s], to(tp - 4))),
            (z <= N_Z - 2, move(src, tp, s, up_send.at[s], up_recv.at[s], to(tp + 4))),
            (crosses, move(src, tp, s, y_send.at[s], y_recv.at[s], to(across))),
            (z >= 0, move(src, tp, s, c_send.at[s], c_recv.at[s], to(mate))),
        )

    def z_moves(kind, q):
        owner = owner_of(tp, kind, q)
        s = lax.rem(q, SUBS)
        src = rows(owner, s)
        got = dn_recv if kind == 1 else up_recv
        send = dn_send if kind == 1 else up_send
        number = SUBS + q + (0 if kind == 1 else HOPS)
        last = (z >= 1) if kind == 1 else (z <= N_Z - 2)
        nxt = lax.rem(q + SUBS, HOPS)
        here = there(kind, q) & by_z(q)
        return (
            here,
            move(src, owner, s, send.at[SUBS + q], got.at[q], to(tp)),
            (
                (here & last & by_z(q + SUBS), move(src, owner, s, send.at[SUBS + q], got.at[nxt], to(tp - 4 if kind == 1 else tp + 4))),
                (here, move(src, owner, s, c_send.at[number], c_recv.at[number], to(mate))),
                (here & crosses, move(src, owner, s, y_send.at[number], y_recv.at[number], to(across))),
                (here & (q >= HOPS - SUBS) & (n_dp > 1), move(src, owner, s, v_send.at[number], v_recv.at[number], beside)),
            ),
        )

    def v_moves(kind, q):
        q0 = lax.rem(q + HOPS, HOPS)
        owner, s, number = owner_of(tp, kind, q0), lax.rem(q0, SUBS), SUBS + q0 + (0 if kind == 1 else HOPS)
        src = rows(owner, s)
        here = there(kind, q) & jnp.logical_not(by_z(q))
        return (
            here,
            move(src, owner, s, v_send.at[number], v_recv.at[number], to(tp)),
            ((here, move(src, owner, s, c_send.at[number], c_recv.at[number], to(mate))),),
        )

    def far_parts(kind, q):
        if kind == 0:
            q0 = lax.rem(q + SUBS, SUBS)
            return across, q0, q0, (q >= 0) & (q < SUBS)
        q0 = lax.rem(q + HOPS, HOPS)
        return owner_of(across, kind, q0), lax.rem(q0, SUBS), SUBS + q0 + (0 if kind == 1 else HOPS), there(kind, q)

    def y_moves(kind, q):
        owner, s, number, here = far_parts(kind, q)
        src = rows(owner, s)
        return (
            here & crosses,
            move(src, owner, s, y_send.at[number], y_recv.at[number], to(tp)),
            (
                (here & crosses & (n_dp > 1), move(src, owner, s, x_send.at[number], x_recv.at[number], beside)),
                (here & crosses, move(src, owner, s, c_send.at[IDS + number], c_recv.at[IDS + number], to(mate))),
            ),
        )

    def x_moves(kind, q):
        owner, s, number, here = far_parts(kind, q)
        src = rows(owner, s)
        return (
            here & jnp.logical_not(crosses),
            move(src, owner, s, x_send.at[number], x_recv.at[number], to(tp)),
            ((here & jnp.logical_not(crosses), move(src, owner, s, c_send.at[IDS + number], c_recv.at[IDS + number], to(mate))),),
        )

    def start_all(moves):
        for cond, copy in moves:

            @pl.when(cond)
            def _():
                copy.start()

    def relay(group):
        cond, arrival, moves = group

        @pl.when(cond)
        def _():
            arrival.wait_recv()

        start_all(moves)

    def service(q):
        for kind in (1, 2):
            relay(z_moves(kind, q))
        relay(y_moves(0, jnp.minimum(q - 1, SUBS)))
        for kind in (1, 2):
            relay(y_moves(kind, q - LAG_Y))
        if n_dp > 1:
            for kind in (1, 2):
                relay(v_moves(kind, q - LAG_Y))
            relay(x_moves(0, jnp.minimum(q + 1 - LAG_X, SUBS)))
            for kind in (1, 2):
                relay(x_moves(kind, q - LAG_X))

    def enc_copy(i):
        slot = lax.rem(i, 2)
        return pltpu.make_async_copy(enc_hbm.at[pl.ds(i * n_seq, n_seq)], encbuf.at[slot], enc_sem.at[slot])

    def z_copy(i):
        slot = lax.rem(i, 2)
        size = n_seq * n_frames
        return pltpu.make_async_copy(zbuf.at[slot], z_hbm.at[:, pl.ds(pl.multiple_of(i * size, 128), size)], z_sem.at[slot])

    enc_copy(0).start()
    for s in range(SUBS):
        start_all(own_moves(s))
    seq_r = lax.div(lax.broadcasted_iota(jnp.int32, bias.shape, 0), SLOTS)
    seq_c = lax.div(lax.broadcasted_iota(jnp.int32, bias.shape, 1), n_frames)
    bias[...] = jnp.where(seq_r == seq_c, NEG_FILL, 0.0).astype(bias.dtype)
    col = tp * block + lax.broadcasted_iota(jnp.int32, (block, n_seq * SLOTS), 0)

    busy = min(2 * SUBS, n_dev)
    per = n_dev // busy

    def tile(i, carry):
        enc_copy(i).wait()

        @pl.when(i + 1 < n_dev)
        def _():
            enc_copy(i + 1).start()

        slot = lax.rem(i, 2)
        enc = encbuf[slot].reshape(n_seq * n_frames, depth)
        zt = dot(w_ref[...], enc, NT)
        top = jnp.max(zt, axis=0, keepdims=True)
        st[i, 0:1, :] = top
        st[i, 1:2, :] = jnp.sum(jnp.exp(zt - top), axis=0, keepdims=True)

        @pl.when(i >= 2)
        def _():
            z_copy(i - 2).wait()

        hot = (col == lab_ref[i]).astype(jnp.bfloat16)
        zbuf[slot] = zt + dot(hot, bias[...], NN)
        z_copy(i).start()
        return carry

    def with_tiles(q, carry):
        lax.fori_loop(q * per, (q + 1) * per, tile, 0)
        service(q)
        return carry

    def plain(q, carry):
        service(q)
        return carry

    lax.fori_loop(0, busy, with_tiles, 0)
    first = []
    for d in range(1, n_dev):
        peer = lax.rem(tp + d, n_dev)
        first.append(
            pltpu.make_async_remote_copy(
                src_ref=st.at[peer], dst_ref=recv.at[tp], send_sem=s1_send.at[d], recv_sem=s1_recv.at[d], device_id=to(peer), device_id_type=MESH
            )
        )
    for copy in first:
        copy.start()
    recv[tp] = st[tp]
    lax.fori_loop(busy, busy + 1, plain, 0)
    for copy in first:
        copy.wait()
    top = recv[0, 0:1, :]
    for j in range(1, n_dev):
        top = jnp.maximum(top, recv[j, 0:1, :])
    total = jnp.zeros_like(top)
    for j in range(n_dev):
        total = total + recv[j, 1:2, :] * jnp.exp(recv[j, 0:1, :] - top)
    lse = top + jnp.log(total)
    mine[...] = lse
    lse_ref[tp] = lse
    second = []
    for d in range(1, n_dev):
        peer = lax.rem(tp + d, n_dev)
        second.append(
            pltpu.make_async_remote_copy(
                src_ref=mine, dst_ref=lse_ref.at[tp], send_sem=s2_send.at[d], recv_sem=s2_recv.at[d], device_id=to(peer), device_id_type=MESH
            )
        )
    for copy in second:
        copy.start()
    lax.fori_loop(busy + 1, HOPS, plain, 0)

    def late(q, carry):
        for kind in (1, 2):
            relay(y_moves(kind, q - LAG_Y))
            if n_dp > 1:
                relay(v_moves(kind, q - LAG_Y))
                relay(x_moves(kind, q - LAG_X))
        return carry

    lax.fori_loop(HOPS, HOPS + LAG_X, late, 0)
    for copy in second:
        copy.wait()
    own.wait()
    for i in (n_dev - 2, n_dev - 1):
        z_copy(i).wait()

    def drain(cond, copy):
        @pl.when(cond)
        def _():
            copy.wait_send()

    def finish_own(s, carry):
        for cond, copy in own_moves(s):
            drain(cond, copy)
        move(rows(mate, s), mate, s, c_send.at[s], c_recv.at[s], to(tp)).wait_recv()
        far = mate + across - tp
        move(rows(far, s), far, s, c_send.at[IDS + s], c_recv.at[IDS + s], to(tp)).wait_recv()
        for _, _, moves in (y_moves(0, s), x_moves(0, s)) if n_dp > 1 else (y_moves(0, s),):
            for cond, copy in moves:
                drain(cond, copy)
        return carry

    def finish(q, carry):
        for kind in (1, 2):
            here = there(kind, q)
            groups = (z_moves(kind, q), y_moves(kind, q))
            if n_dp > 1:
                groups += (v_moves(kind, q), x_moves(kind, q))
            for _, _, moves in groups:
                for cond, copy in moves:
                    drain(cond, copy)
            number = SUBS + q + (0 if kind == 1 else HOPS)
            s = lax.rem(q, SUBS)

            @pl.when(here)
            def _():
                near = owner_of(mate, kind, q)
                move(rows(near, s), near, s, c_send.at[number], c_recv.at[number], to(tp)).wait_recv()
                far = owner_of(mate + across - tp, kind, q)
                move(rows(far, s), far, s, c_send.at[IDS + number], c_recv.at[IDS + number], to(tp)).wait_recv()

        return carry

    lax.fori_loop(0, SUBS, finish_own, 0)
    lax.fori_loop(0, HOPS, finish, 0)


def spread_projection(enc, wt, slot_lab, n_dev, n_dp):
    n_batch, n_frames, depth = enc.shape
    n_cols = wt.shape[0]
    n_seq = n_batch // n_dev
    rows = n_seq * n_frames
    dma = pltpu.SemaphoreType.DMA
    sems = [SUBS + HOPS, HOPS] * 2 + [IDS] * 6 + [2 * IDS] * 2 + [n_dev] * 4
    return pl.pallas_call(
        functools.partial(spread_kernel, n_dev, n_dp),
        in_specs=[in_place(), in_vmem(), in_vmem()],
        out_specs=(in_place(), in_vmem(), in_place()),
        out_shape=(
            jax.ShapeDtypeStruct((n_dev * n_cols, depth), wt.dtype),
            jax.ShapeDtypeStruct((n_dev, 1, rows), jnp.float32),
            jax.ShapeDtypeStruct((n_cols, n_batch * n_frames), jnp.float32),
        ),
        scratch_shapes=[
            pltpu.VMEM((2, n_seq, n_frames, depth), enc.dtype),
            pltpu.VMEM((n_dev, 2, rows), jnp.float32),
            pltpu.VMEM((n_dev, 2, rows), jnp.float32),
            pltpu.VMEM((1, rows), jnp.float32),
            pltpu.VMEM((n_seq * SLOTS, rows), jnp.bfloat16),
            pltpu.VMEM((2, n_cols, rows), jnp.float32),
            dma((2,)),
            dma,
            dma((2,)),
            *[dma((n,)) for n in sems],
        ],
        compiler_params=params(collective_id=0, has_side_effects=True),
        cost_estimate=pl.CostEstimate(flops=2 * n_batch * n_frames * depth * n_cols, bytes_accessed=2 * enc.size, transcendentals=0),
        name="spread_projection",
    )(enc, wt, slot_lab.reshape(n_dev, 1, n_seq * SLOTS))


def label_kernel(n_lab, step_seqs, lab_ref, scal_ref, enc_ref, tab_ref, wt_hbm, out_ref, rows_ref, buf, sem):
    i = pl.program_id(0)
    n_mine, span, depth = buf.shape
    used = n_lab * ROWS

    def fetch(s, carry):
        for u in range(n_lab):
            base = pl.multiple_of(lab_ref[s * n_lab + u] & -ROWS, ROWS)
            pltpu.make_async_copy(wt_hbm.at[pl.ds(base, ROWS), :], buf.at[s, pl.ds(u * ROWS, ROWS), :], sem.at[s]).start()
        return carry

    ahead = 2 * step_seqs

    @pl.when(i == 0)
    def _():
        lax.fori_loop(0, jnp.minimum(ahead, n_mine), fetch, 0)
        buf[:, used:, :] = jnp.zeros((n_mine, span - used, depth), buf.dtype)

    lax.fori_loop(jnp.minimum(i * step_seqs + ahead, n_mine), jnp.minimum((i + 1) * step_seqs + ahead, n_mine), fetch, 0)

    lane = lax.broadcasted_iota(jnp.int32, (SLOTS, span), 1)
    row = lax.broadcasted_iota(jnp.int32, (SLOTS, span), 0)
    for s in range(step_seqs):
        at = i * step_seqs + s
        pltpu.make_async_copy(wt_hbm.at[pl.ds(0, used), :], buf.at[at, pl.ds(0, used), :], sem.at[at]).wait()
    table = tab_ref[...]
    seq = lax.broadcasted_iota(jnp.int32, table.shape, 1)
    for s in range(step_seqs):
        mine = jnp.sum(jnp.where(seq == i * step_seqs + s, table, 0.0), axis=1, keepdims=True).astype(jnp.int32)
        pick = ((lane == row * ROWS + (mine & (ROWS - 1))) & (row < n_lab)).astype(jnp.bfloat16)
        rows_ref[s] = dot(pick, buf[i * step_seqs + s], NN).astype(rows_ref.dtype)
    for s in range(step_seqs):
        out_ref[s] = dot(rows_ref[s], enc_ref[s], NT)


def label_logits(lab_flat, scal, enc, table, wt_all, n_mine, n_lab):
    _, n_frames, depth = enc.shape
    step_seqs = GROUP
    steps = n_mine // step_seqs
    span = (n_lab * ROWS + 15) // 16 * 16
    return pl.pallas_call(
        functools.partial(label_kernel, n_lab, step_seqs),
        grid_spec=pltpu.PrefetchScalarGridSpec(
            num_scalar_prefetch=2,
            grid=(steps,),
            in_specs=[
                blocks((step_seqs, n_frames, depth), lambda i, lab, scal: scal[0] * steps + i),
                whole(*table.shape),
                in_place(),
            ],
            out_specs=(blocks((step_seqs, SLOTS, n_frames), lambda i, *_: i), blocks((step_seqs, SLOTS, depth), lambda i, *_: i)),
            scratch_shapes=[pltpu.VMEM((n_mine, span, depth), jnp.bfloat16), pltpu.SemaphoreType.DMA((n_mine,))],
        ),
        out_shape=(jax.ShapeDtypeStruct((n_mine, SLOTS, n_frames), jnp.float32), jax.ShapeDtypeStruct((n_mine, SLOTS, depth), jnp.bfloat16)),
        compiler_params=params(),
        cost_estimate=pl.CostEstimate(flops=2 * n_mine * n_lab * ROWS * n_frames * depth, bytes_accessed=4 * n_mine * n_lab * ROWS * depth, transcendentals=0),
        name="label_logits",
    )(lab_flat, scal, enc, table, wt_all)


def several(body, n, width):
    def run(i, carry):
        for j in range(width):
            carry = body(i * width + j, carry)
        return carry

    return 0, n // width, run


def lattice_kernel(n_lab, dup_ref, seq_ref, lse_ref, lab_ref, out_ref, loss_ref, zl_ref, gl_ref, turned, bb, lb, ll, bl, sl, occ):
    n_frames, n_seq = lse_ref.shape
    shape = lab_ref.shape
    slots = shape[0]
    slot = lax.broadcasted_iota(jnp.int32, shape, 0)
    for u in range(slots):
        zl_ref[pl.ds(u, n_frames, slots), :] = jnp.transpose(seq_ref[pl.ds(u, n_seq, slots), :])

    def at(t):
        return pl.ds(pl.multiple_of(t * slots, slots), slots)

    blank_slot = n_lab - 1
    lab = lab_ref[...]
    in_len = lab_ref[blank_slot:n_lab, :]
    lab_len = lab_ref[n_lab : n_lab + 1, :]
    skip = (slot > 0) & (lab != pltpu.roll(lab, 1, 0))
    first = slot < lab_len
    for v in range(blank_slot - 1):
        first = first & ((lab != lab_ref[v : v + 1, :]) | (slot <= v))
    first = (first & (slot < blank_slot)) | (slot == blank_slot)
    neg = jnp.full(shape, NEG_FILL, jnp.float32)

    def forward(t, carry):
        b, l = carry
        e = zl_ref[at(t), :] - lse_ref[pl.ds(t, 1), :]
        eb = e[blank_slot:n_lab, :]
        prev = jnp.where(slot == 0, neg, pltpu.roll(l, 1, 0))
        top_b = jnp.maximum(b, prev)
        x0 = jnp.exp(b - top_b)
        x1 = jnp.exp(prev - top_b)
        sum_b = x0 + x1
        hop = jnp.where(skip, prev, neg)
        top_l = jnp.maximum(jnp.maximum(l, b), hop)
        y0 = jnp.exp(l - top_l)
        y1 = jnp.exp(b - top_l)
        y2 = jnp.exp(hop - top_l)
        sum_l = y0 + y1 + y2
        inv_b = 1.0 / sum_b
        inv_l = 1.0 / sum_l
        bb[t] = x0 * inv_b
        lb[t] = x1 * inv_b
        ll[t] = y0 * inv_l
        bl[t] = y1 * inv_l
        sl[t] = y2 * inv_l
        live = t < in_len
        new_b = jnp.where(live, top_b + jnp.log(sum_b) + eb, b)
        new_l = jnp.where(live, top_l + jnp.log(sum_l) + e, l)
        return new_b, new_l

    b, l = lax.fori_loop(*several(forward, n_frames, 4), (jnp.where(slot == 0, 0.0, neg), neg))
    end_b = jnp.where(slot == lab_len, b, neg)
    end_l = jnp.where(slot == lab_len - 1, l, neg)
    top = jnp.max(jnp.maximum(end_b, end_l), axis=0, keepdims=True)
    total = jnp.sum(jnp.exp(end_b - top) + jnp.exp(end_l - top), axis=0, keepdims=True)
    log_like = top + jnp.log(total)
    loss_ref[...] = -log_like

    def backward(i, carry):
        t = n_frames - 1 - i
        gb, gl = carry
        live = t < in_len
        blank = jnp.sum(gb, axis=0, keepdims=True)
        occ[t] = jnp.where(live, jnp.where(slot < blank_slot, gl, jnp.where(slot == blank_slot, blank, 0.0)), 0.0)
        back = pltpu.roll(gb * lb[t] + gl * sl[t], shape[0] - 1, 0)
        new_b = gb * bb[t] + gl * bl[t]
        new_l = gl * ll[t] + back
        return jnp.where(live, new_b, gb), jnp.where(live, new_l, gl)

    lax.fori_loop(*several(backward, n_frames, 4), (jnp.exp(end_b - log_like), jnp.exp(end_l - log_like)))

    for v in range(1, blank_slot):

        @pl.when(dup_ref[v] > 0)
        def _():
            take = (lab == lab_ref[v : v + 1, :]) & first & (slot < v)

            def add(t, _):
                row = occ[t]
                occ[t] = row + jnp.where(take, row[v : v + 1, :], 0.0)
                return 0

            lax.fori_loop(0, n_frames, add, 0)

    def emit(t, _):
        p = jnp.exp(zl_ref[at(t), :] - lse_ref[pl.ds(t, 1), :])
        gl_ref[at(t), :] = jnp.where(first & (t < in_len), p - occ[t], 0.0)
        return 0

    lax.fori_loop(*several(emit, n_frames, 4), 0)
    turned[...] = jnp.zeros_like(turned)
    for u in range(n_lab):
        turned[pl.ds(u, n_seq, slots), :] = jnp.transpose(gl_ref[pl.ds(u, n_frames, slots), :])
    out_ref[...] = turned[...].astype(out_ref.dtype)


def lattice(dup, zl, lse, table, n_lab):
    n_seq, slots, n_frames = zl.shape
    by_frame = pltpu.VMEM((n_frames * slots, n_seq), jnp.float32)
    by_seq = (n_seq * slots, n_frames)
    gl, loss = pl.pallas_call(
        functools.partial(lattice_kernel, n_lab + 1),
        in_specs=[pl.BlockSpec(memory_space=pltpu.SMEM)] + [in_vmem()] * 3,
        out_specs=(in_vmem(), in_vmem()),
        out_shape=(jax.ShapeDtypeStruct(by_seq, jnp.bfloat16), jax.ShapeDtypeStruct((1, n_seq), jnp.float32)),
        scratch_shapes=[by_frame, by_frame, pltpu.VMEM(by_seq, jnp.float32)] + [pltpu.VMEM((n_frames, slots, n_seq), jnp.float32)] * 6,
        compiler_params=params(),
        cost_estimate=pl.CostEstimate(flops=2 * 10**10, bytes_accessed=2 * zl.size, transcendentals=0),
        name="lattice",
    )(dup, zl.reshape(by_seq), lse, table)
    return gl.reshape(zl.shape), loss


def place_specs(recvs):
    return [blocks((PLACE, r.shape[1]), lambda i, scal, last=r.shape[0] // PLACE - 1: jnp.minimum(i, last)) for r in recvs]


def place_start(recvs, out_ref, scal_ref, sem):
    step = pl.program_id(0)
    copies = []
    for i, (ref, total) in enumerate(recvs):
        n = ref.shape[0]
        row = pl.multiple_of(scal_ref[1 + i] + jnp.minimum(step, total // n - 1) * n, 8)
        copy = pltpu.make_async_copy(ref, out_ref.at[pl.ds(row, n), :], sem.at[i])
        copy.start()
        copies.append(copy)
    return copies


def hs_kernel(n_lab, totals, has_prev, scal_ref, enc_ref, w0_ref, w1_ref, lse_ref, slot_ref, gl_ref, rows_ref, *refs):
    recvs = tuple(zip(refs, totals))
    refs = refs[len(totals) + has_prev :]
    out_ref, sy_ref, sz_ref, shift, sem_r = refs
    j = pl.program_id(0)
    n_seq, n_frames, depth = enc_ref.shape
    half = n_seq // 2
    placed = place_start(recvs, out_ref, scal_ref, sem_r)

    @pl.when(j == 0)
    def _():
        for unit in range(n_seq // UNIT):
            cols = jnp.transpose(lse_ref[unit])
            for s in range(UNIT):
                shift[unit * UNIT + s] = jnp.broadcast_to(cols[:n_frames, s : s + 1], (n_frames, 128))
        for part, acc in ((0, sy_ref), (1, sz_ref)):
            for s in range(half):
                seq = part * half + s
                acc[s * n_frames : (s + 1) * n_frames, :] = dot(gl_ref[seq], rows_ref[seq], TN)

    w = jnp.concatenate([w0_ref[...], w1_ref[...]], axis=0)
    width = w.shape[0]
    col = j * width + lax.broadcasted_iota(jnp.int32, (UNIT, width), 1)
    biases = []
    for unit in range(n_seq // UNIT):
        bias = jnp.zeros((UNIT, width), jnp.float32)
        for u in range(n_lab):
            bias = jnp.where(col == slot_ref[unit, :, u : u + 1], NEG_FILL, bias)
        biases.append(bias)
    for part, acc in ((0, sy_ref), (1, sz_ref)):
        enc = enc_ref[part * half : (part + 1) * half].reshape(half * n_frames, depth)
        z = dot(enc, w, NT)
        ps = []
        for s in range(half):
            seq = part * half + s
            low = jnp.concatenate([shift[seq]] * (width // 128), axis=1)
            row = seq % UNIT
            p = jnp.exp(z[s * n_frames : (s + 1) * n_frames, :] - low + biases[seq // UNIT][row : row + 1, :])
            ps.append(p.astype(jnp.bfloat16))
        p = jnp.concatenate(ps, axis=0)
        acc[...] += dot(p, w, NN)

    for copy in placed:
        copy.wait()


def hs_chunk(off, size, n_mine, n_lab, scal, enc, wt_all, lse, slots, gl, lab_rows, recvs, prev):
    n_batch, n_frames, depth = enc.shape
    n_vocab = wt_all.shape[0]
    width = HS_WIDTH if n_vocab >= 8192 else 128
    steps = n_vocab // width
    per_set, k, units = n_mine // size, off // size, size // UNIT
    half_rows = size // 2 * n_frames

    def here(j, scal):
        return scal[0] * per_set + k

    in_specs = [
        blocks((size, n_frames, depth), here),
        blocks((width // 2, depth), lambda j, scal: 2 * j),
        blocks((width // 2, depth), lambda j, scal: 2 * j + 1),
        blocks((units,) + lse.shape[1:], here),
        blocks((units,) + slots.shape[1:], lambda *_: k),
        blocks((size, SLOTS, n_frames), lambda *_: k),
        blocks((size, SLOTS, depth), lambda *_: k),
    ]
    in_specs += place_specs(recvs)
    args = [scal, enc, wt_all, wt_all, lse, slots, gl, lab_rows, *recvs]
    aliases = {}
    if prev is not None:
        in_specs.append(in_place())
        aliases = {len(args): 0}
        args.append(prev)
    send = jax.ShapeDtypeStruct((half_rows, depth), jnp.float32)
    rows = size * n_frames
    return pl.pallas_call(
        functools.partial(hs_kernel, n_lab, [r.shape[0] for r in recvs], int(prev is not None)),
        grid_spec=pltpu.PrefetchScalarGridSpec(
            num_scalar_prefetch=1,
            grid=(steps,),
            in_specs=in_specs,
            out_specs=(in_place(), whole(half_rows, depth), whole(half_rows, depth)),
            scratch_shapes=[pltpu.VMEM((size, n_frames, 128), jnp.float32), pltpu.SemaphoreType.DMA((max(len(recvs), 1),))],
        ),
        out_shape=(jax.ShapeDtypeStruct((n_batch * n_frames, depth), jnp.float32), send, send),
        input_output_aliases=aliases,
        compiler_params=params(),
        cost_estimate=pl.CostEstimate(flops=4 * rows * depth * n_vocab, bytes_accessed=2 * n_vocab * depth, transcendentals=rows * n_vocab),
        name="hs_chunk",
    )(*args)


def gw_kernel(totals, is_first, is_last, scal_ref, *refs):
    enc_refs, z_refs = refs[:GW_SPLIT], refs[GW_SPLIT : 2 * GW_SPLIT]
    lse_ref, lab0_ref, gl0_ref, lab_ref, gl_ref, *refs = refs[2 * GW_SPLIT :]
    n_recv = len(totals)
    recvs = tuple(zip(refs, totals))
    acc_in = None if is_first else refs[n_recv]
    refs = refs[n_recv + (not is_first) + 1 :]
    out_ref, gw_ref, acc, fan, diag, part, sem_r = refs
    i = pl.program_id(0)
    n_seq, n_frames, depth = enc_refs[0].shape
    n_seq *= GW_SPLIT
    n_cols, rows = acc.shape[0], n_seq * n_frames
    placed = place_start(recvs, out_ref, scal_ref, sem_r)

    def fanned(gl):
        return (dot(gl[...].reshape(n_seq * SLOTS, n_frames), fan[...], NN) * diag[...]).astype(jnp.bfloat16)

    def label_part(lab, wide):
        col = scal_ref[0] + lax.broadcasted_iota(jnp.int32, (n_cols, n_seq * SLOTS), 0)
        return dot((col == lab[0]).astype(jnp.bfloat16), wide, NN).astype(jnp.bfloat16)

    @pl.when(i == 0)
    def _():
        seq_r = lax.div(lax.broadcasted_iota(jnp.int32, diag.shape, 0), SLOTS)
        seq_c = lax.div(lax.broadcasted_iota(jnp.int32, diag.shape, 1), n_frames)
        diag[...] = jnp.where(seq_r == seq_c, 1.0, 0.0)
        t_r = lax.broadcasted_iota(jnp.int32, fan.shape, 0)
        t_c = lax.rem(lax.broadcasted_iota(jnp.int32, fan.shape, 1), n_frames)
        fan[...] = (t_r == t_c).astype(jnp.bfloat16)
        if is_first:
            acc[...] = jnp.zeros_like(acc)
        else:
            acc[...] = acc_in[...]
        part[0] = label_part(lab0_ref, fanned(gl0_ref))

    now = lax.rem(i, 2)
    enc = jnp.concatenate([ref[...].reshape(-1, depth) for ref in enc_refs], axis=0)
    half = depth // 2
    wide = fanned(gl_ref)
    p = jnp.concatenate([jnp.exp(ref[...] - lse_ref[0]).astype(jnp.bfloat16) for ref in z_refs], axis=0)
    g = p + part[now]
    acc[:, :half] += dot(g, enc[:, :half], NN)
    part[1 - now] = label_part(lab_ref, wide)
    acc[:, half:] += dot(g, enc[:, half:], NN)

    @pl.when(i == pl.num_programs(0) - 1)
    def _():
        gw_ref[...] = jnp.transpose(acc[...]) if is_last else acc[...]

    for copy in placed:
        copy.wait()


def gw_part(part, n_part, scal, enc, z, lse_rows, lab_rows, gl, recvs, acc, prev):
    n_batch, n_frames, depth = enc.shape
    n_cols = z.shape[0]
    steps = n_batch // GROUP // n_part
    base = part * steps
    rows = GROUP * n_frames
    is_first, is_last = part == 0, part == n_part - 1

    def here(i, scal):
        return base + i

    def then(i, scal):
        return base + jnp.minimum(i + 1, steps - 1)

    lab_block, gl_block = (1, 1, GROUP * SLOTS), (GROUP, SLOTS, n_frames)
    in_specs = [
        *[blocks((GROUP // GW_SPLIT, n_frames, depth), lambda i, scal, c=c: (base + i) * GW_SPLIT + c) for c in range(GW_SPLIT)],
        *[pl.BlockSpec((n_cols // GW_SPLIT, rows), lambda i, scal, c=c: (c, base + i)) for c in range(GW_SPLIT)],
        blocks((1, 1, rows), here),
        blocks(lab_block, lambda *_: base),
        blocks(gl_block, lambda *_: base),
        blocks(lab_block, then),
        blocks(gl_block, then),
    ]
    in_specs += place_specs(recvs)
    args = [scal, *[enc] * GW_SPLIT, *[z] * GW_SPLIT, lse_rows, lab_rows, gl, lab_rows, gl, *recvs]
    if not is_first:
        in_specs.append(whole(n_cols, depth))
        args.append(acc)
    in_specs.append(in_place())
    aliases = {len(args): 0}
    args.append(prev)
    shape = (depth, n_cols) if is_last else (n_cols, depth)
    return pl.pallas_call(
        functools.partial(gw_kernel, [r.shape[0] for r in recvs], is_first, is_last),
        grid_spec=pltpu.PrefetchScalarGridSpec(
            num_scalar_prefetch=1,
            grid=(steps,),
            in_specs=in_specs,
            out_specs=(in_place(), whole(*shape)),
            scratch_shapes=[
                pltpu.VMEM((n_cols, depth), jnp.float32),
                pltpu.VMEM((n_frames, rows), jnp.bfloat16),
                pltpu.VMEM((GROUP * SLOTS, rows), jnp.float32),
                pltpu.VMEM((2, n_cols, rows), jnp.bfloat16),
                pltpu.SemaphoreType.DMA((max(len(recvs), 1),)),
            ],
        ),
        out_shape=(jax.ShapeDtypeStruct(prev.shape, jnp.float32), jax.ShapeDtypeStruct(shape, jnp.float32)),
        input_output_aliases=aliases,
        compiler_params=params(),
        cost_estimate=pl.CostEstimate(flops=2 * steps * rows * depth * n_cols, bytes_accessed=4 * steps * rows * n_cols, transcendentals=steps * rows * n_cols),
        name="gw_part",
    )(*args)


def place_kernel(totals, scal_ref, *refs):
    n = len(totals)
    copies = place_start(tuple(zip(refs, totals)), refs[n + 1], scal_ref, refs[n + 2])
    for copy in copies:
        copy.wait()


def place(scal, recvs, prev):
    totals = [r.shape[0] for r in recvs]
    return pl.pallas_call(
        functools.partial(place_kernel, totals),
        grid_spec=pltpu.PrefetchScalarGridSpec(
            num_scalar_prefetch=1,
            grid=(max(totals) // PLACE,),
            in_specs=place_specs(recvs) + [in_place()],
            out_specs=in_place(),
            scratch_shapes=[pltpu.SemaphoreType.DMA((len(recvs),))],
        ),
        out_shape=jax.ShapeDtypeStruct(prev.shape, jnp.float32),
        input_output_aliases={1 + len(recvs): 0},
        compiler_params=params(),
        name="place",
    )(scal, *recvs, prev)


def solution(mesh):
    n_dev = mesh.shape["tp"]

    def swap(x, bit):
        return lax.ppermute(x, "tp", [(i, i ^ bit) for i in range(n_dev)])

    def device_fn(enc, w_loc, labels, in_len, lab_len):
        n_batch, n_frames, depth = enc.shape
        n_cols = w_loc.shape[1]
        n_lab = labels.shape[1]
        n_mine = n_batch // 4
        sizes = [2 * UNIT] * (n_mine // (2 * UNIT) - 1) + [UNIT] * 2
        n_chunk = len(sizes)
        offs = [sum(sizes[:k]) for k in range(n_chunk)]
        tp = lax.axis_index("tp")
        core = tp % 2
        colour = (tp // 2 + tp // 4) % 2
        mine = 2 * colour + core

        u = jnp.arange(n_lab)
        valid = u[None, :] < lab_len[:, None]
        earlier = (labels[:, :, None] == labels[:, None, :]) & (u[None, :] < u[:, None])[None]
        first = valid & ~jnp.any(earlier, axis=2)
        slot_lab = jnp.concatenate(
            [jnp.where(first, labels, -1), jnp.zeros((n_batch, 1), jnp.int32), jnp.full((n_batch, SLOTS - n_lab - 1), -1, jnp.int32)], axis=1
        )

        wt = w_loc.T
        wt_all, lse, z_loc = spread_projection(enc, wt, slot_lab, n_dev, mesh.shape["dp"])
        lse = lse.reshape(n_batch, n_frames)
        lse_live = jnp.where(jnp.arange(n_frames)[None, :] < in_len[:, None], lse, BIG)
        lse_pad = jnp.pad(lse_live.reshape(-1, UNIT, n_frames), ((0, 0), (0, -UNIT % 8), (0, 128 - n_frames)), constant_values=BIG)

        def take(x):
            return lax.dynamic_slice_in_dim(x, mine * n_mine, n_mine, axis=0)

        lab_m = take(labels)
        slot_m = take(slot_lab)
        ext_m = jnp.concatenate([lab_m, jnp.zeros((n_mine, SLOTS - n_lab), jnp.int32)], axis=1)
        table = jnp.concatenate([lab_m, take(in_len)[:, None], take(lab_len)[:, None], ext_m[:, n_lab + 2 :]], axis=1).T
        lab_cols = ext_m.T.astype(jnp.float32)
        dup = jnp.pad(jnp.any(take(valid & ~first), axis=0).astype(jnp.int32), (0, SLOTS - n_lab))

        zl, lab_proj = label_logits(ext_m[:, : n_lab + 1].reshape(-1), jnp.stack([mine, mine]).astype(jnp.int32), enc, lab_cols, wt_all, n_mine, n_lab + 1)
        gl_gw, loss_m = lattice(dup, zl, take(lse).T, table, n_lab)
        loss_m = loss_m[0]

        def spread(x):
            other = swap(x, 2)
            partner = swap(x, 1)
            last = swap(other, 1)
            out = jnp.zeros((4,) + x.shape, x.dtype)
            for value, where in ((x, mine), (other, mine ^ 2), (partner, mine ^ 1), (last, mine ^ 3)):
                out = lax.dynamic_update_index_in_dim(out, value, where, 0)
            return out.reshape((4 * x.shape[0],) + x.shape[1:])

        loss = spread(loss_m)
        gl_all = spread(gl_gw)

        set_rows = n_mine * n_frames
        moved = {}

        def pick(*wanted):
            kinds = [(k, part, flip) for k, flip in wanted if k >= 0 for part in (0, 1)]
            return kinds, [moved[kind] for kind in kinds]

        def scal_of(head, kinds):
            vals = [head] + [(mine ^ flip) * set_rows + (offs[k] + part * (sizes[k] // 2)) * n_frames for k, part, flip in kinds]
            vals += [0] * (SLOTS // 2 - len(vals))
            return jnp.stack([jnp.asarray(v, jnp.int32) for v in vals])

        def forward(k, after):
            for part in (0, 1):
                block, after = lax.optimization_barrier((moved[(k, part, 2)], after))
                moved[(k, part, 3)] = swap(block, 1)
            return after

        out = None
        for k in range(n_chunk):
            kinds, data = pick((k - 1, 0), (k - 2, 1), (k - 3, 2), (k - 4, 3))
            scal = scal_of(mine, kinds)
            if k == 2:
                scal, loss, gl_all = lax.optimization_barrier((scal, loss, gl_all))
            out, sy, sz = hs_chunk(
                offs[k], sizes[k], n_mine, n_lab + 1, scal, enc, wt_all, lse_pad, slot_m.reshape(-1, UNIT, SLOTS), gl_gw, lab_proj, data, out
            )
            if k >= 2:
                sy = forward(k - 2, sy)
            for part, x, bit in ((0, sy, 2), (1, sz, 4)):
                moved[(k, part, 0)] = x
                moved[(k, part, 1)] = swap(x, 1)
                moved[(k, part, 2)] = swap(x, bit)

        lse_rows = lse_live.reshape(n_batch // GROUP, 1, GROUP * n_frames)
        lab_rows = slot_lab.reshape(n_batch // GROUP, 1, GROUP * SLOTS)
        acc = None
        n = n_chunk
        late = (((n - 1, 0), (n - 2, 1), (n - 3, 2), (n - 4, 3)), ((n - 1, 1), (n - 3, 3)), ((n - 2, 2),))
        for part, wanted in enumerate(late):
            kinds, data = pick(*wanted)
            out, acc = gw_part(part, len(late), scal_of(tp * n_cols, kinds), enc, z_loc, lse_rows, lab_rows, gl_all, data, acc, out)
            acc = forward(n - 2, acc) if part == 1 else acc
        acc = forward(n - 1, acc)
        kinds, data = pick((n - 2, 3), (n - 1, 2), (n - 1, 3))
        out = place(scal_of(tp, kinds), data, out)
        return loss, acc, out.reshape(n_batch, n_frames, depth)

    return jax.shard_map(
        device_fn,
        mesh=mesh,
        in_specs=(P("dp"), P(None, "tp"), P("dp"), P("dp"), P("dp")),
        out_specs=(P("dp"), P("dp", "tp"), P("dp")),
        check_vma=False,
    )
```

```python
import functools

import jax
import jax.numpy as jnp
import numpy as np
from jax import lax
from jax.experimental import pallas as pl
from jax.experimental.pallas import tpu as pltpu
from jax.sharding import PartitionSpec as P


NEG_FILL = -1.0e30
NEW = None
BIG = 1.0e30
MESH = pl.DeviceIdType.MESH
NT = (((1,), (1,)), ((), ()))
NN = (((1,), (0,)), ((), ()))
TN = (((0,), (0,)), ((), ()))
SLOTS = 32
ROWS = 8
HS_WIDTH = 1024
ROW = 16
SPARE = 48
LARGE = 64
PLACE = 4
GROUP = 8
GW_SPLIT = 4
VMEM_LIMIT = 60 * 1024 * 1024


def dot(a, b, dims):
    return lax.dot_general(a, b, dims, preferred_element_type=jnp.float32)


def whole(*shape):
    return pl.BlockSpec(shape, lambda *_: (0,) * len(shape))


def blocks(shape, first):
    return pl.BlockSpec(shape, lambda *g: (first(*g),) + (0,) * (len(shape) - 1))


def in_place():
    return pl.BlockSpec(memory_space=pl.ANY)


def in_vmem():
    return pl.BlockSpec(memory_space=pltpu.VMEM)


def params(**kw):
    return pltpu.CompilerParams(vmem_limit_bytes=VMEM_LIMIT, **kw)


SUBS = 4
N_Z = 4
HOPS = SUBS * (N_Z - 1)
LAG_Y, LAG_X = 2, 4
IDS = SUBS + 2 * HOPS
KINDS = 1, 2


def spread_kernel(n_dev, n_dp, enc_hbm, w_ref, lab_ref, flag_ref, all_ref, lse_ref, z_hbm, any_ref, *scratch):
    encbuf, st, recv, mine, bias, zbuf, flag, enc_sem, own_sem, z_sem, f_send, f_recv, *sems = scratch
    dn_send, dn_recv, up_send, up_recv, y_send, y_recv, x_send, x_recv, v_send, v_recv, c_send, c_recv, s1_send, s1_recv, s2_send, s2_recv = sems
    dp = lax.axis_index("dp")
    tp = lax.axis_index("tp")
    core = lax.rem(tp, 2)
    z = lax.div(tp, 4)
    mate = tp + 1 - 2 * core
    across = tp + 2 - 4 * lax.rem(lax.div(tp, 2), 2)
    block = w_ref.shape[0]
    piece = block // SUBS
    crosses = (core == dp) if n_dp > 1 else (core >= 0)
    n_seq, n_frames, depth = encbuf.shape[1:]

    def rows(owner, s):
        return all_ref.at[pl.ds(pl.multiple_of(owner * block + s * piece, piece), piece), :]

    def move(src, owner, s, send, got, dst):
        return pltpu.make_async_remote_copy(src_ref=src, dst_ref=rows(owner, s), send_sem=send, recv_sem=got, device_id=dst, device_id_type=MESH)

    def to(dev):
        return {"tp": dev}

    beside = {"dp": 1 - dp} if n_dp > 1 else to(tp)

    def owner_of(base, kind, q):
        hop = lax.div(q, SUBS) + 1
        return base + (4 * hop if kind == 1 else -4 * hop)

    def there(kind, q):
        hop = lax.div(q, SUBS) + 1
        return (q >= 0) & (q < HOPS) & ((z + hop <= N_Z - 1) if kind == 1 else (z - hop >= 0))

    inner = (z >= 1) & (z <= N_Z - 2)

    def by_z(q):
        return (q >= SUBS) | crosses | inner

    barrier = pltpu.get_barrier_semaphore()
    for d in range(1, n_dev):
        pl.semaphore_signal(barrier, inc=1, device_id={"tp": lax.rem(tp + d, n_dev)}, device_id_type=MESH)
    if n_dp > 1:
        pl.semaphore_signal(barrier, inc=1, device_id=beside, device_id_type=MESH)
    pl.semaphore_wait(barrier, n_dev - 1 + (n_dp > 1))

    told = pltpu.make_async_remote_copy(src_ref=flag_ref, dst_ref=flag, send_sem=f_send, recv_sem=f_recv, device_id=beside, device_id_type=MESH)
    if n_dp > 1:
        told.start()
    else:
        flag[...] = flag_ref[...]
    own = pltpu.make_async_copy(w_ref, all_ref.at[pl.ds(pl.multiple_of(tp * block, block), block), :], own_sem)
    own.start()

    def own_moves(s):
        src = w_ref.at[pl.ds(pl.multiple_of(s * piece, piece), piece), :]
        return (
            ((z >= 2) | ((z == 1) & crosses), move(src, tp, s, dn_send.at[s], dn_recv.at[s], to(tp - 4))),
            ((z < N_Z - 2) | ((z == N_Z - 2) & crosses), move(src, tp, s, up_send.at[s], up_recv.at[s], to(tp + 4))),
            (crosses, move(src, tp, s, y_send.at[s], y_recv.at[s], to(across))),
            (z >= 0, move(src, tp, s, c_send.at[s], c_recv.at[s], to(mate))),
        )

    def z_moves(kind, q):
        owner = owner_of(tp, kind, q)
        s = lax.rem(q, SUBS)
        src = rows(owner, s)
        got = dn_recv if kind == 1 else up_recv
        send = dn_send if kind == 1 else up_send
        number = SUBS + q + (0 if kind == 1 else HOPS)
        last = (z >= 1) if kind == 1 else (z <= N_Z - 2)
        nxt = lax.rem(q + SUBS, HOPS)
        here = there(kind, q) & by_z(q)
        return (
            here,
            move(src, owner, s, send.at[SUBS + q], got.at[q], to(tp)),
            (
                (here & last, move(src, owner, s, send.at[SUBS + q], got.at[nxt], to(tp - 4 if kind == 1 else tp + 4))),
                (here, move(src, owner, s, c_send.at[number], c_recv.at[number], to(mate))),
                (here & crosses, move(src, owner, s, y_send.at[number], y_recv.at[number], to(across))),
                (here & (q < SUBS) & jnp.logical_not(inner) & (n_dp > 1), move(src, owner, s, v_send.at[number], v_recv.at[number], beside)),
            ),
        )

    def v_moves(kind, q):
        q0 = lax.rem(q + HOPS, HOPS)
        owner, s, number = owner_of(tp, kind, q0), lax.rem(q0, SUBS), SUBS + q0 + (0 if kind == 1 else HOPS)
        src = rows(owner, s)
        here = there(kind, q) & jnp.logical_not(by_z(q))
        return (
            here,
            move(src, owner, s, v_send.at[number], v_recv.at[number], to(tp)),
            ((here, move(src, owner, s, c_send.at[number], c_recv.at[number], to(mate))),),
        )

    def far_parts(kind, q):
        if kind == 0:
            q0 = lax.rem(q + SUBS, SUBS)
            return across, q0, q0, (q >= 0) & (q < SUBS)
        q0 = lax.rem(q + HOPS, HOPS)
        return owner_of(across, kind, q0), lax.rem(q0, SUBS), SUBS + q0 + (0 if kind == 1 else HOPS), there(kind, q)

    def y_moves(kind, q):
        owner, s, number, here = far_parts(kind, q)
        src = rows(owner, s)
        return (
            here & crosses,
            move(src, owner, s, y_send.at[number], y_recv.at[number], to(tp)),
            (
                (here & crosses & (n_dp > 1), move(src, owner, s, x_send.at[number], x_recv.at[number], beside)),
                (here & crosses, move(src, owner, s, c_send.at[IDS + number], c_recv.at[IDS + number], to(mate))),
            ),
        )

    def x_moves(kind, q):
        owner, s, number, here = far_parts(kind, q)
        src = rows(owner, s)
        return (
            here & jnp.logical_not(crosses),
            move(src, owner, s, x_send.at[number], x_recv.at[number], to(tp)),
            ((here & jnp.logical_not(crosses), move(src, owner, s, c_send.at[IDS + number], c_recv.at[IDS + number], to(mate))),),
        )

    def start_all(moves):
        for cond, copy in moves:

            @pl.when(cond)
            def _():
                copy.start()

    def relay(group):
        cond, arrival, moves = group

        @pl.when(cond)
        def _():
            arrival.wait_recv()

        start_all(moves)

    def service(q):
        for kind in KINDS:
            relay(z_moves(kind, q))
        relay(y_moves(0, jnp.minimum(q - 1, SUBS)))
        for kind in KINDS:
            relay(y_moves(kind, q - LAG_Y))
        if n_dp > 1:
            for kind in KINDS:
                relay(v_moves(kind, q - LAG_Y))
            relay(x_moves(0, jnp.minimum(q + 1 - LAG_X, SUBS)))
            for kind in KINDS:
                relay(x_moves(kind, q - LAG_X))

    def enc_copy(i):
        slot = lax.rem(i, 2)
        return pltpu.make_async_copy(enc_hbm.at[pl.ds(i * n_seq, n_seq)], encbuf.at[slot], enc_sem.at[slot])

    def z_copy(i):
        slot = lax.rem(i, 2)
        size = n_seq * n_frames
        return pltpu.make_async_copy(zbuf.at[slot], z_hbm.at[:, pl.ds(pl.multiple_of(i * size, 128), size)], z_sem.at[slot])

    enc_copy(0).start()
    for s in range(SUBS):
        start_all(own_moves(s))
    seq_r = lax.div(lax.broadcasted_iota(jnp.int32, bias.shape, 0), SLOTS)
    seq_c = lax.div(lax.broadcasted_iota(jnp.int32, bias.shape, 1), n_frames)
    bias[...] = jnp.where(seq_r == seq_c, NEG_FILL, 0.0).astype(bias.dtype)
    col = tp * block + lax.broadcasted_iota(jnp.int32, (block, n_seq * SLOTS), 0)

    busy = n_dev - SUBS - 2

    def tile(i, carry):
        enc_copy(i).wait()

        @pl.when(i + 1 < n_dev)
        def _():
            enc_copy(i + 1).start()

        slot = lax.rem(i, 2)
        enc = encbuf[slot].reshape(n_seq * n_frames, depth)
        zt = dot(w_ref[...], enc, NT)
        top = jnp.max(zt, axis=0, keepdims=True)
        st[i, 0:1, :] = top
        st[i, 1:2, :] = jnp.sum(jnp.exp(zt - top), axis=0, keepdims=True)

        @pl.when(i >= 2)
        def _():
            z_copy(i - 2).wait()

        hot = (col == lab_ref[i]).astype(jnp.bfloat16)
        zbuf[slot] = zt + dot(hot, bias[...], NN)
        z_copy(i).start()
        return carry

    def tiles(q):
        return jnp.minimum(2 * q + 1, q + n_dev - busy + 1)

    def with_tiles(q, carry):
        lax.fori_loop(jnp.maximum(tiles(q - 1), 0), tiles(q), tile, 0)
        service(q)
        return carry

    def plain(q, carry):
        service(q)
        return carry

    lax.fori_loop(0, busy, with_tiles, 0)
    first = []
    for d in range(1, n_dev):
        peer = lax.rem(tp + d, n_dev)
        first.append(
            pltpu.make_async_remote_copy(
                src_ref=st.at[peer], dst_ref=recv.at[tp], send_sem=s1_send.at[d], recv_sem=s1_recv.at[d], device_id=to(peer), device_id_type=MESH
            )
        )
    for copy in first:
        copy.start()
    recv[tp] = st[tp]
    lax.fori_loop(busy, busy + 1, plain, 0)
    for copy in first:
        copy.wait()
    top = recv[0, 0:1, :]
    for j in range(1, n_dev):
        top = jnp.maximum(top, recv[j, 0:1, :])
    total = jnp.zeros_like(top)
    for j in range(n_dev):
        total = total + recv[j, 1:2, :] * jnp.exp(recv[j, 0:1, :] - top)
    lse = top + jnp.log(total)
    mine[...] = lse
    lse_ref[tp] = lse
    second = []
    for d in range(1, n_dev):
        peer = lax.rem(tp + d, n_dev)
        second.append(
            pltpu.make_async_remote_copy(
                src_ref=mine, dst_ref=lse_ref.at[tp], send_sem=s2_send.at[d], recv_sem=s2_recv.at[d], device_id=to(peer), device_id_type=MESH
            )
        )
    for copy in second:
        copy.start()
    lax.fori_loop(busy + 1, HOPS, plain, 0)

    def late(q, carry):
        for kind in KINDS:
            relay(y_moves(kind, q - LAG_Y))
            if n_dp > 1:
                relay(v_moves(kind, q - LAG_Y))
                relay(x_moves(kind, q - LAG_X))
        return carry

    lax.fori_loop(HOPS, HOPS + LAG_X, late, 0)
    for copy in second:
        copy.wait()
    own.wait()
    if n_dp > 1:
        told.wait()
    any_ref[...] = jnp.maximum(flag_ref[...], flag[...])
    for i in (n_dev - 2, n_dev - 1):
        z_copy(i).wait()

    def drain(cond, copy):
        @pl.when(cond)
        def _():
            copy.wait_send()

    def finish_own(s, carry):
        for cond, copy in own_moves(s):
            drain(cond, copy)
        move(rows(mate, s), mate, s, c_send.at[s], c_recv.at[s], to(tp)).wait_recv()
        far = mate + across - tp
        move(rows(far, s), far, s, c_send.at[IDS + s], c_recv.at[IDS + s], to(tp)).wait_recv()
        for _, _, moves in (y_moves(0, s), x_moves(0, s)) if n_dp > 1 else (y_moves(0, s),):
            for cond, copy in moves:
                drain(cond, copy)
        return carry

    def finish(q, carry):
        for kind in KINDS:
            here = there(kind, q)
            groups = (z_moves(kind, q), y_moves(kind, q))
            if n_dp > 1:
                groups += (v_moves(kind, q), x_moves(kind, q))
            for _, _, moves in groups:
                for cond, copy in moves:
                    drain(cond, copy)
            number = SUBS + q + (0 if kind == 1 else HOPS)
            s = lax.rem(q, SUBS)

            @pl.when(here)
            def _():
                near = owner_of(mate, kind, q)
                move(rows(near, s), near, s, c_send.at[number], c_recv.at[number], to(tp)).wait_recv()
                far = owner_of(mate + across - tp, kind, q)
                move(rows(far, s), far, s, c_send.at[IDS + number], c_recv.at[IDS + number], to(tp)).wait_recv()

        return carry

    lax.fori_loop(0, SUBS, finish_own, 0)
    lax.fori_loop(0, HOPS, finish, 0)


def spread_projection(enc, wt, slot_lab, flag, n_dev, n_dp):
    n_batch, n_frames, depth = enc.shape
    n_cols = wt.shape[0]
    n_seq = n_batch // n_dev
    rows = n_seq * n_frames
    dma = pltpu.SemaphoreType.DMA
    sems = [SUBS + HOPS, HOPS] * 2 + [IDS] * 6 + [2 * IDS] * 2 + [n_dev] * 4
    return pl.pallas_call(
        functools.partial(spread_kernel, n_dev, n_dp),
        in_specs=[in_place()] + [in_vmem()] * 3,
        out_specs=(in_place(), in_vmem(), in_place(), in_vmem()),
        out_shape=(
            jax.ShapeDtypeStruct((n_dev * n_cols, depth), wt.dtype),
            jax.ShapeDtypeStruct((n_dev, 1, rows), jnp.float32),
            jax.ShapeDtypeStruct((n_cols, n_batch * n_frames), jnp.float32),
            jax.ShapeDtypeStruct(flag.shape, flag.dtype),
        ),
        scratch_shapes=[
            pltpu.VMEM((2, n_seq, n_frames, depth), enc.dtype),
            pltpu.VMEM((n_dev, 2, rows), jnp.float32),
            pltpu.VMEM((n_dev, 2, rows), jnp.float32),
            pltpu.VMEM((1, rows), jnp.float32),
            pltpu.VMEM((n_seq * SLOTS, rows), jnp.bfloat16),
            pltpu.VMEM((2, n_cols, rows), jnp.float32),
            pltpu.VMEM(flag.shape, flag.dtype),
            dma((2,)),
            dma,
            dma((2,)),
            dma,
            dma,
            *[dma((n,)) for n in sems],
        ],
        compiler_params=params(collective_id=0, has_side_effects=True),
        cost_estimate=pl.CostEstimate(flops=2 * n_batch * n_frames * depth * n_cols, bytes_accessed=2 * enc.size, transcendentals=0),
        name="spread_projection",
    )(enc, wt, slot_lab.reshape(n_dev, 1, n_seq * SLOTS), flag)


def label_kernel(n_lab, step_seqs, lab_ref, enc_ref, tab_ref, wt_hbm, out_ref, rows_ref, buf, sem):
    i = pl.program_id(0)
    n_mine, span, depth = buf.shape
    used = n_lab * ROWS

    def fetch(s, carry):
        for u in range(n_lab):
            base = pl.multiple_of(lab_ref[s * n_lab + u] & -ROWS, ROWS)
            pltpu.make_async_copy(wt_hbm.at[pl.ds(base, ROWS), :], buf.at[s, pl.ds(u * ROWS, ROWS), :], sem.at[s]).start()
        return carry

    ahead = 2 * step_seqs

    @pl.when(i == 0)
    def _():
        lax.fori_loop(0, jnp.minimum(ahead, n_mine), fetch, 0)
        buf[:, used:, :] = jnp.zeros((n_mine, span - used, depth), buf.dtype)

    lax.fori_loop(jnp.minimum(i * step_seqs + ahead, n_mine), jnp.minimum((i + 1) * step_seqs + ahead, n_mine), fetch, 0)

    lane = lax.broadcasted_iota(jnp.int32, (SLOTS, span), 1)
    row = lax.broadcasted_iota(jnp.int32, (SLOTS, span), 0)
    for s in range(step_seqs):
        at = i * step_seqs + s
        pltpu.make_async_copy(wt_hbm.at[pl.ds(0, used), :], buf.at[at, pl.ds(0, used), :], sem.at[at]).wait()
    table = tab_ref[...]
    seq = lax.broadcasted_iota(jnp.int32, table.shape, 1)
    for s in range(step_seqs):
        mine = jnp.sum(jnp.where(seq == i * step_seqs + s, table, 0.0), axis=1, keepdims=True).astype(jnp.int32)
        pick = ((lane == row * ROWS + (mine & (ROWS - 1))) & (row < n_lab)).astype(jnp.bfloat16)
        rows_ref[s] = dot(pick, buf[i * step_seqs + s], NN).astype(rows_ref.dtype)
    for s in range(step_seqs):
        out_ref[s] = dot(rows_ref[s], enc_ref[s], NT)


def label_logits(lab_flat, enc, table, wt_all, n_mine, n_lab):
    _, n_frames, depth = enc.shape
    step_seqs = GROUP
    steps = n_mine // step_seqs
    span = (n_lab * ROWS + 15) // 16 * 16
    return pl.pallas_call(
        functools.partial(label_kernel, n_lab, step_seqs),
        grid_spec=pltpu.PrefetchScalarGridSpec(
            num_scalar_prefetch=1,
            grid=(steps,),
            in_specs=[
                blocks((step_seqs, n_frames, depth), lambda i, lab: lab[n_mine * n_lab] * steps + i),
                whole(*table.shape),
                in_place(),
            ],
            out_specs=(blocks((step_seqs, SLOTS, n_frames), lambda i, *_: i), blocks((step_seqs, SLOTS, depth), lambda i, *_: i)),
            scratch_shapes=[pltpu.VMEM((n_mine, span, depth), jnp.bfloat16), pltpu.SemaphoreType.DMA((n_mine,))],
        ),
        out_shape=(jax.ShapeDtypeStruct((n_mine, SLOTS, n_frames), jnp.float32), jax.ShapeDtypeStruct((n_mine, SLOTS, depth), jnp.bfloat16)),
        compiler_params=params(),
        cost_estimate=pl.CostEstimate(flops=2 * n_mine * n_lab * ROWS * n_frames * depth, bytes_accessed=4 * n_mine * n_lab * ROWS * depth, transcendentals=0),
        name="label_logits",
    )(lab_flat, enc, table, wt_all)


def several(body, n, width):
    def run(i, carry):
        for j in range(width):
            carry = body(i * width + j, carry)
        return carry

    return 0, n // width, run


def lattice_kernel(n_lab, dup_ref, seq_ref, lse_ref, lab_ref, out_ref, loss_ref, zl_ref, gl_ref, turned, bb, lb, ll, bl, sl, occ):
    n_frames, n_seq = lse_ref.shape
    shape = lab_ref.shape
    slots = shape[0]
    slot = lax.broadcasted_iota(jnp.int32, shape, 0)
    for u in range(slots):
        zl_ref[pl.ds(u, n_frames, slots), :] = jnp.transpose(seq_ref[pl.ds(u, n_seq, slots), :])

    def at(t):
        return pl.ds(pl.multiple_of(t * slots, slots), slots)

    blank_slot = n_lab - 1
    lab = lab_ref[...]
    in_len = lab_ref[blank_slot:n_lab, :]
    lab_len = lab_ref[n_lab : n_lab + 1, :]
    skip = (slot > 0) & (lab != pltpu.roll(lab, 1, 0))
    first = slot < lab_len
    for v in range(blank_slot - 1):
        first = first & ((lab != lab_ref[v : v + 1, :]) | (slot <= v))
    first = (first & (slot < blank_slot)) | (slot == blank_slot)
    neg = jnp.full(shape, NEG_FILL, jnp.float32)

    def forward(t, carry):
        b, l = carry
        e = zl_ref[at(t), :] - lse_ref[pl.ds(t, 1), :]
        eb = e[blank_slot:n_lab, :]
        prev = jnp.where(slot == 0, neg, pltpu.roll(l, 1, 0))
        top_b = jnp.maximum(b, prev)
        x0 = jnp.exp(b - top_b)
        x1 = jnp.exp(prev - top_b)
        sum_b = x0 + x1
        hop = jnp.where(skip, prev, neg)
        top_l = jnp.maximum(jnp.maximum(l, b), hop)
        y0 = jnp.exp(l - top_l)
        y1 = jnp.exp(b - top_l)
        y2 = jnp.exp(hop - top_l)
        sum_l = y0 + y1 + y2
        inv_b = 1.0 / sum_b
        inv_l = 1.0 / sum_l
        bb[t] = x0 * inv_b
        lb[t] = x1 * inv_b
        ll[t] = y0 * inv_l
        bl[t] = y1 * inv_l
        sl[t] = y2 * inv_l
        live = t < in_len
        new_b = jnp.where(live, top_b + jnp.log(sum_b) + eb, b)
        new_l = jnp.where(live, top_l + jnp.log(sum_l) + e, l)
        return new_b, new_l

    b, l = lax.fori_loop(*several(forward, n_frames, 4), (jnp.where(slot == 0, 0.0, neg), neg))
    end_b = jnp.where(slot == lab_len, b, neg)
    end_l = jnp.where(slot == lab_len - 1, l, neg)
    top = jnp.max(jnp.maximum(end_b, end_l), axis=0, keepdims=True)
    total = jnp.sum(jnp.exp(end_b - top) + jnp.exp(end_l - top), axis=0, keepdims=True)
    log_like = top + jnp.log(total)
    loss_ref[...] = -log_like

    def backward(i, carry):
        t = n_frames - 1 - i
        gb, gl = carry
        live = t < in_len
        blank = jnp.sum(gb, axis=0, keepdims=True)
        occ[t] = jnp.where(live, jnp.where(slot < blank_slot, gl, jnp.where(slot == blank_slot, blank, 0.0)), 0.0)
        back = pltpu.roll(gb * lb[t] + gl * sl[t], shape[0] - 1, 0)
        new_b = gb * bb[t] + gl * bl[t]
        new_l = gl * ll[t] + back
        return jnp.where(live, new_b, gb), jnp.where(live, new_l, gl)

    lax.fori_loop(*several(backward, n_frames, 4), (jnp.exp(end_b - log_like), jnp.exp(end_l - log_like)))

    for v in range(1, blank_slot):

        @pl.when(dup_ref[v] > 0)
        def _():
            take = (lab == lab_ref[v : v + 1, :]) & first & (slot < v)

            def add(t, _):
                row = occ[t]
                occ[t] = row + jnp.where(take, row[v : v + 1, :], 0.0)
                return 0

            lax.fori_loop(0, n_frames, add, 0)

    def emit(t, _):
        p = jnp.exp(zl_ref[at(t), :] - lse_ref[pl.ds(t, 1), :])
        gl_ref[at(t), :] = jnp.where(first & (t < in_len), p - occ[t], 0.0)
        return 0

    lax.fori_loop(*several(emit, n_frames, 4), 0)
    turned[...] = jnp.zeros_like(turned)
    for u in range(n_lab):
        turned[pl.ds(u, n_seq, slots), :] = jnp.transpose(gl_ref[pl.ds(u, n_frames, slots), :])
    out_ref[...] = turned[...].astype(out_ref.dtype)


def lattice(dup, zl, lse, table, n_lab):
    n_seq, slots, n_frames = zl.shape
    by_frame = pltpu.VMEM((n_frames * slots, n_seq), jnp.float32)
    by_seq = (n_seq * slots, n_frames)
    gl, loss = pl.pallas_call(
        functools.partial(lattice_kernel, n_lab + 1),
        in_specs=[pl.BlockSpec(memory_space=pltpu.SMEM)] + [in_vmem()] * 3,
        out_specs=(in_vmem(), in_vmem()),
        out_shape=(jax.ShapeDtypeStruct(by_seq, jnp.bfloat16), jax.ShapeDtypeStruct((1, n_seq), jnp.float32)),
        scratch_shapes=[by_frame, by_frame, pltpu.VMEM(by_seq, jnp.float32)] + [pltpu.VMEM((n_frames, slots, n_seq), jnp.float32)] * 6,
        compiler_params=params(),
        cost_estimate=pl.CostEstimate(flops=2 * 10**10, bytes_accessed=2 * zl.size, transcendentals=0),
        name="lattice",
    )(dup, zl.reshape(by_seq), lse, table)
    return gl.reshape(zl.shape), loss


class Plan:
    def __init__(self, n_batch, n_frames):
        self.groups = n_batch * n_frames // ROW // 4
        self.seq = 4 * self.groups
        self.mine = self.seq + self.groups
        self.column = self.mine + 1
        self.row = self.column + 1


def place_specs(recvs):
    return [blocks((PLACE * ROW, r.shape[1]), lambda i, plan, last=r.shape[0] // (PLACE * ROW) - 1: jnp.minimum(i, last)) for r in recvs]


def placing(refs, where, out_ref, plan, plan_ref, sem, act):
    step = pl.program_id(0)
    for i, (ref, (first, total, flip)) in enumerate(zip(refs, where)):

        @pl.when(step < total // PLACE)
        def _():
            if act == "wait":
                pltpu.make_async_copy(ref, out_ref.at[pl.ds(0, PLACE * ROW), :], sem.at[i]).wait()
            else:
                start_groups(ref, PLACE, (plan_ref[plan.mine] ^ flip) * plan.groups + first + step * PLACE, out_ref, plan_ref, sem.at[i])


def start_groups(ref, n, at, out_ref, plan_ref, sem):
    for g in range(n):
        row = pl.multiple_of(plan_ref[at + g], ROW)
        pltpu.make_async_copy(ref.at[pl.ds(g * ROW, ROW), :], out_ref.at[pl.ds(row, ROW), :], sem).start()


def hs_kernel(n_lab, plan, first, n_groups, where, has_prev, plan_ref, enc_hbm, w0_ref, w1_ref, lse_ref, slot_ref, gl_ref, rows_ref, *refs):
    n_recv = len(where)
    recvs = refs[:n_recv]
    out_ref, sy_ref, sz_ref, enc, slots, shift, sem_e, sem_r = refs[n_recv + has_prev :]
    j = pl.program_id(0)
    half = n_groups // 2
    spots = (recvs, where, out_ref, plan, plan_ref, sem_r)
    placing(*spots, "start")

    @pl.when(j == 0)
    def _():
        mine = plan_ref[plan.mine] * plan.groups + first

        def gather(i, carry):
            for g in range(8):
                r = i * 8 + g
                row = pl.multiple_of(plan_ref[mine + r], ROW)
                to = pl.ds(pl.multiple_of(r * ROW, ROW), ROW)
                pltpu.make_async_copy(enc_hbm.at[pl.ds(row, ROW), :], enc.at[to, :], sem_e).start()
                slots[pl.ds(r, 1), :] = slot_ref[pl.ds(plan_ref[plan.seq + first + r], 1), :]
            return carry

        lax.fori_loop(0, n_groups // 8, gather, 0)
        lane = lax.broadcasted_iota(jnp.int32, (ROW, lse_ref.shape[1]), 1)
        for r in range(n_groups):
            seq = plan_ref[plan.seq + first + r]
            frame = pl.multiple_of(plan_ref[mine + r] - plan_ref[plan.row] - seq * lse_ref.shape[0], ROW)
            column = jnp.sum(jnp.where(lane == seq, lse_ref[pl.ds(frame, ROW), :], 0.0), axis=1, keepdims=True)
            shift[r] = jnp.broadcast_to(column, (ROW, 128))
        for part, acc in enumerate((sy_ref, sz_ref)):

            def share(i, carry):
                for g in range(8):
                    r = i * 8 + g
                    row = pl.multiple_of(plan_ref[mine + part * half + r] - plan_ref[plan.row], ROW)
                    seq = plan_ref[plan.seq + first + part * half + r]
                    acc[pl.ds(pl.multiple_of(r * ROW, ROW), ROW), :] = dot(gl_ref[pl.ds(row, ROW), :], rows_ref[seq], NN)
                return carry

            lax.fori_loop(0, half // 8, share, 0)
        pltpu.make_async_copy(enc_hbm.at[pl.ds(0, n_groups * ROW), :], enc, sem_e).wait()

    w = jnp.concatenate([w0_ref[...], w1_ref[...]], axis=0)
    width = w.shape[0]
    col = j * width + lax.broadcasted_iota(jnp.int32, (8, width), 1)
    biases = []
    for i in range(n_groups // 8):
        bias = jnp.zeros((8, width), jnp.float32)
        for u in range(n_lab):
            bias = jnp.where(col == slots[i * 8 : (i + 1) * 8, u : u + 1], NEG_FILL, bias)
        biases.append(bias)
    for part, acc in enumerate((sy_ref, sz_ref)):
        z = dot(enc[part * half * ROW : (part + 1) * half * ROW, :], w, NT)
        ps = []
        for g in range(half):
            r = part * half + g
            low = jnp.concatenate([shift[r]] * (width // 128), axis=1)
            p = jnp.exp(z[g * ROW : (g + 1) * ROW, :] - low + biases[r // 8][r % 8 : r % 8 + 1, :])
            ps.append(p.astype(jnp.bfloat16))
        acc[...] += dot(jnp.concatenate(ps, axis=0), w, NN)

    placing(*spots, "wait")


def hs_chunk(first, n_groups, plan, table, enc, wt_all, lse, slots, gl, lab_rows, n_lab, recvs, where, prev):
    n_rows, depth = enc.shape
    n_vocab = wt_all.shape[0]
    width = HS_WIDTH if n_vocab >= 8192 else 128
    steps = n_vocab // width
    in_specs = [
        in_place(),
        blocks((width // 2, depth), lambda j, table: 2 * j),
        blocks((width // 2, depth), lambda j, table: 2 * j + 1),
        whole(*lse.shape),
        whole(*slots.shape),
        whole(*gl.shape),
        whole(*lab_rows.shape),
    ]
    in_specs += place_specs(recvs)
    args = [table, enc, wt_all, wt_all, lse, slots, gl, lab_rows, *recvs]
    aliases = {}
    if prev is not None:
        in_specs.append(in_place())
        aliases = {len(args): 0}
        args.append(prev)
    rows = n_groups * ROW
    send = jax.ShapeDtypeStruct((rows // 2, depth), jnp.float32)
    return pl.pallas_call(
        functools.partial(hs_kernel, n_lab, plan, first, n_groups, where, int(prev is not None)),
        grid_spec=pltpu.PrefetchScalarGridSpec(
            num_scalar_prefetch=1,
            grid=(steps,),
            in_specs=in_specs,
            out_specs=(in_place(), whole(*send.shape), whole(*send.shape)),
            scratch_shapes=[
                pltpu.VMEM((rows, depth), jnp.bfloat16),
                pltpu.VMEM((n_groups, SLOTS), jnp.int32),
                pltpu.VMEM((n_groups, ROW, 128), jnp.float32),
                pltpu.SemaphoreType.DMA,
                pltpu.SemaphoreType.DMA((max(len(recvs), 1),)),
            ],
        ),
        out_shape=(jax.ShapeDtypeStruct((n_rows, depth), jnp.float32), send, send),
        input_output_aliases=aliases,
        compiler_params=params(),
        cost_estimate=pl.CostEstimate(flops=4 * rows * depth * n_vocab, bytes_accessed=2 * n_vocab * depth, transcendentals=rows * n_vocab),
        name="hs_chunk",
    )(*args)


def gw_kernel(plan, where, base, per_set, last_step, is_first, is_last, plan_ref, *refs):
    enc_refs, z_refs = refs[:GW_SPLIT], refs[GW_SPLIT : 2 * GW_SPLIT]
    lse_ref, lab0_ref, lab_ref, *refs = refs[2 * GW_SPLIT :]
    gl0_refs, gl_refs, refs = refs[:4], refs[4:8], refs[8:]
    n_recv = len(where)
    recvs = refs[:n_recv]
    acc_in = None if is_first else refs[n_recv]
    out_ref, gw_ref, acc, fan, diag, part, zero, sem_r, sem_z = refs[n_recv + (not is_first) + 1 :]
    i = pl.program_id(0)
    n_seq, n_frames, depth = enc_refs[0].shape
    n_seq *= GW_SPLIT
    n_cols, rows = acc.shape[0], n_seq * n_frames
    spots = (recvs, where, out_ref, plan, plan_ref, sem_r)
    placing(*spots, "start")

    def fanned(gls, step):
        owner = lax.div(base + step, per_set) ^ plan_ref[plan.mine]
        gl = gls[0][...]
        for flip in range(1, 4):
            gl = jnp.where(owner == flip, gls[flip][...], gl)
        return (dot(gl.reshape(n_seq * SLOTS, n_frames), fan[...], NN) * diag[...]).astype(jnp.bfloat16)

    def label_part(lab, wide):
        col = plan_ref[plan.column] + lax.broadcasted_iota(jnp.int32, (n_cols, n_seq * SLOTS), 0)
        return dot((col == lab[0]).astype(jnp.bfloat16), wide, NN).astype(jnp.bfloat16)

    @pl.when(i == 0)
    def _():
        seq_r = lax.div(lax.broadcasted_iota(jnp.int32, diag.shape, 0), SLOTS)
        seq_c = lax.div(lax.broadcasted_iota(jnp.int32, diag.shape, 1), n_frames)
        diag[...] = jnp.where(seq_r == seq_c, 1.0, 0.0)
        t_r = lax.broadcasted_iota(jnp.int32, fan.shape, 0)
        t_c = lax.rem(lax.broadcasted_iota(jnp.int32, fan.shape, 1), n_frames)
        fan[...] = (t_r == t_c).astype(jnp.bfloat16)
        zero[...] = jnp.zeros_like(zero)
        if is_first:
            acc[...] = jnp.zeros_like(acc)
        else:
            acc[...] = acc_in[...]
        part[0] = label_part(lab0_ref, fanned(gl0_refs, 0))

    def blank(act):
        n = 4 * SPARE // last_step
        at = lax.div(i * n, SPARE) * plan.groups + plan.groups - SPARE + lax.rem(i * n, SPARE)
        for g in range(n):
            row = pl.multiple_of(plan_ref[at + g], ROW)
            act(pltpu.make_async_copy(zero, out_ref.at[pl.ds(row, ROW), :], sem_z))

    if is_first:
        blank(lambda copy: copy.start())

    now = lax.rem(i, 2)
    enc = jnp.concatenate([ref[...].reshape(-1, depth) for ref in enc_refs], axis=0)
    half = depth // 2
    wide = fanned(gl_refs, jnp.minimum(i + 1, pl.num_programs(0) - 1))
    p = jnp.concatenate([jnp.exp(ref[...] - lse_ref[0]).astype(jnp.bfloat16) for ref in z_refs], axis=0)
    g = p + part[now]
    acc[:, :half] += dot(g, enc[:, :half], NN)
    part[1 - now] = label_part(lab_ref, wide)
    acc[:, half:] += dot(g, enc[:, half:], NN)

    @pl.when(i == pl.num_programs(0) - 1)
    def _():
        gw_ref[...] = jnp.transpose(acc[...]) if is_last else acc[...]

    if is_first:
        blank(lambda copy: copy.wait())
    placing(*spots, "wait")


def gw_part(part, n_part, plan, table, enc, z, lse_rows, lab_rows, gls, recvs, where, acc, prev):
    n_batch, n_frames, depth = enc.shape
    n_cols = z.shape[0]
    steps = n_batch // GROUP // n_part
    base = part * steps
    per_set = n_batch // GROUP // 4
    rows = GROUP * n_frames
    is_first, is_last = part == 0, part == n_part - 1

    def here(i, scal):
        return base + i

    def then(i, scal):
        return base + jnp.minimum(i + 1, steps - 1)

    lab_block, gl_block = (1, 1, GROUP * SLOTS), (GROUP, SLOTS, n_frames)
    in_specs = [
        *[blocks((GROUP // GW_SPLIT, n_frames, depth), lambda i, scal, c=c: (base + i) * GW_SPLIT + c) for c in range(GW_SPLIT)],
        *[pl.BlockSpec((n_cols // GW_SPLIT, rows), lambda i, scal, c=c: (c, base + i)) for c in range(GW_SPLIT)],
        blocks((1, 1, rows), here),
        blocks(lab_block, lambda *_: base),
        blocks(lab_block, then),
        *[blocks(gl_block, lambda *_: base % per_set)] * 4,
        *[blocks(gl_block, lambda i, plan: lax.rem(then(i, plan), per_set))] * 4,
    ]
    in_specs += place_specs(recvs)
    args = [table, *[enc] * GW_SPLIT, *[z] * GW_SPLIT, lse_rows, lab_rows, lab_rows, *gls, *gls, *recvs]
    if not is_first:
        in_specs.append(whole(n_cols, depth))
        args.append(acc)
    in_specs.append(in_place())
    aliases = {len(args): 0}
    args.append(prev)
    shape = (depth, n_cols) if is_last else (n_cols, depth)
    return pl.pallas_call(
        functools.partial(gw_kernel, plan, where, base, per_set, steps, is_first, is_last),
        grid_spec=pltpu.PrefetchScalarGridSpec(
            num_scalar_prefetch=1,
            grid=(steps,),
            in_specs=in_specs,
            out_specs=(in_place(), whole(*shape)),
            scratch_shapes=[
                pltpu.VMEM((n_cols, depth), jnp.float32),
                pltpu.VMEM((n_frames, rows), jnp.bfloat16),
                pltpu.VMEM((GROUP * SLOTS, rows), jnp.float32),
                pltpu.VMEM((2, n_cols, rows), jnp.bfloat16),
                pltpu.VMEM((ROW, depth), jnp.float32),
                pltpu.SemaphoreType.DMA((max(len(recvs), 1),)),
                pltpu.SemaphoreType.DMA,
            ],
        ),
        out_shape=(jax.ShapeDtypeStruct(prev.shape, jnp.float32), jax.ShapeDtypeStruct(shape, jnp.float32)),
        input_output_aliases=aliases,
        compiler_params=params(),
        cost_estimate=pl.CostEstimate(flops=2 * steps * rows * depth * n_cols, bytes_accessed=4 * steps * rows * n_cols, transcendentals=steps * rows * n_cols),
        name="gw_part",
    )(*args)


def place_kernel(plan, where, plan_ref, *refs):
    n = len(where)
    out_ref = refs[n + 1]
    bufs, sem_in, sem_out = refs[n + 2 : -2], *refs[-2:]
    loads = [pltpu.make_async_copy(ref, buf, sem_in.at[i]) for i, (ref, buf) in enumerate(zip(refs, bufs))]
    for copy in loads:
        copy.start()
    for i, (copy, buf, (first, total, flip)) in enumerate(zip(loads, bufs, where)):
        copy.wait()
        start_groups(buf, total, (plan_ref[plan.mine] ^ flip) * plan.groups + first, out_ref, plan_ref, sem_out.at[i])
    for i, buf in enumerate(bufs):
        pltpu.make_async_copy(buf, out_ref.at[pl.ds(0, buf.shape[0]), :], sem_out.at[i]).wait()


def place(plan, table, recvs, where, prev):
    n = len(recvs)
    return pl.pallas_call(
        functools.partial(place_kernel, plan, where),
        grid_spec=pltpu.PrefetchScalarGridSpec(
            num_scalar_prefetch=1,
            grid=(),
            in_specs=[in_place()] * (n + 1),
            out_specs=in_place(),
            scratch_shapes=[pltpu.VMEM(r.shape, r.dtype) for r in recvs] + [pltpu.SemaphoreType.DMA((n,))] * 2,
        ),
        out_shape=jax.ShapeDtypeStruct(prev.shape, jnp.float32),
        input_output_aliases={1 + n: 0},
        compiler_params=params(),
        name="place",
    )(table, *recvs, prev)


def solution(mesh):
    n_dev = mesh.shape["tp"]

    def swap(x, bit):
        return lax.ppermute(x, "tp", [(i, i ^ bit) for i in range(n_dev)])

    def device_fn(enc, w_loc, labels, in_len, lab_len):
        n_batch, n_frames, depth = enc.shape
        n_cols = w_loc.shape[1]
        n_lab = labels.shape[1]
        n_mine = n_batch // 4
        plan = Plan(n_batch, n_frames)
        room = plan.groups - SPARE
        sizes = [LARGE] * (room // LARGE) + [room % LARGE]
        n_chunk = len(sizes)
        offs = [sum(sizes[:k]) for k in range(n_chunk + 1)]
        sizes.append(SPARE)
        tp = lax.axis_index("tp")
        core = tp % 2
        colour = (tp // 2 + tp // 4) % 2
        mine = 2 * colour + core

        u = np.arange(n_lab)
        valid = u[NEW, :] < lab_len[:, NEW]
        earlier = (labels[:, :, NEW] == labels[:, NEW, :]) & (u[NEW, :] < u[:, NEW])[NEW]
        first = valid & ~jnp.any(earlier, axis=2)
        slot_lab = jnp.concatenate(
            [jnp.where(first, labels, -1), jnp.zeros((n_batch, 1), jnp.int32), jnp.full((n_batch, SLOTS - n_lab - 1), -1, jnp.int32)], axis=1
        )

        wt = w_loc.T
        count = lax.shift_right_logical(in_len + (ROW - 1), ROW.bit_length() - 1).reshape(4, n_mine)
        n_live = jnp.sum(count, axis=1)
        full = n_frames // ROW
        pos = np.arange(plan.groups)[NEW, :, NEW]
        before = np.tri(n_mine, k=-1, dtype=bool)[NEW]
        number = np.arange(n_mine)
        seq_of = group_of = 0
        for n_kind, skip, shift in ((count, 0, 0), (full - count, count, n_live)):
            start = jnp.sum(jnp.where(before, n_kind[:, NEW, :], 0), axis=2)
            start = (start + jnp.broadcast_to(shift, (4,))[:, NEW])[:, NEW, :]
            inside = (start <= pos) & (pos < start + n_kind[:, NEW, :])
            seq_of += jnp.sum(jnp.where(inside, number, 0), axis=2)
            group_of += jnp.sum(jnp.where(inside, pos - start + number * full + jnp.broadcast_to(skip, count.shape)[:, NEW, :], 0), axis=2)
        first_row = (np.arange(4)[:, NEW] * plan.groups + group_of) * ROW
        own = jnp.stack([mine, tp * n_cols, mine * n_mine * n_frames])
        ints = jnp.concatenate([first_row.reshape(-1), lax.dynamic_index_in_dim(seq_of, mine, 0, keepdims=False), own]).astype(jnp.int32)
        flag = jnp.broadcast_to(jnp.max(n_live) > room, (8, 128)).astype(jnp.float32)

        wt_all, lse, z_loc, flag = spread_projection(enc, wt, slot_lab, flag, n_dev, mesh.shape["dp"])
        lse = lse.reshape(n_batch, n_frames)
        lse_live = lax.optimization_barrier(jnp.where(jnp.arange(n_frames)[NEW, :] < in_len[:, NEW], lse, BIG))
        def take(x):
            return lax.dynamic_slice_in_dim(x, mine * n_mine, n_mine, axis=0)

        lab_m = take(labels)
        slot_m = take(slot_lab)
        ext_m = jnp.concatenate([lab_m, jnp.zeros((n_mine, SLOTS - n_lab), jnp.int32)], axis=1)
        table = jnp.concatenate([lab_m, take(in_len)[:, NEW], take(lab_len)[:, NEW], ext_m[:, n_lab + 2 :]], axis=1).T
        lab_cols = ext_m.T.astype(jnp.float32)
        dup = jnp.pad(jnp.any(take(valid & ~first), axis=0).astype(jnp.int32), (0, SLOTS - n_lab))

        lab_flat = jnp.concatenate([ext_m[:, : n_lab + 1].reshape(-1), mine[NEW].astype(jnp.int32)])
        zl, lab_proj = label_logits(lab_flat, enc, lab_cols, wt_all, n_mine, n_lab + 1)
        lse_m = take(lse_live).T
        gl_gw, loss_m = lattice(dup, zl, lse_m, table, n_lab)
        loss_m = loss_m[0]
        gl_hs = jnp.transpose(gl_gw, (0, 2, 1)).reshape(-1, SLOTS)

        def spread(x):
            other = swap(x, 2)
            return [x, swap(x, 1), other, swap(other, 1)]

        losses = spread(loss_m)
        owner = (np.arange(4) ^ mine)[:, NEW]
        loss = sum(jnp.where(owner == flip, x[NEW, :], 0.0) for flip, x in enumerate(losses)).reshape(-1)
        gls = spread(gl_gw)

        moved = {}
        enc_rows = enc.reshape(-1, depth)

        def pick(*wanted):
            kinds = [(k, part, flip) for k, flip in wanted if k >= 0 for part in (0, 1)]
            return [moved[kind] for kind in kinds], [(offs[k] + part * (sizes[k] // 2), sizes[k] // 2, flip) for k, part, flip in kinds]

        def chunk(k, spots, prev, ints):
            return hs_chunk(offs[k], sizes[k], plan, ints, enc_rows, wt_all, lse_m, slot_m, gl_hs, lab_proj, n_lab + 1, *spots, prev)

        def send(k, sy, sz):
            for part, (x, bit) in enumerate(((sy, 2), (sz, 4))):
                moved[(k, part, 0)] = x
                moved[(k, part, 1)] = swap(x, 1)
                moved[(k, part, 2)] = swap(x, bit)

        def forward(k, after):
            for part in (0, 1):
                block, after = lax.optimization_barrier((moved[(k, part, 2)], after))
                moved[(k, part, 3)] = swap(block, 1)
            return after

        lse_rows = lse_live.reshape(n_batch // GROUP, 1, GROUP * n_frames)
        lab_rows = slot_lab.reshape(n_batch // GROUP, 1, GROUP * SLOTS)
        out = None
        for k in range(n_chunk):
            if k == min(2, n_chunk - 1):
                ints, loss, gls, lse_rows, lab_rows = lax.optimization_barrier((ints, loss, gls, lse_rows, lab_rows))
            out, sy, sz = chunk(k, pick((k - 1, 0), (k - 2, 1), (k - 2, 2), (k - 3, 3)), out, ints)
            if k > 0:
                sy = forward(k - 1, sy)
            send(k, sy, sz)

        acc = None
        n = n_chunk
        late = (((n - 1, 0), (n - 2, 1), (n - 2, 2), (n - 3, 3)), ((n - 1, 1), (n - 2, 3), (n - 1, 2)))
        for part, wanted in enumerate(late):
            out, acc = gw_part(part, len(late), plan, ints, enc, z_loc, lse_rows, lab_rows, gls, *pick(*wanted), acc, out)
            acc = acc if part else forward(n - 1, acc)
        out = place(plan, ints, *pick((n - 1, 3)), out)

        def rest(out):
            out, sy, sz = chunk(n, ([], []), out, ints)
            send(n, sy, sz)
            forward(n, out)
            return place(plan, ints, *pick(*[(n, flip) for flip in range(4)]), out)

        out = lax.cond(flag[0, 0] > 0, rest, lambda out: out, out)
        return loss, acc, out.reshape(n_batch, n_frames, depth)

    return jax.shard_map(
        device_fn,
        mesh=mesh,
        in_specs=(P("dp"), P(None, "tp"), P("dp"), P("dp"), P("dp")),
        out_specs=(P("dp"), P("dp", "tp"), P("dp")),
        check_vma=False,
    )
```

```python
import functools

import jax
import jax.numpy as jnp
import numpy as np
from jax import lax
from jax.experimental import pallas as pl
from jax.experimental.pallas import tpu as pltpu
from jax.sharding import PartitionSpec as P


NEG_FILL = -1.0e30
NEW = None
BIG = 1.0e30
MESH = pl.DeviceIdType.MESH
NT = (((1,), (1,)), ((), ()))
NN = (((1,), (0,)), ((), ()))
TN = (((0,), (0,)), ((), ()))
SLOTS = 32
ROWS = 8
HS_WIDTH = 1024
ROW = 16
SPARE = 48
LARGE = 80
PLACE = 5
GROUP = 8
GW_SPLIT = 4
Z_SEQS = 4
VMEM_LIMIT = 60 * 1024 * 1024


def dot(a, b, dims):
    return lax.dot_general(a, b, dims, preferred_element_type=jnp.float32)


def whole(*shape):
    return pl.BlockSpec(shape, lambda *_: (0,) * len(shape))


def blocks(shape, first):
    return pl.BlockSpec(shape, lambda *g: (first(*g),) + (0,) * (len(shape) - 1))


def in_place():
    return pl.BlockSpec(memory_space=pl.ANY)


def in_vmem():
    return pl.BlockSpec(memory_space=pltpu.VMEM)


def params(**kw):
    return pltpu.CompilerParams(vmem_limit_bytes=VMEM_LIMIT, **kw)


SUBS = 4
N_Z = 4
HOPS = SUBS * (N_Z - 1)
LAG_Y, LAG_X = 2, 4
IDS = SUBS + 2 * HOPS
KINDS = 1, 2


def spread_kernel(n_dev, n_dp, enc_hbm, w_ref, lab_ref, flag_ref, all_ref, lse_ref, z_hbm, any_ref, *scratch):
    encbuf, st, recv, mine, bias, zbuf, flag, enc_sem, own_sem, z_sem, f_send, f_recv, *sems = scratch
    dn_send, dn_recv, up_send, up_recv, y_send, y_recv, x_send, x_recv, v_send, v_recv, c_send, c_recv, s1_send, s1_recv, s2_send, s2_recv = sems
    dp = lax.axis_index("dp")
    tp = lax.axis_index("tp")
    core = lax.rem(tp, 2)
    z = lax.div(tp, 4)
    mate = tp + 1 - 2 * core
    across = tp + 2 - 4 * lax.rem(lax.div(tp, 2), 2)
    block = w_ref.shape[0]
    piece = block // SUBS
    crosses = (core == dp) if n_dp > 1 else (core >= 0)
    n_seq, n_frames, depth = encbuf.shape[1:]

    def rows(owner, s):
        return all_ref.at[pl.ds(pl.multiple_of(owner * block + s * piece, piece), piece), :]

    def move(src, owner, s, send, got, dst):
        return pltpu.make_async_remote_copy(src_ref=src, dst_ref=rows(owner, s), send_sem=send, recv_sem=got, device_id=dst, device_id_type=MESH)

    def to(dev):
        return {"tp": dev}

    beside = {"dp": 1 - dp} if n_dp > 1 else to(tp)

    def owner_of(base, kind, q):
        hop = lax.div(q, SUBS) + 1
        return base + (4 * hop if kind == 1 else -4 * hop)

    def there(kind, q):
        hop = lax.div(q, SUBS) + 1
        return (q >= 0) & (q < HOPS) & ((z + hop <= N_Z - 1) if kind == 1 else (z - hop >= 0))

    inner = (z >= 1) & (z <= N_Z - 2)

    def by_z(q):
        return (q >= SUBS) | crosses | inner

    barrier = pltpu.get_barrier_semaphore()
    for d in range(1, n_dev):
        pl.semaphore_signal(barrier, inc=1, device_id={"tp": lax.rem(tp + d, n_dev)}, device_id_type=MESH)
    if n_dp > 1:
        pl.semaphore_signal(barrier, inc=1, device_id=beside, device_id_type=MESH)
    pl.semaphore_wait(barrier, n_dev - 1 + (n_dp > 1))

    told = pltpu.make_async_remote_copy(src_ref=flag_ref, dst_ref=flag, send_sem=f_send, recv_sem=f_recv, device_id=beside, device_id_type=MESH)
    if n_dp > 1:
        told.start()
    else:
        flag[...] = flag_ref[...]
    own = pltpu.make_async_copy(w_ref, all_ref.at[pl.ds(pl.multiple_of(tp * block, block), block), :], own_sem)
    own.start()

    def own_moves(s):
        src = w_ref.at[pl.ds(pl.multiple_of(s * piece, piece), piece), :]
        return (
            ((z >= 2) | ((z == 1) & crosses), move(src, tp, s, dn_send.at[s], dn_recv.at[s], to(tp - 4))),
            ((z < N_Z - 2) | ((z == N_Z - 2) & crosses), move(src, tp, s, up_send.at[s], up_recv.at[s], to(tp + 4))),
            (crosses, move(src, tp, s, y_send.at[s], y_recv.at[s], to(across))),
            (z >= 0, move(src, tp, s, c_send.at[s], c_recv.at[s], to(mate))),
        )

    def z_moves(kind, q):
        owner = owner_of(tp, kind, q)
        s = lax.rem(q, SUBS)
        src = rows(owner, s)
        got = dn_recv if kind == 1 else up_recv
        send = dn_send if kind == 1 else up_send
        number = SUBS + q + (0 if kind == 1 else HOPS)
        last = (z >= 1) if kind == 1 else (z <= N_Z - 2)
        nxt = lax.rem(q + SUBS, HOPS)
        here = there(kind, q) & by_z(q)
        return (
            here,
            move(src, owner, s, send.at[SUBS + q], got.at[q], to(tp)),
            (
                (here & last, move(src, owner, s, send.at[SUBS + q], got.at[nxt], to(tp - 4 if kind == 1 else tp + 4))),
                (here, move(src, owner, s, c_send.at[number], c_recv.at[number], to(mate))),
                (here & crosses, move(src, owner, s, y_send.at[number], y_recv.at[number], to(across))),
                (here & (q < SUBS) & jnp.logical_not(inner) & (n_dp > 1), move(src, owner, s, v_send.at[number], v_recv.at[number], beside)),
            ),
        )

    def v_moves(kind, q):
        q0 = lax.rem(q + HOPS, HOPS)
        owner, s, number = owner_of(tp, kind, q0), lax.rem(q0, SUBS), SUBS + q0 + (0 if kind == 1 else HOPS)
        src = rows(owner, s)
        here = there(kind, q) & jnp.logical_not(by_z(q))
        return (
            here,
            move(src, owner, s, v_send.at[number], v_recv.at[number], to(tp)),
            ((here, move(src, owner, s, c_send.at[number], c_recv.at[number], to(mate))),),
        )

    def far_parts(kind, q):
        if kind == 0:
            q0 = lax.rem(q + SUBS, SUBS)
            return across, q0, q0, (q >= 0) & (q < SUBS)
        q0 = lax.rem(q + HOPS, HOPS)
        return owner_of(across, kind, q0), lax.rem(q0, SUBS), SUBS + q0 + (0 if kind == 1 else HOPS), there(kind, q)

    def y_moves(kind, q):
        owner, s, number, here = far_parts(kind, q)
        src = rows(owner, s)
        return (
            here & crosses,
            move(src, owner, s, y_send.at[number], y_recv.at[number], to(tp)),
            (
                (here & crosses & (n_dp > 1), move(src, owner, s, x_send.at[number], x_recv.at[number], beside)),
                (here & crosses, move(src, owner, s, c_send.at[IDS + number], c_recv.at[IDS + number], to(mate))),
            ),
        )

    def x_moves(kind, q):
        owner, s, number, here = far_parts(kind, q)
        src = rows(owner, s)
        return (
            here & jnp.logical_not(crosses),
            move(src, owner, s, x_send.at[number], x_recv.at[number], to(tp)),
            ((here & jnp.logical_not(crosses), move(src, owner, s, c_send.at[IDS + number], c_recv.at[IDS + number], to(mate))),),
        )

    def start_all(moves):
        for cond, copy in moves:

            @pl.when(cond)
            def _():
                copy.start()

    def relay(group):
        cond, arrival, moves = group

        @pl.when(cond)
        def _():
            arrival.wait_recv()

        start_all(moves)

    def service(q):
        for kind in KINDS:
            relay(z_moves(kind, q))
        relay(y_moves(0, jnp.minimum(q - 1, SUBS)))
        for kind in KINDS:
            relay(y_moves(kind, q - LAG_Y))
        if n_dp > 1:
            for kind in KINDS:
                relay(v_moves(kind, q - LAG_Y))
            relay(x_moves(0, jnp.minimum(q + 1 - LAG_X, SUBS)))
            for kind in KINDS:
                relay(x_moves(kind, q - LAG_X))

    def enc_copy(i):
        slot = lax.rem(i, 2)
        return pltpu.make_async_copy(enc_hbm.at[pl.ds(i * n_seq, n_seq)], encbuf.at[slot], enc_sem.at[slot])

    n_part = zbuf.shape[1]

    def z_copy(i):
        slot = lax.rem(i, 2)
        return pltpu.make_async_copy(zbuf.at[slot], z_hbm.at[pl.ds(i * n_part, n_part)], z_sem.at[slot])

    enc_copy(0).start()
    for s in range(SUBS):
        start_all(own_moves(s))
    seq_r = lax.div(lax.broadcasted_iota(jnp.int32, bias.shape, 0), SLOTS)
    seq_c = lax.div(lax.broadcasted_iota(jnp.int32, bias.shape, 1), n_frames)
    bias[...] = jnp.where(seq_r == seq_c, NEG_FILL, 0.0).astype(bias.dtype)
    col = tp * block + lax.broadcasted_iota(jnp.int32, (block, n_seq * SLOTS), 0)

    busy = n_dev - SUBS - 2

    def tile(i, carry):
        enc_copy(i).wait()

        @pl.when(i + 1 < n_dev)
        def _():
            enc_copy(i + 1).start()

        slot = lax.rem(i, 2)
        enc = encbuf[slot].reshape(n_seq * n_frames, depth)
        zt = dot(w_ref[...], enc, NT)
        top = jnp.max(zt, axis=0, keepdims=True)
        st[i, 0:1, :] = top
        st[i, 1:2, :] = jnp.sum(jnp.exp(zt - top), axis=0, keepdims=True)

        @pl.when(i >= 2)
        def _():
            z_copy(i - 2).wait()

        hot = (col == lab_ref[i]).astype(jnp.bfloat16)
        masked = zt + dot(hot, bias[...], NN)
        size = zbuf.shape[-1]
        for c in range(n_part):
            zbuf[slot, c] = masked[:, c * size : (c + 1) * size]
        z_copy(i).start()
        return carry

    def tiles(q):
        return jnp.minimum(2 * q + 1, q + n_dev - busy + 1)

    def with_tiles(q, carry):
        lax.fori_loop(jnp.maximum(tiles(q - 1), 0), tiles(q), tile, 0)
        service(q)
        return carry

    def plain(q, carry):
        service(q)
        return carry

    lax.fori_loop(0, busy, with_tiles, 0)
    first = []
    for d in range(1, n_dev):
        peer = lax.rem(tp + d, n_dev)
        first.append(
            pltpu.make_async_remote_copy(
                src_ref=st.at[peer], dst_ref=recv.at[tp], send_sem=s1_send.at[d], recv_sem=s1_recv.at[d], device_id=to(peer), device_id_type=MESH
            )
        )
    for copy in first:
        copy.start()
    recv[tp] = st[tp]
    lax.fori_loop(busy, busy + 1, plain, 0)
    for copy in first:
        copy.wait()
    top = recv[0, 0:1, :]
    for j in range(1, n_dev):
        top = jnp.maximum(top, recv[j, 0:1, :])
    total = jnp.zeros_like(top)
    for j in range(n_dev):
        total = total + recv[j, 1:2, :] * jnp.exp(recv[j, 0:1, :] - top)
    lse = top + jnp.log(total)
    mine[...] = lse
    lse_ref[tp] = lse
    second = []
    for d in range(1, n_dev):
        peer = lax.rem(tp + d, n_dev)
        second.append(
            pltpu.make_async_remote_copy(
                src_ref=mine, dst_ref=lse_ref.at[tp], send_sem=s2_send.at[d], recv_sem=s2_recv.at[d], device_id=to(peer), device_id_type=MESH
            )
        )
    for copy in second:
        copy.start()
    lax.fori_loop(busy + 1, HOPS, plain, 0)

    def late(q, carry):
        for kind in KINDS:
            relay(y_moves(kind, q - LAG_Y))
            if n_dp > 1:
                relay(v_moves(kind, q - LAG_Y))
                relay(x_moves(kind, q - LAG_X))
        return carry

    lax.fori_loop(HOPS, HOPS + LAG_X, late, 0)
    for copy in second:
        copy.wait()
    own.wait()
    if n_dp > 1:
        told.wait()
    any_ref[...] = jnp.maximum(flag_ref[...], flag[...])
    for i in range(n_dev - 2, n_dev):
        z_copy(i).wait()

    def drain(cond, copy):
        @pl.when(cond)
        def _():
            copy.wait_send()

    def finish_own(s, carry):
        for cond, copy in own_moves(s):
            drain(cond, copy)
        move(rows(mate, s), mate, s, c_send.at[s], c_recv.at[s], to(tp)).wait_recv()
        far = mate + across - tp
        move(rows(far, s), far, s, c_send.at[IDS + s], c_recv.at[IDS + s], to(tp)).wait_recv()
        for _, _, moves in (y_moves(0, s), x_moves(0, s)) if n_dp > 1 else (y_moves(0, s),):
            for cond, copy in moves:
                drain(cond, copy)
        return carry

    def finish(q, carry):
        for kind in KINDS:
            here = there(kind, q)
            groups = (z_moves(kind, q), y_moves(kind, q))
            if n_dp > 1:
                groups += (v_moves(kind, q), x_moves(kind, q))
            for _, _, moves in groups:
                for cond, copy in moves:
                    drain(cond, copy)
            number = SUBS + q + (0 if kind == 1 else HOPS)
            s = lax.rem(q, SUBS)

            @pl.when(here)
            def _():
                near = owner_of(mate, kind, q)
                move(rows(near, s), near, s, c_send.at[number], c_recv.at[number], to(tp)).wait_recv()
                far = owner_of(mate + across - tp, kind, q)
                move(rows(far, s), far, s, c_send.at[IDS + number], c_recv.at[IDS + number], to(tp)).wait_recv()

        return carry

    lax.fori_loop(0, SUBS, finish_own, 0)
    lax.fori_loop(0, HOPS, finish, 0)


def spread_projection(enc, wt, slot_lab, flag, n_dev, n_dp):
    n_batch, n_frames, depth = enc.shape
    n_cols = wt.shape[0]
    n_seq = n_batch // n_dev
    rows = n_seq * n_frames
    z_seqs = min(Z_SEQS, n_seq)
    dma = pltpu.SemaphoreType.DMA
    sems = [SUBS + HOPS, HOPS] * 2 + [IDS] * 6 + [2 * IDS] * 2 + [n_dev] * 4
    return pl.pallas_call(
        functools.partial(spread_kernel, n_dev, n_dp),
        in_specs=[in_place()] + [in_vmem()] * 3,
        out_specs=(in_place(), in_vmem(), in_place(), in_vmem()),
        out_shape=(
            jax.ShapeDtypeStruct((n_dev * n_cols, depth), wt.dtype),
            jax.ShapeDtypeStruct((n_dev, 1, rows), jnp.float32),
            jax.ShapeDtypeStruct((n_batch // z_seqs, n_cols, z_seqs * n_frames), jnp.float32),
            jax.ShapeDtypeStruct(flag.shape, flag.dtype),
        ),
        scratch_shapes=[
            pltpu.VMEM((2, n_seq, n_frames, depth), enc.dtype),
            pltpu.VMEM((n_dev, 2, rows), jnp.float32),
            pltpu.VMEM((n_dev, 2, rows), jnp.float32),
            pltpu.VMEM((1, rows), jnp.float32),
            pltpu.VMEM((n_seq * SLOTS, rows), jnp.bfloat16),
            pltpu.VMEM((2, n_seq // z_seqs, n_cols, z_seqs * n_frames), jnp.float32),
            pltpu.VMEM(flag.shape, flag.dtype),
            dma((2,)),
            dma,
            dma((2,)),
            dma,
            dma,
            *[dma((n,)) for n in sems],
        ],
        compiler_params=params(collective_id=0, has_side_effects=True),
        cost_estimate=pl.CostEstimate(flops=2 * n_batch * n_frames * depth * n_cols, bytes_accessed=2 * enc.size, transcendentals=0),
        name="spread_projection",
    )(enc, wt, slot_lab.reshape(n_dev, 1, n_seq * SLOTS), flag)


def label_kernel(n_lab, step_seqs, lab_ref, enc_ref, tab_ref, wt_hbm, out_ref, rows_ref, buf, sem):
    i = pl.program_id(0)
    n_mine, span, depth = buf.shape
    used = n_lab * ROWS

    def fetch(s, carry):
        for u in range(n_lab):
            base = pl.multiple_of(lab_ref[s * n_lab + u] & -ROWS, ROWS)
            pltpu.make_async_copy(wt_hbm.at[pl.ds(base, ROWS), :], buf.at[s, pl.ds(u * ROWS, ROWS), :], sem.at[s]).start()
        return carry

    ahead = 2 * step_seqs

    @pl.when(i == 0)
    def _():
        lax.fori_loop(0, jnp.minimum(ahead, n_mine), fetch, 0)
        buf[:, used:, :] = jnp.zeros((n_mine, span - used, depth), buf.dtype)

    lax.fori_loop(jnp.minimum(i * step_seqs + ahead, n_mine), jnp.minimum((i + 1) * step_seqs + ahead, n_mine), fetch, 0)

    lane = lax.broadcasted_iota(jnp.int32, (SLOTS, span), 1)
    row = lax.broadcasted_iota(jnp.int32, (SLOTS, span), 0)
    for s in range(step_seqs):
        at = i * step_seqs + s
        pltpu.make_async_copy(wt_hbm.at[pl.ds(0, used), :], buf.at[at, pl.ds(0, used), :], sem.at[at]).wait()
    table = tab_ref[...]
    seq = lax.broadcasted_iota(jnp.int32, table.shape, 1)
    for s in range(step_seqs):
        mine = jnp.sum(jnp.where(seq == i * step_seqs + s, table, 0.0), axis=1, keepdims=True).astype(jnp.int32)
        pick = ((lane == row * ROWS + (mine & (ROWS - 1))) & (row < n_lab)).astype(jnp.bfloat16)
        rows_ref[s] = dot(pick, buf[i * step_seqs + s], NN).astype(rows_ref.dtype)
    for s in range(step_seqs):
        out_ref[s] = dot(rows_ref[s], enc_ref[s], NT)


def label_logits(lab_flat, enc, table, wt_all, n_mine, n_lab):
    _, n_frames, depth = enc.shape
    step_seqs = GROUP
    steps = n_mine // step_seqs
    span = (n_lab * ROWS + 15) // 16 * 16
    return pl.pallas_call(
        functools.partial(label_kernel, n_lab, step_seqs),
        grid_spec=pltpu.PrefetchScalarGridSpec(
            num_scalar_prefetch=1,
            grid=(steps,),
            in_specs=[
                blocks((step_seqs, n_frames, depth), lambda i, lab: lab[n_mine * n_lab] * steps + i),
                whole(*table.shape),
                in_place(),
            ],
            out_specs=(blocks((step_seqs, SLOTS, n_frames), lambda i, *_: i), blocks((step_seqs, SLOTS, depth), lambda i, *_: i)),
            scratch_shapes=[pltpu.VMEM((n_mine, span, depth), jnp.bfloat16), pltpu.SemaphoreType.DMA((n_mine,))],
        ),
        out_shape=(jax.ShapeDtypeStruct((n_mine, SLOTS, n_frames), jnp.float32), jax.ShapeDtypeStruct((n_mine, SLOTS, depth), jnp.bfloat16)),
        compiler_params=params(),
        cost_estimate=pl.CostEstimate(flops=2 * n_mine * n_lab * ROWS * n_frames * depth, bytes_accessed=4 * n_mine * n_lab * ROWS * depth, transcendentals=0),
        name="label_logits",
    )(lab_flat, enc, table, wt_all)


def several(body, n, width):
    def run(i, carry):
        for j in range(width):
            carry = body(i * width + j, carry)
        return carry

    return 0, n // width, run


def lattice_kernel(n_lab, dup_ref, seq_ref, lse_ref, lab_ref, out_ref, loss_ref, zl_ref, gl_ref, turned, bb, lb, ll, bl, sl, occ):
    n_frames, n_seq = lse_ref.shape
    shape = lab_ref.shape
    slots = shape[0]
    slot = lax.broadcasted_iota(jnp.int32, shape, 0)
    for u in range(slots):
        zl_ref[pl.ds(u, n_frames, slots), :] = jnp.transpose(seq_ref[pl.ds(u, n_seq, slots), :])

    def at(t):
        return pl.ds(pl.multiple_of(t * slots, slots), slots)

    blank_slot = n_lab - 1
    lab = lab_ref[...]
    in_len = lab_ref[blank_slot:n_lab, :]
    lab_len = lab_ref[n_lab : n_lab + 1, :]
    skip = (slot > 0) & (lab != pltpu.roll(lab, 1, 0))
    first = slot < lab_len
    for v in range(blank_slot - 1):
        first = first & ((lab != lab_ref[v : v + 1, :]) | (slot <= v))
    first = (first & (slot < blank_slot)) | (slot == blank_slot)
    neg = jnp.full(shape, NEG_FILL, jnp.float32)

    def forward(t, carry):
        b, l = carry
        e = zl_ref[at(t), :] - lse_ref[pl.ds(t, 1), :]
        eb = e[blank_slot:n_lab, :]
        prev = jnp.where(slot == 0, neg, pltpu.roll(l, 1, 0))
        top_b = jnp.maximum(b, prev)
        x0 = jnp.exp(b - top_b)
        x1 = jnp.exp(prev - top_b)
        sum_b = x0 + x1
        hop = jnp.where(skip, prev, neg)
        top_l = jnp.maximum(jnp.maximum(l, b), hop)
        y0 = jnp.exp(l - top_l)
        y1 = jnp.exp(b - top_l)
        y2 = jnp.exp(hop - top_l)
        sum_l = y0 + y1 + y2
        inv_b = 1.0 / sum_b
        inv_l = 1.0 / sum_l
        bb[t] = x0 * inv_b
        lb[t] = x1 * inv_b
        ll[t] = y0 * inv_l
        bl[t] = y1 * inv_l
        sl[t] = y2 * inv_l
        live = t < in_len
        new_b = jnp.where(live, top_b + jnp.log(sum_b) + eb, b)
        new_l = jnp.where(live, top_l + jnp.log(sum_l) + e, l)
        return new_b, new_l

    b, l = lax.fori_loop(*several(forward, n_frames, 4), (jnp.where(slot == 0, 0.0, neg), neg))
    end_b = jnp.where(slot == lab_len, b, neg)
    end_l = jnp.where(slot == lab_len - 1, l, neg)
    top = jnp.max(jnp.maximum(end_b, end_l), axis=0, keepdims=True)
    total = jnp.sum(jnp.exp(end_b - top) + jnp.exp(end_l - top), axis=0, keepdims=True)
    log_like = top + jnp.log(total)
    loss_ref[...] = -log_like

    def backward(i, carry):
        t = n_frames - 1 - i
        gb, gl = carry
        live = t < in_len
        blank = jnp.sum(gb, axis=0, keepdims=True)
        occ[t] = jnp.where(live, jnp.where(slot < blank_slot, gl, jnp.where(slot == blank_slot, blank, 0.0)), 0.0)
        back = pltpu.roll(gb * lb[t] + gl * sl[t], shape[0] - 1, 0)
        new_b = gb * bb[t] + gl * bl[t]
        new_l = gl * ll[t] + back
        return jnp.where(live, new_b, gb), jnp.where(live, new_l, gl)

    lax.fori_loop(*several(backward, n_frames, 4), (jnp.exp(end_b - log_like), jnp.exp(end_l - log_like)))

    for v in range(1, blank_slot):

        @pl.when(dup_ref[v] > 0)
        def _():
            take = (lab == lab_ref[v : v + 1, :]) & first & (slot < v)

            def add(t, _):
                row = occ[t]
                occ[t] = row + jnp.where(take, row[v : v + 1, :], 0.0)
                return 0

            lax.fori_loop(0, n_frames, add, 0)

    def emit(t, _):
        p = jnp.exp(zl_ref[at(t), :] - lse_ref[pl.ds(t, 1), :])
        gl_ref[at(t), :] = jnp.where(first & (t < in_len), p - occ[t], 0.0)
        return 0

    lax.fori_loop(*several(emit, n_frames, 4), 0)
    turned[...] = jnp.zeros_like(turned)
    for u in range(n_lab):
        turned[pl.ds(u, n_seq, slots), :] = jnp.transpose(gl_ref[pl.ds(u, n_frames, slots), :])
    out_ref[...] = turned[...].astype(out_ref.dtype)


def lattice(dup, zl, lse, table, n_lab):
    n_seq, slots, n_frames = zl.shape
    by_frame = pltpu.VMEM((n_frames * slots, n_seq), jnp.float32)
    by_seq = (n_seq * slots, n_frames)
    gl, loss = pl.pallas_call(
        functools.partial(lattice_kernel, n_lab + 1),
        in_specs=[pl.BlockSpec(memory_space=pltpu.SMEM)] + [in_vmem()] * 3,
        out_specs=(in_vmem(), in_vmem()),
        out_shape=(jax.ShapeDtypeStruct(by_seq, jnp.bfloat16), jax.ShapeDtypeStruct((1, n_seq), jnp.float32)),
        scratch_shapes=[by_frame, by_frame, pltpu.VMEM(by_seq, jnp.float32)] + [pltpu.VMEM((n_frames, slots, n_seq), jnp.float32)] * 6,
        compiler_params=params(),
        cost_estimate=pl.CostEstimate(flops=2 * 10**10, bytes_accessed=2 * zl.size, transcendentals=0),
        name="lattice",
    )(dup, zl.reshape(by_seq), lse, table)
    return gl.reshape(zl.shape), loss


class Plan:
    def __init__(self, n_batch, n_frames):
        self.groups = n_batch * n_frames // ROW // 4
        self.seq = 4 * self.groups
        self.mine = self.seq + self.groups
        self.column = self.mine + 1
        self.row = self.column + 1


def place_specs(recvs):
    return [blocks((PLACE * ROW, r.shape[1]), lambda i, plan, last=r.shape[0] // (PLACE * ROW) - 1: jnp.minimum(i, last)) for r in recvs]


def placing(refs, where, out_ref, plan, plan_ref, sem, act):
    step = pl.program_id(0)
    for i, (ref, (first, total, flip)) in enumerate(zip(refs, where)):

        @pl.when(step < total // PLACE)
        def _():
            if act == "wait":
                pltpu.make_async_copy(ref, out_ref.at[pl.ds(0, PLACE * ROW), :], sem.at[i]).wait()
            else:
                start_groups(ref, PLACE, (plan_ref[plan.mine] ^ flip) * plan.groups + first + step * PLACE, out_ref, plan_ref, sem.at[i])


def start_groups(ref, n, at, out_ref, plan_ref, sem):
    for g in range(n):
        row = pl.multiple_of(plan_ref[at + g], ROW)
        pltpu.make_async_copy(ref.at[pl.ds(g * ROW, ROW), :], out_ref.at[pl.ds(row, ROW), :], sem).start()


def hs_kernel(n_lab, plan, first, n_groups, where, has_prev, plan_ref, enc_hbm, w0_ref, w1_ref, lse_ref, slot_ref, gl_ref, rows_ref, *refs):
    n_recv = len(where)
    recvs = refs[:n_recv]
    out_ref, sy_ref, sz_ref, enc, slots, shift, sem_e, sem_r = refs[n_recv + has_prev :]
    j = pl.program_id(0)
    half = n_groups // 2
    spots = (recvs, where, out_ref, plan, plan_ref, sem_r)
    placing(*spots, "start")

    @pl.when(j == 0)
    def _():
        mine = plan_ref[plan.mine] * plan.groups + first

        def gather(i, carry):
            for g in range(8):
                r = i * 8 + g
                row = pl.multiple_of(plan_ref[mine + r], ROW)
                to = pl.ds(pl.multiple_of(r * ROW, ROW), ROW)
                pltpu.make_async_copy(enc_hbm.at[pl.ds(row, ROW), :], enc.at[to, :], sem_e).start()
                slots[pl.ds(r, 1), :] = slot_ref[pl.ds(plan_ref[plan.seq + first + r], 1), :]
            return carry

        lax.fori_loop(0, n_groups // 8, gather, 0)
        lane = lax.broadcasted_iota(jnp.int32, (ROW, lse_ref.shape[1]), 1)
        for r in range(n_groups):
            seq = plan_ref[plan.seq + first + r]
            frame = pl.multiple_of(plan_ref[mine + r] - plan_ref[plan.row] - seq * lse_ref.shape[0], ROW)
            column = jnp.sum(jnp.where(lane == seq, lse_ref[pl.ds(frame, ROW), :], 0.0), axis=1, keepdims=True)
            shift[r] = jnp.broadcast_to(column, (ROW, 128))
        for part, acc in enumerate((sy_ref, sz_ref)):

            def share(i, carry):
                for g in range(8):
                    r = i * 8 + g
                    seq = plan_ref[plan.seq + first + part * half + r]
                    frame = plan_ref[mine + part * half + r] - plan_ref[plan.row] - seq * gl_ref.shape[1]
                    share_g = gl_ref[seq, pl.ds(pl.multiple_of(frame, ROW), ROW), :]
                    acc[pl.ds(pl.multiple_of(r * ROW, ROW), ROW), :] = dot(share_g, rows_ref[seq], NN)
                return carry

            lax.fori_loop(0, half // 8, share, 0)
        pltpu.make_async_copy(enc_hbm.at[pl.ds(0, n_groups * ROW), :], enc, sem_e).wait()

    w = jnp.concatenate([w0_ref[...], w1_ref[...]], axis=0)
    width = w.shape[0]
    col = j * width + lax.broadcasted_iota(jnp.int32, (8, width), 1)
    biases = []
    for i in range(n_groups // 8):
        bias = jnp.zeros((8, width), jnp.float32)
        for u in range(n_lab):
            bias = jnp.where(col == slots[i * 8 : (i + 1) * 8, u : u + 1], NEG_FILL, bias)
        biases.append(bias)
    for part, acc in enumerate((sy_ref, sz_ref)):
        z = dot(enc[part * half * ROW : (part + 1) * half * ROW, :], w, NT)
        ps = []
        for g in range(half):
            r = part * half + g
            low = jnp.concatenate([shift[r]] * (width // 128), axis=1)
            p = jnp.exp(z[g * ROW : (g + 1) * ROW, :] - low + biases[r // 8][r % 8 : r % 8 + 1, :])
            ps.append(p.astype(jnp.bfloat16))
        acc[...] += dot(jnp.concatenate(ps, axis=0), w, NN)

    placing(*spots, "wait")


def hs_chunk(first, n_groups, plan, table, enc, wt_all, lse, slots, gl, lab_rows, n_lab, recvs, where, prev):
    n_rows, depth = enc.shape
    n_vocab = wt_all.shape[0]
    width = HS_WIDTH if n_vocab >= 8192 else 128
    steps = n_vocab // width
    in_specs = [
        in_place(),
        blocks((width // 2, depth), lambda j, table: 2 * j),
        blocks((width // 2, depth), lambda j, table: 2 * j + 1),
        whole(*lse.shape),
        whole(*slots.shape),
        whole(*gl.shape),
        whole(*lab_rows.shape),
    ]
    in_specs += place_specs(recvs)
    args = [table, enc, wt_all, wt_all, lse, slots, gl, lab_rows, *recvs]
    aliases = {}
    if prev is not None:
        in_specs.append(in_place())
        aliases = {len(args): 0}
        args.append(prev)
    rows = n_groups * ROW
    send = jax.ShapeDtypeStruct((rows // 2, depth), jnp.float32)
    return pl.pallas_call(
        functools.partial(hs_kernel, n_lab, plan, first, n_groups, where, int(prev is not None)),
        grid_spec=pltpu.PrefetchScalarGridSpec(
            num_scalar_prefetch=1,
            grid=(steps,),
            in_specs=in_specs,
            out_specs=(in_place(), whole(*send.shape), whole(*send.shape)),
            scratch_shapes=[
                pltpu.VMEM((rows, depth), jnp.bfloat16),
                pltpu.VMEM((n_groups, SLOTS), jnp.int32),
                pltpu.VMEM((n_groups, ROW, 128), jnp.float32),
                pltpu.SemaphoreType.DMA,
                pltpu.SemaphoreType.DMA((max(len(recvs), 1),)),
            ],
        ),
        out_shape=(jax.ShapeDtypeStruct((n_rows, depth), jnp.float32), send, send),
        input_output_aliases=aliases,
        compiler_params=params(),
        cost_estimate=pl.CostEstimate(flops=4 * rows * depth * n_vocab, bytes_accessed=2 * n_vocab * depth, transcendentals=rows * n_vocab),
        name="hs_chunk",
    )(*args)


def gw_kernel(plan, where, base, per_set, last_step, n_z, is_first, is_last, plan_ref, *refs):
    enc_refs, z_refs = refs[:GW_SPLIT], refs[GW_SPLIT : GW_SPLIT + n_z]
    lse_ref, lab0_ref, lab_ref, *refs = refs[GW_SPLIT + n_z :]
    gl0_refs, gl_refs, refs = refs[:4], refs[4:8], refs[8:]
    n_recv = len(where)
    recvs = refs[:n_recv]
    acc_in = None if is_first else refs[n_recv]
    out_ref, gw_ref, acc, fan, diag, part, zero, sem_r, sem_z = refs[n_recv + (not is_first) + 1 :]
    i = pl.program_id(0)
    n_seq, n_frames, depth = enc_refs[0].shape
    n_seq *= GW_SPLIT
    n_cols, rows = acc.shape[0], n_seq * n_frames
    spots = (recvs, where, out_ref, plan, plan_ref, sem_r)
    placing(*spots, "start")

    def fanned(gls, step):
        owner = lax.div(base + step, per_set) ^ plan_ref[plan.mine]
        gl = gls[0][...]
        for flip in range(1, 4):
            gl = jnp.where(owner == flip, gls[flip][...], gl)
        return (dot(gl.reshape(n_seq * SLOTS, n_frames), fan[...], NN) * diag[...]).astype(jnp.bfloat16)

    def label_part(lab, wide):
        col = plan_ref[plan.column] + lax.broadcasted_iota(jnp.int32, (n_cols, n_seq * SLOTS), 0)
        return dot((col == lab[0]).astype(jnp.bfloat16), wide, NN).astype(jnp.bfloat16)

    @pl.when(i == 0)
    def _():
        seq_r = lax.div(lax.broadcasted_iota(jnp.int32, diag.shape, 0), SLOTS)
        seq_c = lax.div(lax.broadcasted_iota(jnp.int32, diag.shape, 1), n_frames)
        diag[...] = jnp.where(seq_r == seq_c, 1.0, 0.0)
        t_r = lax.broadcasted_iota(jnp.int32, fan.shape, 0)
        t_c = lax.rem(lax.broadcasted_iota(jnp.int32, fan.shape, 1), n_frames)
        fan[...] = (t_r == t_c).astype(jnp.bfloat16)
        zero[...] = jnp.zeros_like(zero)
        if is_first:
            acc[...] = jnp.zeros_like(acc)
        else:
            acc[...] = acc_in[...]
        part[0] = label_part(lab0_ref, fanned(gl0_refs, 0))

    def blank(act):
        n = 4 * SPARE // last_step
        at = lax.div(i * n, SPARE) * plan.groups + plan.groups - SPARE + lax.rem(i * n, SPARE)
        for g in range(n):
            row = pl.multiple_of(plan_ref[at + g], ROW)
            act(pltpu.make_async_copy(zero, out_ref.at[pl.ds(row, ROW), :], sem_z))

    if is_first:
        blank(lambda copy: copy.start())

    now = lax.rem(i, 2)
    enc = jnp.concatenate([ref[...].reshape(-1, depth) for ref in enc_refs], axis=0)
    half = depth // 2
    wide = fanned(gl_refs, jnp.minimum(i + 1, pl.num_programs(0) - 1))
    ps = []
    for c, ref in enumerate(z_refs):
        size = ref.shape[-1]
        ps.append(jnp.exp(ref[0] - lse_ref[0, :, c * size : (c + 1) * size]).astype(jnp.bfloat16))
    g = jnp.concatenate(ps, axis=1) + part[now]
    acc[:, :half] += dot(g, enc[:, :half], NN)
    part[1 - now] = label_part(lab_ref, wide)
    acc[:, half:] += dot(g, enc[:, half:], NN)

    @pl.when(i == pl.num_programs(0) - 1)
    def _():
        gw_ref[...] = jnp.transpose(acc[...]) if is_last else acc[...]

    if is_first:
        blank(lambda copy: copy.wait())
    placing(*spots, "wait")


def gw_part(part, n_part, plan, table, enc, z, lse_rows, lab_rows, gls, recvs, where, acc, prev):
    n_batch, n_frames, depth = enc.shape
    n_cols = z.shape[1]
    n_z = GROUP * n_frames // z.shape[2]
    steps = n_batch // GROUP // n_part
    base = part * steps
    per_set = n_batch // GROUP // 4
    rows = GROUP * n_frames
    is_first, is_last = part == 0, part == n_part - 1

    def here(i, scal):
        return base + i

    def then(i, scal):
        return base + jnp.minimum(i + 1, steps - 1)

    lab_block, gl_block = (1, 1, GROUP * SLOTS), (GROUP, SLOTS, n_frames)
    in_specs = [
        *[blocks((GROUP // GW_SPLIT, n_frames, depth), lambda i, scal, c=c: (base + i) * GW_SPLIT + c) for c in range(GW_SPLIT)],
        *[blocks((1,) + z.shape[1:], lambda i, plan, c=c: (base + i) * n_z + c) for c in range(n_z)],
        blocks((1, 1, rows), here),
        blocks(lab_block, lambda *_: base),
        blocks(lab_block, then),
        *[blocks(gl_block, lambda *_: base % per_set)] * 4,
        *[blocks(gl_block, lambda i, plan: lax.rem(then(i, plan), per_set))] * 4,
    ]
    in_specs += place_specs(recvs)
    args = [table, *[enc] * GW_SPLIT, *[z] * n_z, lse_rows, lab_rows, lab_rows, *gls, *gls, *recvs]
    if not is_first:
        in_specs.append(whole(n_cols, depth))
        args.append(acc)
    in_specs.append(in_place())
    aliases = {len(args): 0}
    args.append(prev)
    shape = (depth, n_cols) if is_last else (n_cols, depth)
    return pl.pallas_call(
        functools.partial(gw_kernel, plan, where, base, per_set, steps, n_z, is_first, is_last),
        grid_spec=pltpu.PrefetchScalarGridSpec(
            num_scalar_prefetch=1,
            grid=(steps,),
            in_specs=in_specs,
            out_specs=(in_place(), whole(*shape)),
            scratch_shapes=[
                pltpu.VMEM((n_cols, depth), jnp.float32),
                pltpu.VMEM((n_frames, rows), jnp.bfloat16),
                pltpu.VMEM((GROUP * SLOTS, rows), jnp.float32),
                pltpu.VMEM((2, n_cols, rows), jnp.bfloat16),
                pltpu.VMEM((ROW, depth), jnp.float32),
                pltpu.SemaphoreType.DMA((max(len(recvs), 1),)),
                pltpu.SemaphoreType.DMA,
            ],
        ),
        out_shape=(jax.ShapeDtypeStruct(prev.shape, jnp.float32), jax.ShapeDtypeStruct(shape, jnp.float32)),
        input_output_aliases=aliases,
        compiler_params=params(),
        cost_estimate=pl.CostEstimate(flops=2 * steps * rows * depth * n_cols, bytes_accessed=4 * steps * rows * n_cols, transcendentals=steps * rows * n_cols),
        name="gw_part",
    )(*args)


def place_kernel(plan, where, plan_ref, *refs):
    n = len(where)
    out_ref = refs[n + 1]
    bufs, sem_in, sem_out = refs[n + 2 : -2], *refs[-2:]
    loads = [pltpu.make_async_copy(ref, buf, sem_in.at[i]) for i, (ref, buf) in enumerate(zip(refs, bufs))]
    for copy in loads:
        copy.start()
    for i, (copy, buf, (first, total, flip)) in enumerate(zip(loads, bufs, where)):
        copy.wait()
        start_groups(buf, total, (plan_ref[plan.mine] ^ flip) * plan.groups + first, out_ref, plan_ref, sem_out.at[i])
    for i, buf in enumerate(bufs):
        pltpu.make_async_copy(buf, out_ref.at[pl.ds(0, buf.shape[0]), :], sem_out.at[i]).wait()


def place(plan, table, recvs, where, prev):
    n = len(recvs)
    return pl.pallas_call(
        functools.partial(place_kernel, plan, where),
        grid_spec=pltpu.PrefetchScalarGridSpec(
            num_scalar_prefetch=1,
            grid=(),
            in_specs=[in_place()] * (n + 1),
            out_specs=in_place(),
            scratch_shapes=[pltpu.VMEM(r.shape, r.dtype) for r in recvs] + [pltpu.SemaphoreType.DMA((n,))] * 2,
        ),
        out_shape=jax.ShapeDtypeStruct(prev.shape, jnp.float32),
        input_output_aliases={1 + n: 0},
        compiler_params=params(),
        name="place",
    )(table, *recvs, prev)


def solution(mesh):
    n_dev = mesh.shape["tp"]

    def swap(x, bit):
        return lax.ppermute(x, "tp", [(i, i ^ bit) for i in range(n_dev)])

    def device_fn(enc, w_loc, labels, in_len, lab_len):
        n_batch, n_frames, depth = enc.shape
        n_cols = w_loc.shape[1]
        n_lab = labels.shape[1]
        n_mine = n_batch // 4
        plan = Plan(n_batch, n_frames)
        room = plan.groups - SPARE
        sizes = [min(LARGE, room - at) for at in range(0, room, LARGE)]
        n_chunk = len(sizes)
        offs = [sum(sizes[:k]) for k in range(n_chunk + 1)]
        sizes.append(SPARE)
        tp = lax.axis_index("tp")
        core = tp % 2
        colour = (tp // 2 + tp // 4) % 2
        mine = 2 * colour + core

        u = np.arange(n_lab)
        valid = u[NEW, :] < lab_len[:, NEW]
        earlier = (labels[:, :, NEW] == labels[:, NEW, :]) & (u[NEW, :] < u[:, NEW])[NEW]
        first = valid & ~jnp.any(earlier, axis=2)
        slot_lab = jnp.concatenate(
            [jnp.where(first, labels, -1), jnp.zeros((n_batch, 1), jnp.int32), jnp.full((n_batch, SLOTS - n_lab - 1), -1, jnp.int32)], axis=1
        )

        wt = w_loc.T
        count = lax.shift_right_logical(in_len + (ROW - 1), ROW.bit_length() - 1).reshape(4, n_mine)
        n_live = jnp.sum(count, axis=1)
        full = n_frames // ROW
        pos = np.arange(plan.groups)[NEW, :, NEW]
        before = np.tri(n_mine, k=-1, dtype=bool)[NEW]
        number = np.arange(n_mine)
        seq_of = group_of = 0
        for n_kind, skip, shift in ((count, 0, 0), (full - count, count, n_live)):
            start = jnp.sum(jnp.where(before, n_kind[:, NEW, :], 0), axis=2)
            start = (start + jnp.broadcast_to(shift, (4,))[:, NEW])[:, NEW, :]
            inside = (start <= pos) & (pos < start + n_kind[:, NEW, :])
            seq_of += jnp.sum(jnp.where(inside, number, 0), axis=2)
            group_of += jnp.sum(jnp.where(inside, pos - start + number * full + jnp.broadcast_to(skip, count.shape)[:, NEW, :], 0), axis=2)
        first_row = (np.arange(4)[:, NEW] * plan.groups + group_of) * ROW
        own = jnp.stack([mine, tp * n_cols, mine * n_mine * n_frames])
        ints = jnp.concatenate([first_row.reshape(-1), lax.dynamic_index_in_dim(seq_of, mine, 0, keepdims=False), own]).astype(jnp.int32)
        flag = jnp.broadcast_to(jnp.max(n_live) > room, (8, 128)).astype(jnp.float32)

        wt_all, lse, z_loc, flag = spread_projection(enc, wt, slot_lab, flag, n_dev, mesh.shape["dp"])
        lse = lse.reshape(n_batch, n_frames)
        lse_live = lax.optimization_barrier(jnp.where(jnp.arange(n_frames)[NEW, :] < in_len[:, NEW], lse, BIG))
        def take(x):
            return lax.dynamic_slice_in_dim(x, mine * n_mine, n_mine, axis=0)

        lab_m = take(labels)
        slot_m = take(slot_lab)
        ext_m = jnp.concatenate([lab_m, jnp.zeros((n_mine, SLOTS - n_lab), jnp.int32)], axis=1)
        table = jnp.concatenate([lab_m, take(in_len)[:, NEW], take(lab_len)[:, NEW], ext_m[:, n_lab + 2 :]], axis=1).T
        lab_cols = ext_m.T.astype(jnp.float32)
        dup = jnp.pad(jnp.any(take(valid & ~first), axis=0).astype(jnp.int32), (0, SLOTS - n_lab))

        lab_flat = jnp.concatenate([ext_m[:, : n_lab + 1].reshape(-1), mine[NEW].astype(jnp.int32)])
        zl, lab_proj = label_logits(lab_flat, enc, lab_cols, wt_all, n_mine, n_lab + 1)
        lse_m = take(lse_live).T
        gl_gw, loss_m = lattice(dup, zl, lse_m, table, n_lab)
        loss_m = loss_m[0]
        gl_hs = jnp.transpose(gl_gw, (0, 2, 1))

        def spread(x):
            other = swap(x, 2)
            return [x, swap(x, 1), other, swap(other, 1)]

        losses = spread(loss_m)
        owner = (np.arange(4) ^ mine)[:, NEW]
        loss = sum(jnp.where(owner == flip, x[NEW, :], 0.0) for flip, x in enumerate(losses)).reshape(-1)
        gls = spread(gl_gw)

        moved = {}
        enc_rows = enc.reshape(-1, depth)

        def pick(*wanted):
            kinds = [(k, part, flip) for k, flip in wanted if k >= 0 for part in range(2)]
            return [moved[kind] for kind in kinds], [(offs[k] + part * (sizes[k] // 2), sizes[k] // 2, flip) for k, part, flip in kinds]

        def chunk(k, spots, prev, ints):
            return hs_chunk(offs[k], sizes[k], plan, ints, enc_rows, wt_all, lse_m, slot_m, gl_hs, lab_proj, n_lab + 1, *spots, prev)

        def send(k, sy, sz):
            for part, (x, bit) in enumerate(((sy, 2), (sz, 4))):
                moved[(k, part, 0)] = x
                moved[(k, part, 1)] = swap(x, 1)
                moved[(k, part, 2)] = swap(x, bit)

        def forward(k, after):
            for part in range(2):
                block, after = lax.optimization_barrier((moved[(k, part, 2)], after))
                moved[(k, part, 3)] = swap(block, 1)
            return after

        lse_rows = lse_live.reshape(n_batch // GROUP, 1, GROUP * n_frames)
        lab_rows = slot_lab.reshape(n_batch // GROUP, 1, GROUP * SLOTS)
        out = None
        for k in range(n_chunk):
            if k == 0:
                ints, lse_rows, lab_rows = lax.optimization_barrier((ints, lse_rows, lab_rows))
            if k == min(2, n_chunk - 1):
                ints, loss, gls = lax.optimization_barrier((ints, loss, gls))
            out, sy, sz = chunk(k, pick((k - 1, 0), (k - 2, 1), (k - 2, 2), (k - 3, 3)), out, ints)
            if 0 < k < n_chunk - 1:
                sy = forward(k - 1, sy)
            send(k, sy, sz)

        acc = None
        n = n_chunk
        late = (((n - 1, 0), (n - 2, 1), (n - 3, 3)), ((n - 1, 1), (n - 2, 2)))
        for part, wanted in enumerate(late):
            out, acc = gw_part(part, len(late), plan, ints, enc, z_loc, lse_rows, lab_rows, gls, *pick(*wanted), acc, out)
            acc = forward(n - 2 + part, acc)
        out = place(plan, ints, *pick((n - 2, 3), (n - 1, 2)), out)
        out = place(plan, ints, *pick((n - 1, 3)), out)

        def rest(out):
            out, sy, sz = chunk(n, ([], []), out, ints)
            send(n, sy, sz)
            forward(n, out)
            return place(plan, ints, *pick(*[(n, flip) for flip in range(4)]), out)

        out = lax.cond(flag[0, 0] > 0, rest, lambda out: out, out)
        return loss, acc, out.reshape(n_batch, n_frames, depth)

    return jax.shard_map(
        device_fn,
        mesh=mesh,
        in_specs=(P("dp"), P(None, "tp"), P("dp"), P("dp"), P("dp")),
        out_specs=(P("dp"), P("dp", "tp"), P("dp")),
        check_vma=False,
    )
```

```python
import functools

import jax
import jax.numpy as jnp
import numpy as np
from jax import lax
from jax.experimental import pallas as pl
from jax.experimental.pallas import tpu as pltpu
from jax.sharding import PartitionSpec as P


NEG_FILL = -1.0e30
NEW = None
BIG = 1.0e30
MESH = pl.DeviceIdType.MESH
NT = (((1,), (1,)), ((), ()))
NN = (((1,), (0,)), ((), ()))
TN = (((0,), (0,)), ((), ()))
SLOTS = 32
ROWS = 8
HS_WIDTH = 1024
ROW = 16
SPARE = 48
LARGE = 80
PLACE = 5
GROUP = 8
GW_SPLIT = 2
GW_AHEAD = 3
Z_SEQS = 4
VMEM_LIMIT = 60 * 1024 * 1024


def dot(a, b, dims):
    return lax.dot_general(a, b, dims, preferred_element_type=jnp.float32)


def whole(*shape):
    return pl.BlockSpec(shape, lambda *_: (0,) * len(shape))


def blocks(shape, first):
    return pl.BlockSpec(shape, lambda *g: (first(*g),) + (0,) * (len(shape) - 1))


def in_place():
    return pl.BlockSpec(memory_space=pl.ANY)


def in_vmem():
    return pl.BlockSpec(memory_space=pltpu.VMEM)


def params(**kw):
    return pltpu.CompilerParams(vmem_limit_bytes=VMEM_LIMIT, **kw)


SUBS = 4
N_Z = 4
HOPS = SUBS * (N_Z - 1)
LAG_Y, LAG_X = 2, 4
IDS = SUBS + 2 * HOPS
KINDS = 1, 2


def spread_kernel(n_dev, n_dp, enc_hbm, w_ref, lab_ref, flag_ref, all_ref, lse_ref, z_hbm, any_ref, *scratch):
    encbuf, st, recv, mine, bias, zbuf, flag, enc_sem, own_sem, z_sem, f_send, f_recv, *sems = scratch
    dn_send, dn_recv, up_send, up_recv, y_send, y_recv, x_send, x_recv, v_send, v_recv, c_send, c_recv, s1_send, s1_recv, s2_send, s2_recv = sems
    dp = lax.axis_index("dp")
    tp = lax.axis_index("tp")
    core = lax.rem(tp, 2)
    z = lax.div(tp, 4)
    mate = tp + 1 - 2 * core
    across = tp + 2 - 4 * lax.rem(lax.div(tp, 2), 2)
    block = w_ref.shape[0]
    piece = block // SUBS
    crosses = (core == dp) if n_dp > 1 else (core >= 0)
    n_seq, n_frames, depth = encbuf.shape[1:]

    def rows(owner, s):
        return all_ref.at[pl.ds(pl.multiple_of(owner * block + s * piece, piece), piece), :]

    def move(src, owner, s, send, got, dst):
        return pltpu.make_async_remote_copy(src_ref=src, dst_ref=rows(owner, s), send_sem=send, recv_sem=got, device_id=dst, device_id_type=MESH)

    def to(dev):
        return {"tp": dev}

    beside = {"dp": 1 - dp} if n_dp > 1 else to(tp)

    def owner_of(base, kind, q):
        hop = lax.div(q, SUBS) + 1
        return base + (4 * hop if kind == 1 else -4 * hop)

    def there(kind, q):
        hop = lax.div(q, SUBS) + 1
        return (q >= 0) & (q < HOPS) & ((z + hop <= N_Z - 1) if kind == 1 else (z - hop >= 0))

    inner = (z >= 1) & (z <= N_Z - 2)

    def by_z(q):
        return (q >= SUBS) | crosses | inner

    barrier = pltpu.get_barrier_semaphore()
    for d in range(1, n_dev):
        pl.semaphore_signal(barrier, inc=1, device_id={"tp": lax.rem(tp + d, n_dev)}, device_id_type=MESH)
    if n_dp > 1:
        pl.semaphore_signal(barrier, inc=1, device_id=beside, device_id_type=MESH)
    pl.semaphore_wait(barrier, n_dev - 1 + (n_dp > 1))

    told = pltpu.make_async_remote_copy(src_ref=flag_ref, dst_ref=flag, send_sem=f_send, recv_sem=f_recv, device_id=beside, device_id_type=MESH)
    if n_dp > 1:
        told.start()
    else:
        flag[...] = flag_ref[...]
    own = pltpu.make_async_copy(w_ref, all_ref.at[pl.ds(pl.multiple_of(tp * block, block), block), :], own_sem)
    own.start()

    def own_moves(s):
        src = w_ref.at[pl.ds(pl.multiple_of(s * piece, piece), piece), :]
        return (
            ((z >= 2) | ((z == 1) & crosses), move(src, tp, s, dn_send.at[s], dn_recv.at[s], to(tp - 4))),
            ((z < N_Z - 2) | ((z == N_Z - 2) & crosses), move(src, tp, s, up_send.at[s], up_recv.at[s], to(tp + 4))),
            (crosses, move(src, tp, s, y_send.at[s], y_recv.at[s], to(across))),
            (z >= 0, move(src, tp, s, c_send.at[s], c_recv.at[s], to(mate))),
        )

    def z_moves(kind, q):
        owner = owner_of(tp, kind, q)
        s = lax.rem(q, SUBS)
        src = rows(owner, s)
        got = dn_recv if kind == 1 else up_recv
        send = dn_send if kind == 1 else up_send
        number = SUBS + q + (0 if kind == 1 else HOPS)
        last = (z >= 1) if kind == 1 else (z <= N_Z - 2)
        nxt = lax.rem(q + SUBS, HOPS)
        here = there(kind, q) & by_z(q)
        return (
            here,
            move(src, owner, s, send.at[SUBS + q], got.at[q], to(tp)),
            (
                (here & last, move(src, owner, s, send.at[SUBS + q], got.at[nxt], to(tp - 4 if kind == 1 else tp + 4))),
                (here, move(src, owner, s, c_send.at[number], c_recv.at[number], to(mate))),
                (here & crosses, move(src, owner, s, y_send.at[number], y_recv.at[number], to(across))),
                (here & (q < SUBS) & jnp.logical_not(inner) & (n_dp > 1), move(src, owner, s, v_send.at[number], v_recv.at[number], beside)),
            ),
        )

    def v_moves(kind, q):
        q0 = lax.rem(q + HOPS, HOPS)
        owner, s, number = owner_of(tp, kind, q0), lax.rem(q0, SUBS), SUBS + q0 + (0 if kind == 1 else HOPS)
        src = rows(owner, s)
        here = there(kind, q) & jnp.logical_not(by_z(q))
        return (
            here,
            move(src, owner, s, v_send.at[number], v_recv.at[number], to(tp)),
            ((here, move(src, owner, s, c_send.at[number], c_recv.at[number], to(mate))),),
        )

    def far_parts(kind, q):
        if kind == 0:
            q0 = lax.rem(q + SUBS, SUBS)
            return across, q0, q0, (q >= 0) & (q < SUBS)
        q0 = lax.rem(q + HOPS, HOPS)
        return owner_of(across, kind, q0), lax.rem(q0, SUBS), SUBS + q0 + (0 if kind == 1 else HOPS), there(kind, q)

    def y_moves(kind, q):
        owner, s, number, here = far_parts(kind, q)
        src = rows(owner, s)
        return (
            here & crosses,
            move(src, owner, s, y_send.at[number], y_recv.at[number], to(tp)),
            (
                (here & crosses & (n_dp > 1), move(src, owner, s, x_send.at[number], x_recv.at[number], beside)),
                (here & crosses, move(src, owner, s, c_send.at[IDS + number], c_recv.at[IDS + number], to(mate))),
            ),
        )

    def x_moves(kind, q):
        owner, s, number, here = far_parts(kind, q)
        src = rows(owner, s)
        return (
            here & jnp.logical_not(crosses),
            move(src, owner, s, x_send.at[number], x_recv.at[number], to(tp)),
            ((here & jnp.logical_not(crosses), move(src, owner, s, c_send.at[IDS + number], c_recv.at[IDS + number], to(mate))),),
        )

    def start_all(moves):
        for cond, copy in moves:

            @pl.when(cond)
            def _():
                copy.start()

    def relay(group):
        cond, arrival, moves = group

        @pl.when(cond)
        def _():
            arrival.wait_recv()

        start_all(moves)

    def service(q):
        for kind in KINDS:
            relay(z_moves(kind, q))
        relay(y_moves(0, jnp.minimum(q - 1, SUBS)))
        for kind in KINDS:
            relay(y_moves(kind, q - LAG_Y))
        if n_dp > 1:
            for kind in KINDS:
                relay(v_moves(kind, q - LAG_Y))
            relay(x_moves(0, jnp.minimum(q + 1 - LAG_X, SUBS)))
            for kind in KINDS:
                relay(x_moves(kind, q - LAG_X))

    def enc_copy(i):
        slot = lax.rem(i, 2)
        return pltpu.make_async_copy(enc_hbm.at[pl.ds(i * n_seq, n_seq)], encbuf.at[slot], enc_sem.at[slot])

    n_part = zbuf.shape[1]

    def z_copy(i):
        slot = lax.rem(i, 2)
        return pltpu.make_async_copy(zbuf.at[slot], z_hbm.at[pl.ds(i * n_part, n_part)], z_sem.at[slot])

    enc_copy(0).start()
    for s in range(SUBS):
        start_all(own_moves(s))
    seq_r = lax.div(lax.broadcasted_iota(jnp.int32, bias.shape, 0), SLOTS)
    seq_c = lax.div(lax.broadcasted_iota(jnp.int32, bias.shape, 1), n_frames)
    bias[...] = jnp.where(seq_r == seq_c, NEG_FILL, 0.0).astype(bias.dtype)
    col = tp * block + lax.broadcasted_iota(jnp.int32, (block, n_seq * SLOTS), 0)

    busy = n_dev - SUBS - 2

    def tile(i, carry):
        enc_copy(i).wait()

        @pl.when(i + 1 < n_dev)
        def _():
            enc_copy(i + 1).start()

        slot = lax.rem(i, 2)
        enc = encbuf[slot].reshape(n_seq * n_frames, depth)
        zt = dot(w_ref[...], enc, NT)
        top = jnp.max(zt, axis=0, keepdims=True)
        st[i, 0:1, :] = top
        st[i, 1:2, :] = jnp.sum(jnp.exp(zt - top), axis=0, keepdims=True)

        @pl.when(i >= 2)
        def _():
            z_copy(i - 2).wait()

        hot = (col == lab_ref[i]).astype(jnp.bfloat16)
        masked = zt + dot(hot, bias[...], NN)
        size = zbuf.shape[-1]
        for c in range(n_part):
            zbuf[slot, c] = masked[:, c * size : (c + 1) * size]
        z_copy(i).start()
        return carry

    def tiles(q):
        return jnp.minimum(2 * q + 1, q + n_dev - busy + 1)

    def with_tiles(q, carry):
        lax.fori_loop(jnp.maximum(tiles(q - 1), 0), tiles(q), tile, 0)
        service(q)
        return carry

    def plain(q, carry):
        service(q)
        return carry

    lax.fori_loop(0, busy, with_tiles, 0)
    first = []
    for d in range(1, n_dev):
        peer = lax.rem(tp + d, n_dev)
        first.append(
            pltpu.make_async_remote_copy(
                src_ref=st.at[peer], dst_ref=recv.at[tp], send_sem=s1_send.at[d], recv_sem=s1_recv.at[d], device_id=to(peer), device_id_type=MESH
            )
        )
    for copy in first:
        copy.start()
    recv[tp] = st[tp]
    lax.fori_loop(busy, busy + 1, plain, 0)
    for copy in first:
        copy.wait()
    top = recv[0, 0:1, :]
    for j in range(1, n_dev):
        top = jnp.maximum(top, recv[j, 0:1, :])
    total = jnp.zeros_like(top)
    for j in range(n_dev):
        total = total + recv[j, 1:2, :] * jnp.exp(recv[j, 0:1, :] - top)
    lse = top + jnp.log(total)
    mine[...] = lse
    lse_ref[tp] = lse
    second = []
    for d in range(1, n_dev):
        peer = lax.rem(tp + d, n_dev)
        second.append(
            pltpu.make_async_remote_copy(
                src_ref=mine, dst_ref=lse_ref.at[tp], send_sem=s2_send.at[d], recv_sem=s2_recv.at[d], device_id=to(peer), device_id_type=MESH
            )
        )
    for copy in second:
        copy.start()
    lax.fori_loop(busy + 1, HOPS, plain, 0)

    def late(q, carry):
        for kind in KINDS:
            relay(y_moves(kind, q - LAG_Y))
            if n_dp > 1:
                relay(v_moves(kind, q - LAG_Y))
                relay(x_moves(kind, q - LAG_X))
        return carry

    lax.fori_loop(HOPS, HOPS + LAG_X, late, 0)
    for copy in second:
        copy.wait()
    own.wait()
    if n_dp > 1:
        told.wait()
    any_ref[...] = jnp.maximum(flag_ref[...], flag[...])
    for i in range(n_dev - 2, n_dev):
        z_copy(i).wait()

    def drain(cond, copy):
        @pl.when(cond)
        def _():
            copy.wait_send()

    def finish_own(s, carry):
        for cond, copy in own_moves(s):
            drain(cond, copy)
        move(rows(mate, s), mate, s, c_send.at[s], c_recv.at[s], to(tp)).wait_recv()
        far = mate + across - tp
        move(rows(far, s), far, s, c_send.at[IDS + s], c_recv.at[IDS + s], to(tp)).wait_recv()
        for _, _, moves in (y_moves(0, s), x_moves(0, s)) if n_dp > 1 else (y_moves(0, s),):
            for cond, copy in moves:
                drain(cond, copy)
        return carry

    def finish(q, carry):
        for kind in KINDS:
            here = there(kind, q)
            groups = (z_moves(kind, q), y_moves(kind, q))
            if n_dp > 1:
                groups += (v_moves(kind, q), x_moves(kind, q))
            for _, _, moves in groups:
                for cond, copy in moves:
                    drain(cond, copy)
            number = SUBS + q + (0 if kind == 1 else HOPS)
            s = lax.rem(q, SUBS)

            @pl.when(here)
            def _():
                near = owner_of(mate, kind, q)
                move(rows(near, s), near, s, c_send.at[number], c_recv.at[number], to(tp)).wait_recv()
                far = owner_of(mate + across - tp, kind, q)
                move(rows(far, s), far, s, c_send.at[IDS + number], c_recv.at[IDS + number], to(tp)).wait_recv()

        return carry

    lax.fori_loop(0, SUBS, finish_own, 0)
    lax.fori_loop(0, HOPS, finish, 0)


def spread_projection(enc, wt, slot_lab, flag, n_dev, n_dp):
    n_batch, n_frames, depth = enc.shape
    n_cols = wt.shape[0]
    n_seq = n_batch // n_dev
    rows = n_seq * n_frames
    z_seqs = min(Z_SEQS, n_seq)
    dma = pltpu.SemaphoreType.DMA
    sems = [SUBS + HOPS, HOPS] * 2 + [IDS] * 6 + [2 * IDS] * 2 + [n_dev] * 4
    return pl.pallas_call(
        functools.partial(spread_kernel, n_dev, n_dp),
        in_specs=[in_place()] + [in_vmem()] * 3,
        out_specs=(in_place(), in_vmem(), in_place(), in_vmem()),
        out_shape=(
            jax.ShapeDtypeStruct((n_dev * n_cols, depth), wt.dtype),
            jax.ShapeDtypeStruct((n_dev, 1, rows), jnp.float32),
            jax.ShapeDtypeStruct((n_batch // z_seqs, n_cols, z_seqs * n_frames), jnp.float32),
            jax.ShapeDtypeStruct(flag.shape, flag.dtype),
        ),
        scratch_shapes=[
            pltpu.VMEM((2, n_seq, n_frames, depth), enc.dtype),
            pltpu.VMEM((n_dev, 2, rows), jnp.float32),
            pltpu.VMEM((n_dev, 2, rows), jnp.float32),
            pltpu.VMEM((1, rows), jnp.float32),
            pltpu.VMEM((n_seq * SLOTS, rows), jnp.bfloat16),
            pltpu.VMEM((2, n_seq // z_seqs, n_cols, z_seqs * n_frames), jnp.float32),
            pltpu.VMEM(flag.shape, flag.dtype),
            dma((2,)),
            dma,
            dma((2,)),
            dma,
            dma,
            *[dma((n,)) for n in sems],
        ],
        compiler_params=params(collective_id=0, has_side_effects=True),
        cost_estimate=pl.CostEstimate(flops=2 * n_batch * n_frames * depth * n_cols, bytes_accessed=2 * enc.size, transcendentals=0),
        name="spread_projection",
    )(enc, wt, slot_lab.reshape(n_dev, 1, n_seq * SLOTS), flag)


def label_kernel(n_lab, step_seqs, lab_ref, enc_ref, tab_ref, wt_hbm, out_ref, rows_ref, buf, sem):
    i = pl.program_id(0)
    n_mine, span, depth = buf.shape
    used = n_lab * ROWS

    def fetch(s, carry):
        for u in range(n_lab):
            base = pl.multiple_of(lab_ref[s * n_lab + u] & -ROWS, ROWS)
            pltpu.make_async_copy(wt_hbm.at[pl.ds(base, ROWS), :], buf.at[s, pl.ds(u * ROWS, ROWS), :], sem.at[s]).start()
        return carry

    ahead = 2 * step_seqs

    @pl.when(i == 0)
    def _():
        lax.fori_loop(0, jnp.minimum(ahead, n_mine), fetch, 0)
        buf[:, used:, :] = jnp.zeros((n_mine, span - used, depth), buf.dtype)

    lax.fori_loop(jnp.minimum(i * step_seqs + ahead, n_mine), jnp.minimum((i + 1) * step_seqs + ahead, n_mine), fetch, 0)

    lane = lax.broadcasted_iota(jnp.int32, (SLOTS, span), 1)
    row = lax.broadcasted_iota(jnp.int32, (SLOTS, span), 0)
    for s in range(step_seqs):
        at = i * step_seqs + s
        pltpu.make_async_copy(wt_hbm.at[pl.ds(0, used), :], buf.at[at, pl.ds(0, used), :], sem.at[at]).wait()
    table = tab_ref[...]
    seq = lax.broadcasted_iota(jnp.int32, table.shape, 1)
    for s in range(step_seqs):
        mine = jnp.sum(jnp.where(seq == i * step_seqs + s, table, 0.0), axis=1, keepdims=True).astype(jnp.int32)
        pick = ((lane == row * ROWS + (mine & (ROWS - 1))) & (row < n_lab)).astype(jnp.bfloat16)
        rows_ref[s] = dot(pick, buf[i * step_seqs + s], NN).astype(rows_ref.dtype)
    for s in range(step_seqs):
        out_ref[s] = dot(rows_ref[s], enc_ref[s], NT)


def label_logits(lab_flat, enc, table, wt_all, n_mine, n_lab):
    _, n_frames, depth = enc.shape
    step_seqs = GROUP
    steps = n_mine // step_seqs
    span = (n_lab * ROWS + 15) // 16 * 16
    return pl.pallas_call(
        functools.partial(label_kernel, n_lab, step_seqs),
        grid_spec=pltpu.PrefetchScalarGridSpec(
            num_scalar_prefetch=1,
            grid=(steps,),
            in_specs=[
                blocks((step_seqs, n_frames, depth), lambda i, lab: lab[n_mine * n_lab] * steps + i),
                whole(*table.shape),
                in_place(),
            ],
            out_specs=(blocks((step_seqs, SLOTS, n_frames), lambda i, *_: i), blocks((step_seqs, SLOTS, depth), lambda i, *_: i)),
            scratch_shapes=[pltpu.VMEM((n_mine, span, depth), jnp.bfloat16), pltpu.SemaphoreType.DMA((n_mine,))],
        ),
        out_shape=(jax.ShapeDtypeStruct((n_mine, SLOTS, n_frames), jnp.float32), jax.ShapeDtypeStruct((n_mine, SLOTS, depth), jnp.bfloat16)),
        compiler_params=params(),
        cost_estimate=pl.CostEstimate(flops=2 * n_mine * n_lab * ROWS * n_frames * depth, bytes_accessed=4 * n_mine * n_lab * ROWS * depth, transcendentals=0),
        name="label_logits",
    )(lab_flat, enc, table, wt_all)


def several(body, n, width):
    def run(i, carry):
        for j in range(width):
            carry = body(i * width + j, carry)
        return carry

    return 0, n // width, run


def lattice_kernel(n_lab, dup_ref, seq_ref, lse_ref, lab_ref, out_ref, loss_ref, zl_ref, gl_ref, turned, bb, lb, ll, bl, sl, occ):
    n_frames, n_seq = lse_ref.shape
    shape = lab_ref.shape
    slots = shape[0]
    slot = lax.broadcasted_iota(jnp.int32, shape, 0)
    for u in range(slots):
        zl_ref[pl.ds(u, n_frames, slots), :] = jnp.transpose(seq_ref[pl.ds(u, n_seq, slots), :])

    def at(t):
        return pl.ds(pl.multiple_of(t * slots, slots), slots)

    blank_slot = n_lab - 1
    lab = lab_ref[...]
    in_len = lab_ref[blank_slot:n_lab, :]
    lab_len = lab_ref[n_lab : n_lab + 1, :]
    skip = (slot > 0) & (lab != pltpu.roll(lab, 1, 0))
    first = slot < lab_len
    for v in range(blank_slot - 1):
        first = first & ((lab != lab_ref[v : v + 1, :]) | (slot <= v))
    first = (first & (slot < blank_slot)) | (slot == blank_slot)
    neg = jnp.full(shape, NEG_FILL, jnp.float32)

    def forward(t, carry):
        b, l = carry
        e = zl_ref[at(t), :] - lse_ref[pl.ds(t, 1), :]
        eb = e[blank_slot:n_lab, :]
        prev = jnp.where(slot == 0, neg, pltpu.roll(l, 1, 0))
        top_b = jnp.maximum(b, prev)
        x0 = jnp.exp(b - top_b)
        x1 = jnp.exp(prev - top_b)
        sum_b = x0 + x1
        hop = jnp.where(skip, prev, neg)
        top_l = jnp.maximum(jnp.maximum(l, b), hop)
        y0 = jnp.exp(l - top_l)
        y1 = jnp.exp(b - top_l)
        y2 = jnp.exp(hop - top_l)
        sum_l = y0 + y1 + y2
        inv_b = 1.0 / sum_b
        inv_l = 1.0 / sum_l
        bb[t] = x0 * inv_b
        lb[t] = x1 * inv_b
        ll[t] = y0 * inv_l
        bl[t] = y1 * inv_l
        sl[t] = y2 * inv_l
        live = t < in_len
        new_b = jnp.where(live, top_b + jnp.log(sum_b) + eb, b)
        new_l = jnp.where(live, top_l + jnp.log(sum_l) + e, l)
        return new_b, new_l

    b, l = lax.fori_loop(*several(forward, n_frames, 4), (jnp.where(slot == 0, 0.0, neg), neg))
    end_b = jnp.where(slot == lab_len, b, neg)
    end_l = jnp.where(slot == lab_len - 1, l, neg)
    top = jnp.max(jnp.maximum(end_b, end_l), axis=0, keepdims=True)
    total = jnp.sum(jnp.exp(end_b - top) + jnp.exp(end_l - top), axis=0, keepdims=True)
    log_like = top + jnp.log(total)
    loss_ref[...] = -log_like

    def backward(i, carry):
        t = n_frames - 1 - i
        gb, gl = carry
        live = t < in_len
        blank = jnp.sum(gb, axis=0, keepdims=True)
        occ[t] = jnp.where(live, jnp.where(slot < blank_slot, gl, jnp.where(slot == blank_slot, blank, 0.0)), 0.0)
        back = pltpu.roll(gb * lb[t] + gl * sl[t], shape[0] - 1, 0)
        new_b = gb * bb[t] + gl * bl[t]
        new_l = gl * ll[t] + back
        return jnp.where(live, new_b, gb), jnp.where(live, new_l, gl)

    lax.fori_loop(*several(backward, n_frames, 4), (jnp.exp(end_b - log_like), jnp.exp(end_l - log_like)))

    for v in range(1, blank_slot):

        @pl.when(dup_ref[v] > 0)
        def _():
            take = (lab == lab_ref[v : v + 1, :]) & first & (slot < v)

            def add(t, _):
                row = occ[t]
                occ[t] = row + jnp.where(take, row[v : v + 1, :], 0.0)
                return 0

            lax.fori_loop(0, n_frames, add, 0)

    def emit(t, _):
        p = jnp.exp(zl_ref[at(t), :] - lse_ref[pl.ds(t, 1), :])
        gl_ref[at(t), :] = jnp.where(first & (t < in_len), p - occ[t], 0.0)
        return 0

    lax.fori_loop(*several(emit, n_frames, 4), 0)
    turned[...] = jnp.zeros_like(turned)
    for u in range(n_lab):
        turned[pl.ds(u, n_seq, slots), :] = jnp.transpose(gl_ref[pl.ds(u, n_frames, slots), :])
    out_ref[...] = turned[...].astype(out_ref.dtype)


def lattice(dup, zl, lse, table, n_lab):
    n_seq, slots, n_frames = zl.shape
    by_frame = pltpu.VMEM((n_frames * slots, n_seq), jnp.float32)
    by_seq = (n_seq * slots, n_frames)
    gl, loss = pl.pallas_call(
        functools.partial(lattice_kernel, n_lab + 1),
        in_specs=[pl.BlockSpec(memory_space=pltpu.SMEM)] + [in_vmem()] * 3,
        out_specs=(in_vmem(), in_vmem()),
        out_shape=(jax.ShapeDtypeStruct(by_seq, jnp.bfloat16), jax.ShapeDtypeStruct((1, n_seq), jnp.float32)),
        scratch_shapes=[by_frame, by_frame, pltpu.VMEM(by_seq, jnp.float32)] + [pltpu.VMEM((n_frames, slots, n_seq), jnp.float32)] * 6,
        compiler_params=params(),
        cost_estimate=pl.CostEstimate(flops=2 * 10**10, bytes_accessed=2 * zl.size, transcendentals=0),
        name="lattice",
    )(dup, zl.reshape(by_seq), lse, table)
    return gl.reshape(zl.shape), loss


class Plan:
    def __init__(self, n_batch, n_frames):
        self.groups = n_batch * n_frames // ROW // 4
        self.seq = 4 * self.groups
        self.mine = self.seq + self.groups
        self.column = self.mine + 1
        self.row = self.column + 1


def place_specs(recvs):
    return [blocks((PLACE * ROW, r.shape[1]), lambda i, plan, last=r.shape[0] // (PLACE * ROW) - 1: jnp.minimum(i, last)) for r in recvs]


def placing(refs, where, out_ref, plan, plan_ref, sem, act):
    step = pl.program_id(0)
    for i, (ref, (first, total, flip)) in enumerate(zip(refs, where)):

        @pl.when(step < total // PLACE)
        def _():
            if act == "wait":
                pltpu.make_async_copy(ref, out_ref.at[pl.ds(0, PLACE * ROW), :], sem.at[i]).wait()
            else:
                start_groups(ref, PLACE, (plan_ref[plan.mine] ^ flip) * plan.groups + first + step * PLACE, out_ref, plan_ref, sem.at[i])


def start_groups(ref, n, at, out_ref, plan_ref, sem):
    for g in range(n):
        row = pl.multiple_of(plan_ref[at + g], ROW)
        pltpu.make_async_copy(ref.at[pl.ds(g * ROW, ROW), :], out_ref.at[pl.ds(row, ROW), :], sem).start()


def hs_kernel(n_lab, plan, first, n_groups, where, has_prev, plan_ref, enc_hbm, w0_ref, w1_ref, lse_ref, slot_ref, gl_ref, rows_ref, *refs):
    n_recv = len(where)
    recvs = refs[:n_recv]
    out_ref, sy_ref, sz_ref, enc, slots, shift, sem_e, sem_r = refs[n_recv + has_prev :]
    j = pl.program_id(0)
    half = n_groups // 2
    spots = (recvs, where, out_ref, plan, plan_ref, sem_r)
    placing(*spots, "start")

    @pl.when(j == 0)
    def _():
        mine = plan_ref[plan.mine] * plan.groups + first

        def gather(i, carry):
            for g in range(8):
                r = i * 8 + g
                row = pl.multiple_of(plan_ref[mine + r], ROW)
                to = pl.ds(pl.multiple_of(r * ROW, ROW), ROW)
                pltpu.make_async_copy(enc_hbm.at[pl.ds(row, ROW), :], enc.at[to, :], sem_e).start()
                slots[pl.ds(r, 1), :] = slot_ref[pl.ds(plan_ref[plan.seq + first + r], 1), :]
            return carry

        lax.fori_loop(0, n_groups // 8, gather, 0)
        lane = lax.broadcasted_iota(jnp.int32, (ROW, lse_ref.shape[1]), 1)
        for r in range(n_groups):
            seq = plan_ref[plan.seq + first + r]
            frame = pl.multiple_of(plan_ref[mine + r] - plan_ref[plan.row] - seq * lse_ref.shape[0], ROW)
            column = jnp.sum(jnp.where(lane == seq, lse_ref[pl.ds(frame, ROW), :], 0.0), axis=1, keepdims=True)
            shift[r] = jnp.broadcast_to(column, (ROW, 128))
        for part, acc in enumerate((sy_ref, sz_ref)):

            def share(i, carry):
                for g in range(8):
                    r = i * 8 + g
                    seq = plan_ref[plan.seq + first + part * half + r]
                    frame = plan_ref[mine + part * half + r] - plan_ref[plan.row] - seq * gl_ref.shape[1]
                    share_g = gl_ref[seq, pl.ds(pl.multiple_of(frame, ROW), ROW), :]
                    acc[pl.ds(pl.multiple_of(r * ROW, ROW), ROW), :] = dot(share_g, rows_ref[seq], NN)
                return carry

            lax.fori_loop(0, half // 8, share, 0)
        pltpu.make_async_copy(enc_hbm.at[pl.ds(0, n_groups * ROW), :], enc, sem_e).wait()

    w = jnp.concatenate([w0_ref[...], w1_ref[...]], axis=0)
    width = w.shape[0]
    col = j * width + lax.broadcasted_iota(jnp.int32, (8, width), 1)
    biases = []
    for i in range(n_groups // 8):
        bias = jnp.zeros((8, width), jnp.float32)
        for u in range(n_lab):
            bias = jnp.where(col == slots[i * 8 : (i + 1) * 8, u : u + 1], NEG_FILL, bias)
        biases.append(bias)
    for part, acc in enumerate((sy_ref, sz_ref)):
        z = dot(enc[part * half * ROW : (part + 1) * half * ROW, :], w, NT)
        ps = []
        for g in range(half):
            r = part * half + g
            low = jnp.concatenate([shift[r]] * (width // 128), axis=1)
            p = jnp.exp(z[g * ROW : (g + 1) * ROW, :] - low + biases[r // 8][r % 8 : r % 8 + 1, :])
            ps.append(p.astype(jnp.bfloat16))
        acc[...] += dot(jnp.concatenate(ps, axis=0), w, NN)

    placing(*spots, "wait")


def hs_chunk(first, n_groups, plan, table, enc, wt_all, lse, slots, gl, lab_rows, n_lab, recvs, where, prev):
    n_rows, depth = enc.shape
    n_vocab = wt_all.shape[0]
    width = HS_WIDTH if n_vocab >= 8192 else 128
    steps = n_vocab // width
    in_specs = [
        in_place(),
        blocks((width // 2, depth), lambda j, table: 2 * j),
        blocks((width // 2, depth), lambda j, table: 2 * j + 1),
        whole(*lse.shape),
        whole(*slots.shape),
        whole(*gl.shape),
        whole(*lab_rows.shape),
    ]
    in_specs += place_specs(recvs)
    args = [table, enc, wt_all, wt_all, lse, slots, gl, lab_rows, *recvs]
    aliases = {}
    if prev is not None:
        in_specs.append(in_place())
        aliases = {len(args): 0}
        args.append(prev)
    rows = n_groups * ROW
    send = jax.ShapeDtypeStruct((rows // 2, depth), jnp.float32)
    return pl.pallas_call(
        functools.partial(hs_kernel, n_lab, plan, first, n_groups, where, int(prev is not None)),
        grid_spec=pltpu.PrefetchScalarGridSpec(
            num_scalar_prefetch=1,
            grid=(steps,),
            in_specs=in_specs,
            out_specs=(in_place(), whole(*send.shape), whole(*send.shape)),
            scratch_shapes=[
                pltpu.VMEM((rows, depth), jnp.bfloat16),
                pltpu.VMEM((n_groups, SLOTS), jnp.int32),
                pltpu.VMEM((n_groups, ROW, 128), jnp.float32),
                pltpu.SemaphoreType.DMA,
                pltpu.SemaphoreType.DMA((max(len(recvs), 1),)),
            ],
        ),
        out_shape=(jax.ShapeDtypeStruct((n_rows, depth), jnp.float32), send, send),
        input_output_aliases=aliases,
        compiler_params=params(),
        cost_estimate=pl.CostEstimate(flops=4 * rows * depth * n_vocab, bytes_accessed=2 * n_vocab * depth, transcendentals=rows * n_vocab),
        name="hs_chunk",
    )(*args)


def gw_kernel(plan, where, base, per_set, last_step, n_z, is_first, is_last, plan_ref, *refs):
    enc_hbm, z_hbm, lse_ref, lab0_ref, lab_ref, *refs = refs
    gl0_refs, gl_refs, refs = refs[:4], refs[4:8], refs[8:]
    n_recv = len(where)
    recvs = refs[:n_recv]
    acc_in = None if is_first else refs[n_recv]
    out_ref, gw_ref, acc, fan, diag, part, zero, enc_bufs, z_bufs, sem_r, sem_z, sem_f = refs[n_recv + (not is_first) + 1 :]
    i = pl.program_id(0)
    n_buf, n_seq, n_frames, depth = enc_bufs.shape
    n_cols, rows = acc.shape[0], n_seq * n_frames
    spots = (recvs, where, out_ref, plan, plan_ref, sem_r)
    placing(*spots, "start")

    def fetch(step, act):
        slot, tile = lax.rem(step, n_buf), base + step
        size = n_seq // GW_SPLIT
        for c in range(GW_SPLIT):
            at = pl.ds(c * size, size)
            act(pltpu.make_async_copy(enc_hbm.at[pl.ds(tile * n_seq + c * size, size)], enc_bufs.at[slot, at], sem_f.at[slot]))
        for c in range(n_z):
            act(pltpu.make_async_copy(z_hbm.at[tile * n_z + c], z_bufs.at[slot, c], sem_f.at[slot]))

    @pl.when(i == 0)
    def _():
        for step in range(n_buf - 1):
            fetch(step, lambda copy: copy.start())

    @pl.when(i + n_buf - 1 < last_step)
    def _():
        fetch(i + n_buf - 1, lambda copy: copy.start())

    def fanned(gls, step):
        owner = lax.div(base + step, per_set) ^ plan_ref[plan.mine]
        gl = gls[0][...]
        for flip in range(1, 4):
            gl = jnp.where(owner == flip, gls[flip][...], gl)
        return (dot(gl.reshape(n_seq * SLOTS, n_frames), fan[...], NN) * diag[...]).astype(jnp.bfloat16)

    def label_part(lab, wide):
        col = plan_ref[plan.column] + lax.broadcasted_iota(jnp.int32, (n_cols, n_seq * SLOTS), 0)
        return dot((col == lab[0]).astype(jnp.bfloat16), wide, NN).astype(jnp.bfloat16)

    @pl.when(i == 0)
    def _():
        seq_r = lax.div(lax.broadcasted_iota(jnp.int32, diag.shape, 0), SLOTS)
        seq_c = lax.div(lax.broadcasted_iota(jnp.int32, diag.shape, 1), n_frames)
        diag[...] = jnp.where(seq_r == seq_c, 1.0, 0.0)
        t_r = lax.broadcasted_iota(jnp.int32, fan.shape, 0)
        t_c = lax.rem(lax.broadcasted_iota(jnp.int32, fan.shape, 1), n_frames)
        fan[...] = (t_r == t_c).astype(jnp.bfloat16)
        zero[...] = jnp.zeros_like(zero)
        if is_first:
            acc[...] = jnp.zeros_like(acc)
        else:
            acc[...] = acc_in[...]
        part[0] = label_part(lab0_ref, fanned(gl0_refs, 0))

    def blank(act):
        n = 4 * SPARE // last_step
        at = lax.div(i * n, SPARE) * plan.groups + plan.groups - SPARE + lax.rem(i * n, SPARE)
        for g in range(n):
            row = pl.multiple_of(plan_ref[at + g], ROW)
            act(pltpu.make_async_copy(zero, out_ref.at[pl.ds(row, ROW), :], sem_z))

    if is_first:
        blank(lambda copy: copy.start())

    now = lax.rem(i, 2)
    fetch(i, lambda copy: copy.wait())
    slot = lax.rem(i, n_buf)
    enc = enc_bufs[slot].reshape(rows, depth)
    half = depth // 2
    wide = fanned(gl_refs, jnp.minimum(i + 1, pl.num_programs(0) - 1))
    ps = []
    size = rows // n_z
    for c in range(n_z):
        ps.append(jnp.exp(z_bufs[slot, c] - lse_ref[0, :, c * size : (c + 1) * size]).astype(jnp.bfloat16))
    g = jnp.concatenate(ps, axis=1) + part[now]
    acc[:, :half] += dot(g, enc[:, :half], NN)
    part[1 - now] = label_part(lab_ref, wide)
    acc[:, half:] += dot(g, enc[:, half:], NN)

    @pl.when(i == pl.num_programs(0) - 1)
    def _():
        gw_ref[...] = jnp.transpose(acc[...]) if is_last else acc[...]

    if is_first:
        blank(lambda copy: copy.wait())
    placing(*spots, "wait")


def gw_part(part, n_part, plan, table, enc, z, lse_rows, lab_rows, gls, recvs, where, acc, prev):
    n_batch, n_frames, depth = enc.shape
    n_cols = z.shape[1]
    n_z = GROUP * n_frames // z.shape[2]
    steps = n_batch // GROUP // n_part
    base = part * steps
    per_set = n_batch // GROUP // 4
    rows = GROUP * n_frames
    is_first, is_last = part == 0, part == n_part - 1

    def here(i, scal):
        return base + i

    def then(i, scal):
        return base + jnp.minimum(i + 1, steps - 1)

    lab_block, gl_block = (1, 1, GROUP * SLOTS), (GROUP, SLOTS, n_frames)
    in_specs = [
        in_place(),
        in_place(),
        blocks((1, 1, rows), here),
        blocks(lab_block, lambda *_: base),
        blocks(lab_block, then),
        *[blocks(gl_block, lambda *_: base % per_set)] * 4,
        *[blocks(gl_block, lambda i, plan: lax.rem(then(i, plan), per_set))] * 4,
    ]
    in_specs += place_specs(recvs)
    args = [table, enc, z, lse_rows, lab_rows, lab_rows, *gls, *gls, *recvs]
    if not is_first:
        in_specs.append(whole(n_cols, depth))
        args.append(acc)
    in_specs.append(in_place())
    aliases = {len(args): 0}
    args.append(prev)
    shape = (depth, n_cols) if is_last else (n_cols, depth)
    return pl.pallas_call(
        functools.partial(gw_kernel, plan, where, base, per_set, steps, n_z, is_first, is_last),
        grid_spec=pltpu.PrefetchScalarGridSpec(
            num_scalar_prefetch=1,
            grid=(steps,),
            in_specs=in_specs,
            out_specs=(in_place(), whole(*shape)),
            scratch_shapes=[
                pltpu.VMEM((n_cols, depth), jnp.float32),
                pltpu.VMEM((n_frames, rows), jnp.bfloat16),
                pltpu.VMEM((GROUP * SLOTS, rows), jnp.float32),
                pltpu.VMEM((2, n_cols, rows), jnp.bfloat16),
                pltpu.VMEM((ROW, depth), jnp.float32),
                pltpu.VMEM((GW_AHEAD, GROUP, n_frames, depth), enc.dtype),
                pltpu.VMEM((GW_AHEAD, n_z) + z.shape[1:], z.dtype),
                pltpu.SemaphoreType.DMA((max(len(recvs), 1),)),
                pltpu.SemaphoreType.DMA,
                pltpu.SemaphoreType.DMA((GW_AHEAD,)),
            ],
        ),
        out_shape=(jax.ShapeDtypeStruct(prev.shape, jnp.float32), jax.ShapeDtypeStruct(shape, jnp.float32)),
        input_output_aliases=aliases,
        compiler_params=params(),
        cost_estimate=pl.CostEstimate(flops=2 * steps * rows * depth * n_cols, bytes_accessed=4 * steps * rows * n_cols, transcendentals=steps * rows * n_cols),
        name="gw_part",
    )(*args)


def place_kernel(plan, where, plan_ref, *refs):
    n = len(where)
    out_ref = refs[n + 1]
    bufs, sem_in, sem_out = refs[n + 2 : -2], *refs[-2:]
    loads = [pltpu.make_async_copy(ref, buf, sem_in.at[i]) for i, (ref, buf) in enumerate(zip(refs, bufs))]
    for copy in loads:
        copy.start()
    for i, (copy, buf, (first, total, flip)) in enumerate(zip(loads, bufs, where)):
        copy.wait()
        start_groups(buf, total, (plan_ref[plan.mine] ^ flip) * plan.groups + first, out_ref, plan_ref, sem_out.at[i])
    for i, buf in enumerate(bufs):
        pltpu.make_async_copy(buf, out_ref.at[pl.ds(0, buf.shape[0]), :], sem_out.at[i]).wait()


def place(plan, table, recvs, where, prev):
    n = len(recvs)
    return pl.pallas_call(
        functools.partial(place_kernel, plan, where),
        grid_spec=pltpu.PrefetchScalarGridSpec(
            num_scalar_prefetch=1,
            grid=(),
            in_specs=[in_place()] * (n + 1),
            out_specs=in_place(),
            scratch_shapes=[pltpu.VMEM(r.shape, r.dtype) for r in recvs] + [pltpu.SemaphoreType.DMA((n,))] * 2,
        ),
        out_shape=jax.ShapeDtypeStruct(prev.shape, jnp.float32),
        input_output_aliases={1 + n: 0},
        compiler_params=params(),
        name="place",
    )(table, *recvs, prev)


def solution(mesh):
    n_dev = mesh.shape["tp"]

    def swap(x, bit):
        return lax.ppermute(x, "tp", [(i, i ^ bit) for i in range(n_dev)])

    def device_fn(enc, w_loc, labels, in_len, lab_len):
        n_batch, n_frames, depth = enc.shape
        n_cols = w_loc.shape[1]
        n_lab = labels.shape[1]
        n_mine = n_batch // 4
        plan = Plan(n_batch, n_frames)
        room = plan.groups - SPARE
        sizes = [min(LARGE, room - at) for at in range(0, room, LARGE)]
        n_chunk = len(sizes)
        offs = [sum(sizes[:k]) for k in range(n_chunk + 1)]
        sizes.append(SPARE)
        tp = lax.axis_index("tp")
        core = tp % 2
        colour = (tp // 2 + tp // 4) % 2
        mine = 2 * colour + core

        u = np.arange(n_lab)
        valid = u[NEW, :] < lab_len[:, NEW]
        earlier = (labels[:, :, NEW] == labels[:, NEW, :]) & (u[NEW, :] < u[:, NEW])[NEW]
        first = valid & ~jnp.any(earlier, axis=2)
        slot_lab = jnp.concatenate(
            [jnp.where(first, labels, -1), jnp.zeros((n_batch, 1), jnp.int32), jnp.full((n_batch, SLOTS - n_lab - 1), -1, jnp.int32)], axis=1
        )

        wt = w_loc.T
        count = lax.shift_right_logical(in_len + (ROW - 1), ROW.bit_length() - 1).reshape(4, n_mine)
        n_live = jnp.sum(count, axis=1)
        full = n_frames // ROW
        pos = np.arange(plan.groups)[NEW, :, NEW]
        before = np.tri(n_mine, k=-1, dtype=bool)[NEW]
        number = np.arange(n_mine)
        seq_of = group_of = 0
        for n_kind, skip, shift in ((count, 0, 0), (full - count, count, n_live)):
            start = jnp.sum(jnp.where(before, n_kind[:, NEW, :], 0), axis=2)
            start = (start + jnp.broadcast_to(shift, (4,))[:, NEW])[:, NEW, :]
            inside = (start <= pos) & (pos < start + n_kind[:, NEW, :])
            seq_of += jnp.sum(jnp.where(inside, number, 0), axis=2)
            group_of += jnp.sum(jnp.where(inside, pos - start + number * full + jnp.broadcast_to(skip, count.shape)[:, NEW, :], 0), axis=2)
        first_row = (np.arange(4)[:, NEW] * plan.groups + group_of) * ROW
        own = jnp.stack([mine, tp * n_cols, mine * n_mine * n_frames])
        ints = jnp.concatenate([first_row.reshape(-1), lax.dynamic_index_in_dim(seq_of, mine, 0, keepdims=False), own]).astype(jnp.int32)
        flag = jnp.broadcast_to(jnp.max(n_live) > room, (8, 128)).astype(jnp.float32)

        wt_all, lse, z_loc, flag = spread_projection(enc, wt, slot_lab, flag, n_dev, mesh.shape["dp"])
        lse = lse.reshape(n_batch, n_frames)
        lse_live = lax.optimization_barrier(jnp.where(jnp.arange(n_frames)[NEW, :] < in_len[:, NEW], lse, BIG))
        def take(x):
            return lax.dynamic_slice_in_dim(x, mine * n_mine, n_mine, axis=0)

        lab_m = take(labels)
        slot_m = take(slot_lab)
        ext_m = jnp.concatenate([lab_m, jnp.zeros((n_mine, SLOTS - n_lab), jnp.int32)], axis=1)
        table = jnp.concatenate([lab_m, take(in_len)[:, NEW], take(lab_len)[:, NEW], ext_m[:, n_lab + 2 :]], axis=1).T
        lab_cols = ext_m.T.astype(jnp.float32)
        dup = jnp.pad(jnp.any(take(valid & ~first), axis=0).astype(jnp.int32), (0, SLOTS - n_lab))

        lab_flat = jnp.concatenate([ext_m[:, : n_lab + 1].reshape(-1), mine[NEW].astype(jnp.int32)])
        zl, lab_proj = label_logits(lab_flat, enc, lab_cols, wt_all, n_mine, n_lab + 1)
        lse_m = take(lse_live).T
        gl_gw, loss_m = lattice(dup, zl, lse_m, table, n_lab)
        loss_m = loss_m[0]
        gl_hs = jnp.transpose(gl_gw, (0, 2, 1))

        def spread(x):
            other = swap(x, 2)
            return [x, swap(x, 1), other, swap(other, 1)]

        losses = spread(loss_m)
        owner = (np.arange(4) ^ mine)[:, NEW]
        loss = sum(jnp.where(owner == flip, x[NEW, :], 0.0) for flip, x in enumerate(losses)).reshape(-1)
        gls = spread(gl_gw)

        moved = {}
        enc_rows = enc.reshape(-1, depth)

        def pick(*wanted):
            kinds = [(k, part, flip) for k, flip in wanted if k >= 0 for part in range(2)]
            return [moved[kind] for kind in kinds], [(offs[k] + part * (sizes[k] // 2), sizes[k] // 2, flip) for k, part, flip in kinds]

        def chunk(k, spots, prev, ints):
            return hs_chunk(offs[k], sizes[k], plan, ints, enc_rows, wt_all, lse_m, slot_m, gl_hs, lab_proj, n_lab + 1, *spots, prev)

        def send(k, sy, sz):
            for part, (x, bit) in enumerate(((sy, 2), (sz, 4))):
                moved[(k, part, 0)] = x
                moved[(k, part, 1)] = swap(x, 1)
                moved[(k, part, 2)] = swap(x, bit)

        def forward(k, after):
            for part in range(2):
                block, after = lax.optimization_barrier((moved[(k, part, 2)], after))
                moved[(k, part, 3)] = swap(block, 1)
            return after

        lse_rows = lse_live.reshape(n_batch // GROUP, 1, GROUP * n_frames)
        lab_rows = slot_lab.reshape(n_batch // GROUP, 1, GROUP * SLOTS)
        out = None
        for k in range(n_chunk):
            if k == 0:
                ints, lse_rows, lab_rows = lax.optimization_barrier((ints, lse_rows, lab_rows))
            if k == min(2, n_chunk - 1):
                ints, loss, gls = lax.optimization_barrier((ints, loss, gls))
            out, sy, sz = chunk(k, pick((k - 1, 0), (k - 2, 1), (k - 2, 2), (k - 3, 3)), out, ints)
            if 0 < k < n_chunk - 1:
                sy = forward(k - 1, sy)
            send(k, sy, sz)

        acc = None
        n = n_chunk
        late = (((n - 1, 0), (n - 2, 1), (n - 3, 3)), ((n - 1, 1), (n - 2, 2)))
        for part, wanted in enumerate(late):
            out, acc = gw_part(part, len(late), plan, ints, enc, z_loc, lse_rows, lab_rows, gls, *pick(*wanted), acc, out)
            acc = forward(n - 2 + part, acc)
        out = place(plan, ints, *pick((n - 2, 3), (n - 1, 2)), out)
        out = place(plan, ints, *pick((n - 1, 3)), out)

        def rest(out):
            out, sy, sz = chunk(n, ([], []), out, ints)
            send(n, sy, sz)
            forward(n, out)
            return place(plan, ints, *pick(*[(n, flip) for flip in range(4)]), out)

        out = lax.cond(flag[0, 0] > 0, rest, lambda out: out, out)
        return loss, acc, out.reshape(n_batch, n_frames, depth)

    return jax.shard_map(
        device_fn,
        mesh=mesh,
        in_specs=(P("dp"), P(None, "tp"), P("dp"), P("dp"), P("dp")),
        out_specs=(P("dp"), P("dp", "tp"), P("dp")),
        check_vma=False,
    )
```
